32 devices in a mesh: dp: 4 (over z), row: 4 (over y, x), col: 2 (over core).
Axes of the slice: x: 2, y: 2, z: 4, core: 2. Of those that a mesh axis runs over, the one named last changes fastest.
Arguments:
- layer_input: bfloat16 [8192, 1536], P(('dp', 'row'), 'col'), may hold values from -6 to 6
- gain_attn: float32 [1536], P('col'), may hold values from 0.25 to 1.75
- gain_ffn: float32 [1536], P('col'), may hold values from 0.25 to 1.75
- w_query: bfloat16 [1536, 1536], P('col', 'row'), may hold values from -0.15625 to 0.15625
- w_key: bfloat16 [1536, 768], P('col', 'row'), may hold values from -0.15625 to 0.15625
- w_value: bfloat16 [1536, 768], P('col', 'row'), may hold values from -0.15625 to 0.15625
- w_out: bfloat16 [1536, 1536], P('row', 'col'), may hold values from -1.25 to 1.25
- w_gate: bfloat16 [1536, 4096], P('col', 'row'), may hold values from -0.15625 to 0.15625
- w_up: bfloat16 [1536, 4096], P('col', 'row'), may hold values from -0.15625 to 0.15625
- w_down: bfloat16 [4096, 1536], P('row', 'col'), may hold values from -0.09375 to 0.09375
- cotangent: bfloat16 [8192, 1536], P(('dp', 'row'), 'col'), may hold values from -6 to 6
Outputs:
- layer_output: float32 [8192, 1536], P(('dp', 'row'), 'col')
- grad_input: float32 [8192, 1536], P(('dp', 'row'), 'col')
- grad_gain_attn: float32 [1536], P('col')
- grad_gain_ffn: float32 [1536], P('col')
- grad_query: float32 [1536, 1536], P('col', 'row')
- grad_key: float32 [1536, 768], P('col', 'row')
- grad_value: float32 [1536, 768], P('col', 'row')
- grad_out: float32 [1536, 1536], P('row', 'col')
- grad_gate: float32 [1536, 4096], P('col', 'row')
- grad_up: float32 [1536, 4096], P('col', 'row')
- grad_down: float32 [4096, 1536], P('row', 'col')
The draws below stay inside these ranges and needn't reach their ends.
All inputs are finite; a program needn't handle non-finite values.
Results may differ from the reference program's by a relative error of at most 0.014.
Values may be sent and summed in bfloat16 or wider, within the bound.
A program may use at most 192 MiB of HBM per device.

```python
import jax
import jax.numpy as jnp
from jax import lax

D = 1536
FF = 4096
QH = 16
KVH = 8
HD = 96
LENGTH = 1024
SEQS_DP = 2
TOKENS = 8192


def steps_of(rng, dims, cuts, smallest, high):
    def one(dim, blocks):
        steps = jax.random.uniform(jax.random.fold_in(jax.random.fold_in(rng, 6), dim), (blocks,), jnp.float32, smallest / len(cuts), high / len(cuts))
        return jnp.repeat(jnp.exp(steps), dims[dim] // blocks).reshape((-1,) + (1,) * (len(dims) - dim - 1))

    factor_of = one(*cuts[0])
    for cut in cuts[1:]:
        factor_of = factor_of * one(*cut)
    return factor_of


def gaussian(stream_key, extent, width, limit, cuts=(), kind=jnp.bfloat16):
    values = jax.random.normal(stream_key, extent, jnp.float32) * width
    if len(cuts) > 0:
        values = steps_of(stream_key, extent, cuts, -0.22, 0.18) * values
    return jnp.clip(values, min=-limit, max=limit).astype(kind)


def setup_inputs(seed: int = 0) -> dict:
    seeds = jax.random.split(jax.random.key(seed), 12)
    layer_input = gaussian(seeds[0], (TOKENS, D), 1.0, 6.0, ((0, 16), (1, 2)))
    gain_attn = jnp.clip(1.0 + 0.15 * jax.random.normal(seeds[1], (D,), jnp.float32), 0.25, 1.75)
    gain_ffn = jnp.clip(1.0 + 0.15 * jax.random.normal(seeds[2], (D,), jnp.float32), 0.25, 1.75)
    w_query = gaussian(seeds[3], (D, QH * HD), D ** -0.5, 0.15625, ((0, 2), (1, 4)))
    w_key = gaussian(seeds[4], (D, KVH * HD), D ** -0.5, 0.15625, ((0, 2), (1, 4)))
    w_value = gaussian(seeds[5], (D, KVH * HD), D ** -0.5, 0.15625, ((0, 2), (1, 4)))
    w_out = gaussian(seeds[6], (QH * HD, D), (D // 64) ** -0.5, 1.25, ((0, 4), (1, 2)))
    w_gate = gaussian(seeds[7], (D, FF), D ** -0.5, 0.15625, ((0, 2), (1, 4)))
    w_up = gaussian(seeds[8], (D, FF), D ** -0.5, 0.15625, ((0, 2), (1, 4)))
    w_down = gaussian(seeds[9], (FF, D), FF ** -0.5, 0.09375, ((0, 4), (1, 2)))
    cotangent = gaussian(seeds[10], (TOKENS, D), 1.0, 6.0, ((0, 16), (1, 2)))
    return dict(layer_input=layer_input, gain_attn=gain_attn, gain_ffn=gain_ffn, w_query=w_query, w_key=w_key, w_value=w_value, w_out=w_out, w_gate=w_gate, w_up=w_up, w_down=w_down, cotangent=cotangent)


EPS = 1e-05
THETA = 100000.0

@jax.custom_vjp
def low(v):
    return lax.optimization_barrier(v.astype(jnp.bfloat16)).astype(jnp.float32)

@jax.custom_vjp
def low_back(v):
    return v

def low_keep(v):
    return (low(v), None)

def low_pass(kept, grad):
    return (grad,)

def back_keep(v):
    return (v, None)

def back_low(kept, grad):
    return (low(grad),)
low.defvjp(low_keep, low_pass)
low_back.defvjp(back_keep, back_low)

def matmul(left, right):
    return jnp.dot(left, right, precision=lax.Precision.HIGHEST, preferred_element_type=jnp.float32)

def rotate(values, heads):
    count = values.shape[0]
    half = HD // 2
    pos = (jnp.arange(count) % LENGTH).astype(jnp.float32)
    freq = THETA ** (-jnp.arange(half).astype(jnp.float32) * 2.0 / HD)
    angle = pos[:, None] * freq[None, :]
    cosine = jnp.cos(angle)[:, None, :]
    sine = jnp.sin(angle)[:, None, :]
    shaped = values.reshape(count, heads, HD)
    first = shaped[..., :half]
    second = shaped[..., half:]
    return jnp.concatenate([first * cosine - second * sine, second * cosine + first * sine], -1).reshape(count, heads * HD)

def attend_one(triple):
    queries, keys, values = triple
    span = queries.shape[0]
    group = QH // KVH
    q3 = queries.reshape(span, QH, HD)
    k3 = jnp.repeat(keys.reshape(span, KVH, HD), group, axis=1)
    v3 = jnp.repeat(values.reshape(span, KVH, HD), group, axis=1)
    scores = jnp.einsum('qhd,khd->hqk', q3, k3, precision=lax.Precision.HIGHEST) * HD ** (-0.5)
    scores = low_back(scores)
    allowed = jnp.arange(span)[None, :] <= jnp.arange(span)[:, None]
    scores = jnp.where(allowed[None], scores, -1e+30)
    expo = jnp.exp(scores - lax.optimization_barrier(jnp.max(scores, -1, keepdims=True)))
    probs = expo / lax.optimization_barrier(jnp.sum(expo, -1, keepdims=True))
    mixed = jnp.einsum('hqk,khd->qhd', low(probs), v3, precision=lax.Precision.HIGHEST)
    return mixed.reshape(span, QH * HD)

def layer(input_f32, gain_attn, gain_ffn, w_query, w_key, w_value, w_out, w_gate, w_up, w_down):
    count = input_f32.shape[0]
    rstd1 = lax.rsqrt(lax.optimization_barrier(jnp.mean(input_f32 * input_f32, axis=1, keepdims=True)) + EPS)
    normed_a = low(input_f32 * rstd1 * gain_attn)
    queries = low(rotate(low_back(matmul(normed_a, w_query)), QH))
    keys = low(rotate(low_back(matmul(normed_a, w_key)), KVH))
    values = low(low_back(matmul(normed_a, w_value)))
    seqs = count // LENGTH
    mixed = lax.map(jax.checkpoint(attend_one), (queries.reshape(seqs, LENGTH, -1), keys.reshape(seqs, LENGTH, -1), values.reshape(seqs, LENGTH, -1)))
    attn = low(low_back(mixed.reshape(count, QH * HD)))
    hidden = input_f32 + low_back(matmul(attn, w_out))
    rstd2 = lax.rsqrt(lax.optimization_barrier(jnp.mean(hidden * hidden, axis=1, keepdims=True)) + EPS)
    normed_f = low(hidden * rstd2 * gain_ffn)
    gate = low_back(matmul(normed_f, w_gate))
    upper = low_back(matmul(normed_f, w_up))
    middle = low(gate / (1.0 + jnp.exp(-gate)) * upper)
    return hidden + low_back(matmul(middle, w_down))

def reference(layer_input, gain_attn, gain_ffn, w_query, w_key, w_value, w_out, w_gate, w_up, w_down, cotangent):
    weights = tuple((w.astype(jnp.float32) for w in (gain_attn, gain_ffn, w_query, w_key, w_value, w_out, w_gate, w_up, w_down)))
    rows = SEQS_DP * LENGTH
    groups = layer_input.shape[0] // rows
    inputs = layer_input.astype(jnp.float32).reshape(groups, rows, D)
    grads_in = cotangent.astype(jnp.float32).reshape(groups, rows, D)
    zero = tuple((jnp.zeros_like(w) for w in weights))

    def one_group(acc, pair):
        piece, seed_grad = pair
        result, pull = jax.vjp(layer, piece, *weights)
        grads = pull(seed_grad)
        return (tuple((a + g for a, g in zip(acc, grads[1:]))), (result, grads[0]))
    acc, (outputs, input_grads) = lax.scan(one_group, zero, (inputs, grads_in))
    return (outputs.reshape(-1, D), input_grads.reshape(-1, D), acc[0], acc[1], acc[2], acc[3], acc[4], acc[5], acc[6], acc[7], acc[8])
```

```python
import jax
import jax.numpy as jnp
import numpy as np
from jax import lax
from jax.experimental import pallas as pl
from jax.experimental.pallas import tpu as pltpu
from jax.sharding import PartitionSpec as P

HD = 96
HALF = HD // 2
LENGTH = 1024
EPS = 1e-05
THETA = 100000.0
SCALE = HD ** (-0.5)
LANE = 128
PIECE = 256

BF = jnp.bfloat16
F32 = jnp.float32
MESH = pl.DeviceIdType.MESH
VM = pl.BlockSpec(memory_space=pltpu.VMEM)
ANY = pl.BlockSpec(memory_space=pl.ANY)
DMA = pltpu.SemaphoreType.DMA


def nn(a, b):
    return lax.dot_general(a, b, (((1,), (0,)), ((), ())), preferred_element_type=F32)


def nt(a, b):
    return lax.dot_general(a, b, (((1,), (1,)), ((), ())), preferred_element_type=F32)


def place():
    r = lax.axis_index("row")
    k = lax.axis_index("col")
    return r, k, r + 1 - 2 * (r % 2), (r + 2) % 4, 3 - r


def greet(rx, ry, k):
    bar = pltpu.get_barrier_semaphore()
    for device in ({"row": rx}, {"row": ry}, {"col": 1 - k}):
        pl.semaphore_signal(bar, inc=1, device_id=device, device_id_type=MESH)
    pl.semaphore_wait(bar, 3)


def remote(src, dst, send, recv, device):
    return pltpu.make_async_remote_copy(
        src_ref=src, dst_ref=dst, send_sem=send, recv_sem=recv, device_id=device, device_id_type=MESH
    )


def rows_of(half):
    return pl.ds(pl.multiple_of(half * PIECE, PIECE), PIECE)


GATHER_SEMS = [DMA((6,)), DMA((6,)), DMA((8,)), DMA((8,)), DMA]


class Gather:
    def __init__(self, own, buf, sems):
        self.own, self.buf = own, buf
        self.isend, self.irecv, self.dsend, self.drecv, self.lsem = sems
        self.r, self.k, self.rx, self.ry, self.r3 = place()

    def piece(self, i):
        side = jnp.where(i % 2 == 0, self.rx, self.ry)
        row = jnp.where(i < 2, self.r, jnp.where(i < 6, side, self.r3))
        half = jnp.where(i // 2 == 2, 1 - i % 2, i % 2)
        return row, half

    def ici(self, sem, row, half, device, src=None):
        dst = self.buf.at[self.k, row, rows_of(half)]
        return remote(dst if src is None else src, dst, self.isend.at[sem], self.irecv.at[sem], {"row": device})

    def pair(self, i, core, row, half, src=None):
        dst = self.buf.at[core, row, rows_of(half)]
        return remote(dst if src is None else src, dst, self.dsend.at[i], self.drecv.at[i], {"col": 1 - self.k})

    def start(self):
        first, second = self.own.at[pl.ds(0, PIECE)], self.own.at[pl.ds(PIECE, PIECE)]
        self.ici(0, self.r, 0, self.rx, first).start()
        self.ici(1, self.r, 1, self.ry, second).start()
        self.ici(2, self.r, 1, self.rx, second).start()
        self.ici(3, self.r, 0, self.ry, first).start()
        self.pair(0, self.k, self.r, 0, first).start()
        self.pair(1, self.k, self.r, 1, second).start()
        self.local = pltpu.make_async_copy(self.own, self.buf.at[self.k, self.r], self.lsem)
        self.local.start()

    def arrive(self, i):
        row, half = self.piece(i)
        self.ici(i - 2, row, half, self.rx).wait_recv()

        @pl.when(i == 2)
        def _():
            self.ici(4, row, half, self.ry).start()

        @pl.when(i == 3)
        def _():
            self.ici(5, row, half, self.rx).start()

        self.pair(i, self.k, row, half).start()

    def ready(self, i):
        row, half = self.piece(i)
        self.pair(i, 1 - self.k, row, half).wait_recv()

    def run(self, compute):
        self.local.wait()

        def step(i, carry):
            self.ready(i)
            row, half = self.piece(i)
            compute(i, row, half)

            @pl.when(i < 6)
            def _():
                self.arrive(i + 2)

            return carry

        lax.fori_loop(0, 8, step, 0)
        self.finish()

    def finish(self):
        for i in range(6):
            self.ici(i, self.r, 0, self.rx).wait_send()
        for i in range(8):
            self.pair(i, self.k, self.r, 0).wait_send()


def sum_scratch(width):
    return [
        pltpu.VMEM((4, PIECE, width), F32),
        pltpu.VMEM((8, PIECE, width), BF),
        pltpu.VMEM((8, PIECE, width), BF),
        pltpu.VMEM((6, PIECE, width), BF),
        pltpu.VMEM((6, PIECE, width), BF),
        DMA((8,)),
        DMA((8,)),
        DMA((6,)),
        DMA((6,)),
    ]


class Sum:
    def __init__(self, scratch):
        self.own, self.ds, self.dr, self.ist, self.irt = scratch[:5]
        self.dsend, self.drecv, self.isend, self.irecv = scratch[5:]
        self.r, self.k, self.rx, self.ry, self.r3 = place()

    def piece(self, j):
        mid = jnp.where(j == 2, self.ry, jnp.where(j == 5, self.ry, self.rx))
        row = jnp.where(j < 2, self.r3, jnp.where(j < 6, mid, self.r))
        return row, j % 2

    def pair(self, j):
        return remote(self.ds.at[j], self.dr.at[j], self.dsend.at[j], self.drecv.at[j], {"col": 1 - self.k})

    def ici(self, j):
        device = jnp.where(j == 0, self.ry, jnp.where(j == 2, self.ry, jnp.where(j == 5, self.ry, self.rx)))
        return remote(self.ist.at[j], self.irt.at[j], self.isend.at[j], self.irecv.at[j], {"row": device})

    def put(self, j, kept, given):
        self.own[j % 4] = kept
        self.ds[j] = given.astype(BF)
        self.pair(j).start()

    def chip(self, j):
        self.pair(j).wait_recv()
        return self.own[j % 4] + self.dr[j].astype(F32)

    def forward(self, j):
        self.ist[j] = self.chip(j).astype(BF)
        self.ici(j).start()

    def relay(self, j):
        value = self.chip(j)
        self.ici(j - 4).wait_recv()
        self.ist[j] = (value + self.irt[j - 4].astype(F32)).astype(BF)
        self.ici(j).start()

    def last(self, j):
        value = self.chip(j)
        self.ici(j - 4).wait_recv()
        value = value + self.irt[j - 4].astype(F32)
        self.ici(j - 2).wait_recv()
        return value + self.irt[j - 2].astype(F32)

    def send_all(self, compute):
        def step(j, carry):
            row, half = self.piece(j)
            kept, given = compute(row, half)
            self.put(j, kept, given)

            @pl.when(j > 0)
            def _():
                @pl.when(j < 5)
                def _():
                    self.forward(j - 1)

            return carry

        lax.fori_loop(0, 8, step, 0)

    def finish(self):
        for j in range(8):
            self.pair(j).wait_send()
        for j in range(6):
            self.ici(j).wait_send()


def call(kernel, cid, outs, ins, args, scratch, flops, vmem=44):
    moved = sum(int(np.prod(a.shape)) * a.dtype.itemsize for a in list(args) + list(outs))
    return pl.pallas_call(
        kernel,
        out_shape=outs,
        in_specs=ins,
        out_specs=[VM] * len(outs),
        scratch_shapes=scratch,
        compiler_params=pltpu.CompilerParams(
            collective_id=cid, has_side_effects=True, vmem_limit_bytes=vmem << 20
        ),
        cost_estimate=pl.CostEstimate(flops=int(flops), bytes_accessed=moved, transcendentals=0),
    )(*args)


def sds(shape, dtype):
    return jax.ShapeDtypeStruct(shape, dtype)


def head_index(iota):
    head, lane = iota // LANE, iota % LANE
    index = jnp.where(lane < HALF, lane, lane - (LANE // 2 - HALF))
    pad = lane % (LANE // 2) >= HALF
    return jnp.where(pad, -1, head * HD + index)


def spread(rows, cols, first):
    source = head_index(lax.broadcasted_iota(jnp.int32, (rows, cols), 1))
    at = lax.broadcasted_iota(jnp.int32, (rows, cols), 0)
    return jnp.where((source >= 0) & (at == source + first), 1.0, 0.0).astype(BF)


def spread_t(rows, cols, first):
    source = head_index(lax.broadcasted_iota(jnp.int32, (rows, cols), 0))
    at = lax.broadcasted_iota(jnp.int32, (rows, cols), 1)
    return jnp.where((source >= 0) & (at == source + first), 1.0, 0.0).astype(BF)


def angle_tables():
    lane = np.arange(LANE)
    freq = np.where(
        lane % (LANE // 2) < HALF, THETA ** (-2.0 * (lane % (LANE // 2)) / HD), 0.0
    )
    fine = np.arange(32)[:, None] * freq[None]
    coarse = fine * 32.0
    return [f(t).astype(np.float32) for t in (coarse, fine) for f in (np.cos, np.sin)]


def project_kernel(
    x, gain, wq, wk, wv, wo, wg, wu, wd, cc, sc, cf, sf,
    normed, qkv, kvt, wqkv_o, wo_o, wg_o, wu_o, wd_o, cos_o, sin_o, rstd_o,
    raw, gains, give_in, give_out, wsem, wrecv, csem, *sems,
):
    r, k, rx, ry, r3 = place()
    width = x.shape[1]
    f_half = wg.shape[1] // 2
    greet(rx, ry, k)
    gather = Gather(x, raw, sems)
    gather.start()
    mate = {"col": 1 - k}
    mine = pl.ds(pl.multiple_of(k * f_half, f_half), f_half)
    his = pl.ds(pl.multiple_of((1 - k) * f_half, f_half), f_half)
    keep = [
        pltpu.make_async_copy(gain, gains.at[k], csem.at[0]),
        pltpu.make_async_copy(wg.at[:, mine], wg_o.at[k], csem.at[1]),
        pltpu.make_async_copy(wu.at[:, mine], wu_o.at[k], csem.at[2]),
        pltpu.make_async_copy(wd.at[mine], wd_o.at[k], csem.at[3]),
    ]
    for c in keep:
        c.start()

    def give(n, src, dst):
        return remote(src, dst.at[k], wsem.at[n], wrecv.at[n], mate)

    gives = [give(0, gain, gains)]
    gives[0].start()
    heads_q = wq.shape[1] // 2
    heads_k = wk.shape[1] // 2
    nq = heads_q // HD * LANE
    nk = heads_k // HD * LANE
    for core, dst_in, dst_out in ((1 - k, give_in, give_out), (k, wqkv_o.at[k], wo_o.at[k])):
        sq = spread(2 * heads_q, nq, core * heads_q)
        sk = spread(2 * heads_k, nk, core * heads_k)
        dst_in[:, 0:nq] = nn(wq[...], sq).astype(BF)
        dst_in[:, nq : nq + nk] = nn(wk[...], sk).astype(BF)
        dst_in[:, nq + nk : nq + 2 * nk] = nn(wv[...], sk).astype(BF)
        dst_out[...] = nn(spread_t(nq, 2 * heads_q, core * heads_q), wo[...]).astype(BF)
    gives += [give(1, give_in, wqkv_o), give(2, give_out, wo_o)]
    gives += [give(3, wg.at[:, his], wg_o), give(4, wu.at[:, his], wu_o), give(5, wd.at[his], wd_o)]
    for g in gives[1:]:
        g.start()
    sign = jnp.where(lax.broadcasted_iota(jnp.int32, (32, LANE), 1) < LANE // 2, -1.0, 1.0)
    for a in range(LENGTH // 32):
        ca, sa = cc[a : a + 1, :], sc[a : a + 1, :]
        cos_o[a * 32 : a * 32 + 32, :] = ca * cf[...] - sa * sf[...]
        sin_o[a * 32 : a * 32 + 32, :] = (sa * cf[...] + ca * sf[...]) * sign
    for c in keep:
        c.wait()
    for n in range(3):
        gives[n].wait_recv()

    def compute(i, row, half):
        at = rows_of(half)
        x0 = raw[0, row, at, :].astype(F32)
        x1 = raw[1, row, at, :].astype(F32)
        total = jnp.sum(x0 * x0, 1, keepdims=True) + jnp.sum(x1 * x1, 1, keepdims=True)
        rstd = lax.rsqrt(total / (2 * width) + EPS)
        n0 = (x0 * rstd * gains[0]).astype(BF)
        n1 = (x1 * rstd * gains[1]).astype(BF)
        normed[0, row, at, :] = n0
        normed[1, row, at, :] = n1

        @pl.when(i < 2)
        def _():
            rstd_o[at, :] = jnp.broadcast_to(rstd, (PIECE, LANE))

        got = nn(n0, wqkv_o[0]) + nn(n1, wqkv_o[1])
        pos = pl.ds(pl.multiple_of((row % 2) * 2 * PIECE + half * PIECE, PIECE), PIECE)
        out = pl.ds(pl.multiple_of(row * 2 * PIECE + half * PIECE, PIECE), PIECE)
        cos, sin = cos_o[pos, :], sin_o[pos, :]
        for part in range(4):
            u = got[:, part * LANE : (part + 1) * LANE]
            if part < 3:
                u = u * cos + pltpu.roll(u, LANE // 2, 1) * sin
            qkv[part, out, :] = u.astype(BF)
            if part >= 2:
                kvt[part - 2, :, out] = u.T.astype(BF)

    gather.run(compute)
    for g in gives[3:]:
        g.wait_recv()
    for g in gives:
        g.wait_send()


def project(x, gain, wq, wk, wv, wo, wg, wu, wd):
    tokens, width = x.shape
    f_half = wg.shape[1] // 2
    cols = 4 * LANE
    tables = [jnp.asarray(t) for t in angle_tables()]
    outs = [
        sds((2, 4, tokens, width), BF),
        sds((4, 4 * tokens, LANE), BF),
        sds((2, LANE, 4 * tokens), BF),
        sds((2, width, cols), BF),
        sds((2, 2 * LANE, width), BF),
        sds((2, width, f_half), BF),
        sds((2, width, f_half), BF),
        sds((2, f_half, width), BF),
        sds((LENGTH, LANE), F32),
        sds((LENGTH, LANE), F32),
        sds((tokens, LANE), F32),
    ]
    scratch = [
        pltpu.VMEM((2, 4, tokens, width), BF),
        pltpu.VMEM((2, 1, width), F32),
        pltpu.VMEM((width, cols), BF),
        pltpu.VMEM((2 * LANE, width), BF),
        DMA((6,)),
        DMA((6,)),
        DMA((4,)),
    ] + GATHER_SEMS
    ins = [ANY, VM, VM, VM, VM, VM, ANY, ANY, ANY] + [VM] * 4
    args = [x, gain, wq, wk, wv, wo, wg, wu, wd] + tables
    return call(project_kernel, 0, outs, ins, args, scratch, 3e10)


def exchange(k, stat, sems):
    copy = remote(stat.at[k], stat.at[k], sems.at[0], sems.at[1], {"col": 1 - k})
    copy.start()
    remote(stat.at[1 - k], stat.at[1 - k], sems.at[0], sems.at[1], {"col": 1 - k}).wait_recv()
    copy.wait_send()
    return stat[0][:, 0:1] + stat[1][:, 0:1]


def causal(shape):
    return lax.broadcasted_iota(jnp.int32, shape, 0) <= lax.broadcasted_iota(jnp.int32, shape, 1)


def attend_kernel(
    qkv, kvt, wo, x, gain, dy,
    attn, lse, hidden, normed, rstd_o, all_dy,
    stat, ssem, *rest,
):
    r, k, rx, ry, r3 = place()
    width = x.shape[1]
    greet(rx, ry, k)
    total = Sum(rest[:9])
    gather = Gather(dy, all_dy, rest[9:])
    gather.start()

    def compute(row, half):
        base = pl.multiple_of(row // 2 * LENGTH, LENGTH)
        at = rows_of(half)
        qrow = pl.ds(pl.multiple_of(row * 2 * PIECE + half * PIECE, PIECE), PIECE)
        order = (row % 2) * 2 + half

        def attend(p):
            span = PIECE * (p + 1)
            for head in range(2):
                keys = qkv[2, pl.ds(base, span), :]
                s = nt(keys, qkv[head, qrow, :])
                tail = jnp.where(causal((PIECE, PIECE)), s[span - PIECE :], -1e30)
                s = tail if p == 0 else jnp.concatenate([s[: span - PIECE], tail], 0)
                top = jnp.max(s, 0, keepdims=True)
                e = jnp.exp((s - top) * SCALE)
                weight = jnp.sum(e, 0, keepdims=True)
                probs = (e * (1.0 / weight)).astype(BF)
                mixed = nn(kvt[1, :, pl.ds(base, span)], probs)
                attn[row, at, head * LANE : (head + 1) * LANE] = mixed.T.astype(BF)
                lse[head, row * 2 + half] = top * SCALE + jnp.log(weight)

        for p in range(4):
            pl.when(order == p)(lambda p=p: attend(p))
        a = attn[row, at, :]
        return nn(a, wo[k]), nn(a, wo[1 - k])

    total.send_all(compute)
    total.relay(4)
    total.relay(5)
    gather.arrive(2)
    gather.arrive(3)
    for half in range(2):
        at = rows_of(half)
        h = x[at, :].astype(F32) + total.last(6 + half)
        hidden[at, :] = h
        stat[k, at, :] = jnp.broadcast_to(jnp.sum(h * h, 1, keepdims=True), (PIECE, LANE))
    rstd = lax.rsqrt(exchange(k, stat, ssem) / (2 * width) + EPS)
    rstd_o[...] = jnp.broadcast_to(rstd, rstd_o.shape)
    normed[...] = (hidden[...] * rstd * gain[...]).astype(BF)
    for i in range(4, 8):
        gather.arrive(i)
    for i in range(8):
        gather.ready(i)
    gather.local.wait()
    gather.finish()
    total.finish()


def attend(qkv, kvt, wo, x, gain, dy):
    tokens, width = x.shape
    outs = [
        sds((4, tokens, 2 * LANE), BF),
        sds((2, 8, 1, PIECE), F32),
        sds((tokens, width), F32),
        sds((tokens, width), BF),
        sds((tokens, LANE), F32),
        sds((2, 4, tokens, width), BF),
    ]
    scratch = [pltpu.VMEM((2, tokens, LANE), F32), DMA((2,))] + sum_scratch(width) + GATHER_SEMS
    return call(
        attend_kernel, 1, outs, [VM] * 5 + [ANY], [qkv, kvt, wo, x, gain, dy], scratch, 3e10
    )


def expand_kernel(nf, all_dy, wg, wu, wd, all_f, middle, d_gate, d_up, *sems):
    r, k, rx, ry, r3 = place()
    greet(rx, ry, k)
    gather = Gather(nf, all_f, sems)
    gather.start()

    def compute(i, row, half):
        at = rows_of(half)
        f0, f1 = all_f[0, row, at, :], all_f[1, row, at, :]
        gate = nn(f0, wg[0]) + nn(f1, wg[1])
        upper = nn(f0, wu[0]) + nn(f1, wu[1])
        d_mid = nt(all_dy[0, row, at, :], wd[0]) + nt(all_dy[1, row, at, :], wd[1])
        sig = 1.0 / (1.0 + jnp.exp(-gate))
        swish = gate * sig
        middle[row, at, :] = (swish * upper).astype(BF)
        d_gate[row, at, :] = (d_mid * upper * sig * (1.0 + gate * (1.0 - sig))).astype(BF)
        d_up[row, at, :] = (d_mid * swish).astype(BF)

    gather.run(compute)


def expand(nf, all_dy, wg, wu, wd):
    tokens, width = nf.shape
    f_half = wg.shape[2]
    outs = [sds((2, 4, tokens, width), BF)] + [sds((4, tokens, f_half), BF)] * 3
    return call(
        expand_kernel, 2, outs, [ANY] + [VM] * 4, [nf, all_dy, wg, wu, wd], list(GATHER_SEMS), 3e10
    )


def contract_kernel(
    d_gate, d_up, wg, wu, hidden, rstd2, gain, dy,
    d_hidden, dya, part,
    stat, ssem, *rest,
):
    r, k, rx, ry, r3 = place()
    width = hidden.shape[1]
    greet(rx, ry, k)
    total = Sum(rest)

    def compute(row, half):
        at = rows_of(half)
        g, u = d_gate[row, at, :], d_up[row, at, :]
        return nt(g, wg[k]) + nt(u, wu[k]), nt(g, wg[1 - k]) + nt(u, wu[1 - k])

    total.send_all(compute)
    total.relay(4)
    total.relay(5)
    gains = jnp.zeros((1, width), F32)
    for half in range(2):
        at = rows_of(half)
        d_nf = total.last(6 + half)
        h = hidden[at, :]
        gains = gains + jnp.sum(d_nf * h * rstd2[at, 0:1], 0, keepdims=True)
        scaled = d_nf * gain[...]
        d_hidden[at, :] = scaled
        stat[k, at, :] = jnp.broadcast_to(jnp.sum(scaled * h, 1, keepdims=True), (PIECE, LANE))
    part[...] = gains
    inner = exchange(k, stat, ssem) / (2 * width)
    rs = rstd2[:, 0:1]
    value = dy[...].astype(F32) + rs * d_hidden[...] - hidden[...] * (rs * rs * rs * inner)
    d_hidden[...] = value
    dya[...] = value.astype(BF)
    total.finish()


def contract(d_gate, d_up, wg, wu, hidden, rstd2, gain, dy):
    tokens, width = hidden.shape
    outs = [sds((tokens, width), F32), sds((tokens, width), BF), sds((1, width), F32)]
    scratch = [pltpu.VMEM((2, tokens, LANE), F32), DMA((2,))] + sum_scratch(width)
    args = [d_gate, d_up, wg, wu, hidden, rstd2, gain, dy]
    return call(contract_kernel, 3, outs, [VM] * 8, args, scratch, 3e10)


def unproject_kernel(dya, wo, all_dya, d_attn, *sems):
    r, k, rx, ry, r3 = place()
    greet(rx, ry, k)
    gather = Gather(dya, all_dya, sems)
    gather.start()

    def compute(i, row, half):
        at = rows_of(half)
        got = nt(all_dya[0, row, at, :], wo[0]) + nt(all_dya[1, row, at, :], wo[1])
        d_attn[row, at, :] = got.astype(BF)

    gather.run(compute)


def unproject(dya, wo):
    tokens, width = dya.shape
    outs = [sds((2, 4, tokens, width), BF), sds((4, tokens, 2 * LANE), BF)]
    return call(unproject_kernel, 4, outs, [ANY, VM], [dya, wo], list(GATHER_SEMS), 3e10)


def backward_kernel(
    qkv, kvt, lse, d_attn, cos, sin, wqkv, middle, wd, hidden, x, rstd1, d_hidden, gain,
    d_proj, output, grad_x, part,
    dk, dv, stat, ssem, *rest,
):
    r, k, rx, ry, r3 = place()
    width = x.shape[1]
    greet(rx, ry, k)
    down = Sum(rest[:9])
    into = Sum(rest[9:])

    def down_piece(row, half):
        m = middle[row, rows_of(half), :]
        return nn(m, wd[k]), nn(m, wd[1 - k])

    down.send_all(down_piece)

    def unrotate(u, p):
        at = pl.ds(p * PIECE, PIECE)
        return u * cos[at, :] - pltpu.roll(u, LANE // 2, 1) * sin[at, :]

    def sequence(seq):
        base = pl.multiple_of(seq * LENGTH, LENGTH)

        def one_head(head, carry):
            for p in range(4):
                span = PIECE * (p + 1)
                row = seq * 2 + p // 2
                at = pl.ds((p % 2) * PIECE, PIECE)
                out = pl.ds(pl.multiple_of(base + p * PIECE, PIECE), PIECE)
                keys = qkv[2, pl.ds(base, span), :]
                q = qkv[head, out, :]
                lane = pl.ds(pl.multiple_of(head * LANE, LANE), LANE)
                do = d_attn[row, at, lane]
                e = jnp.exp(nt(keys, q) * SCALE - lse[head, seq * 4 + p])
                tail = jnp.where(causal((PIECE, PIECE)), e[span - PIECE :], 0.0)
                e = tail if p == 0 else jnp.concatenate([e[: span - PIECE], tail], 0)
                dp = nt(qkv[3, pl.ds(base, span), :], do)
                inner = jnp.sum(e * dp, 0, keepdims=True)
                ds = (e * (dp - inner)).astype(BF)
                dv[0:span, :] += nn(e.astype(BF), do)
                dk[0:span, :] += nn(ds, q)
                dq = nn(kvt[0, :, pl.ds(base, span)], ds).T * SCALE
                d_proj[out, lane] = unrotate(dq, p).astype(BF)
            return carry

        dk[...] = jnp.zeros_like(dk)
        dv[...] = jnp.zeros_like(dv)
        lax.fori_loop(0, 2, one_head, 0)
        for p in range(4):
            at = pl.ds(p * PIECE, PIECE)
            out = pl.ds(pl.multiple_of(base + p * PIECE, PIECE), PIECE)
            d_proj[out, 2 * LANE : 3 * LANE] = unrotate(dk[at, :] * SCALE, p).astype(BF)
            d_proj[out, 3 * LANE : 4 * LANE] = dv[at, :].astype(BF)

    def both(n, carry):
        sequence(jnp.where(n == 0, ry // 2, r // 2))

        @pl.when(n == 0)
        def _():
            down.relay(4)
            down.relay(5)

        return carry

    lax.fori_loop(0, 2, both, 0)

    def into_piece(row, half):
        d = d_proj[pl.ds(pl.multiple_of(row * 2 * PIECE + half * PIECE, PIECE), PIECE), :]
        return nt(d, wqkv[k]), nt(d, wqkv[1 - k])

    into.send_all(into_piece)
    for half in range(2):
        at = rows_of(half)
        output[at, :] = hidden[at, :] + down.last(6 + half)
    into.relay(4)
    into.relay(5)
    gains = jnp.zeros((1, width), F32)
    for half in range(2):
        at = rows_of(half)
        d_na = into.last(6 + half)
        xs = x[at, :].astype(F32)
        gains = gains + jnp.sum(d_na * xs * rstd1[at, 0:1], 0, keepdims=True)
        scaled = d_na * gain[...]
        grad_x[at, :] = scaled
        stat[k, at, :] = jnp.broadcast_to(jnp.sum(scaled * xs, 1, keepdims=True), (PIECE, LANE))
    part[...] = gains
    inner = exchange(k, stat, ssem) / (2 * width)
    rs = rstd1[:, 0:1]
    grad_x[...] = d_hidden[...] + rs * grad_x[...] - x[...].astype(F32) * (rs * rs * rs * inner)
    down.finish()
    into.finish()


def backward(qkv, kvt, lse, d_attn, cos, sin, wqkv, middle, wd, hidden, x, rstd1, d_hidden, gain):
    tokens, width = x.shape
    outs = [
        sds((4 * tokens, 4 * LANE), BF),
        sds((tokens, width), F32),
        sds((tokens, width), F32),
        sds((1, width), F32),
    ]
    scratch = (
        [pltpu.VMEM((LENGTH, LANE), F32)] * 2
        + [pltpu.VMEM((2, tokens, LANE), F32), DMA((2,))]
        + sum_scratch(width)
        + sum_scratch(width)
    )
    args = [qkv, kvt, lse, d_attn, cos, sin, wqkv, middle, wd, hidden, x, rstd1, d_hidden, gain]
    return call(backward_kernel, 5, outs, [VM] * len(args), args, scratch, 5e10)


def gains_kernel(groups, a, f, out, slots, send, recv):
    dp, r = lax.axis_index("dp"), lax.axis_index("row")
    me = dp * 4 + r

    def peer(t):
        other = (me + t) % groups
        return other, {"dp": other // 4, "row": other % 4}

    bar = pltpu.get_barrier_semaphore()

    def hello(t, carry):
        pl.semaphore_signal(bar, inc=1, device_id=peer(t)[1], device_id_type=MESH)
        return carry

    lax.fori_loop(1, groups, hello, 0)
    slots[me, 0:1, :] = a[...]
    slots[me, 1:2, :] = f[...]
    pl.semaphore_wait(bar, groups - 1)

    def start(t, carry):
        remote(slots.at[me], slots.at[me], send.at[t], recv.at[me], peer(t)[1]).start()
        return carry

    lax.fori_loop(1, groups, start, 0)

    def wait(t, carry):
        other, device = peer(t)
        remote(slots.at[me], slots.at[other], send.at[t], recv.at[other], device).wait_recv()
        remote(slots.at[me], slots.at[me], send.at[t], recv.at[me], device).wait_send()
        return carry

    lax.fori_loop(1, groups, wait, 0)
    out[...] = lax.fori_loop(1, groups, lambda g, total: total + slots[g], slots[0])


def gains_total(a, f, groups):
    import functools

    outs = [sds((2, a.shape[1]), F32)]
    scratch = [pltpu.VMEM((groups, 2, a.shape[1]), F32), DMA((groups,)), DMA((groups,))]
    return call(
        functools.partial(gains_kernel, groups), 6, outs, [VM] * 2, [a, f], scratch, 1e6, vmem=8
    )[0]


def dp_total(part):
    n = lax.axis_size("dp")
    z = lax.axis_index("dp")
    mid = n // 2

    def add(a, b):
        return (a.astype(F32) + b.astype(F32)).astype(BF)

    for s in range(mid - 1):
        part = add(part, lax.ppermute(part, "dp", [(s, s + 1), (n - 1 - s, n - 2 - s)]))
    part = add(part, lax.ppermute(part, "dp", [(mid - 1, mid), (mid, mid - 1)]))
    for s in reversed(range(mid - 1)):
        got = lax.ppermute(part, "dp", [(s + 1, s), (n - 2 - s, n - 1 - s)])
        part = jnp.where((z == s) | (z == n - 1 - s), got, part)
    return part


def swap(both, k):
    mine = lax.dynamic_index_in_dim(both, k, 0, False)
    his = lax.dynamic_index_in_dim(both, 1 - k, 0, False)
    return mine, lax.ppermute(his, "col", [(0, 1), (1, 0)])


def weight_grad(left, right):
    return lax.dot_general(left, right, (((0,), (0,)), ((), ())), preferred_element_type=F32).astype(BF)


def side_by_side(mine, his, k, axis):
    first = jnp.where(k == 0, mine, his)
    second = jnp.where(k == 0, his, mine)
    return jnp.concatenate([first, second], axis)


def on_device(
    layer_input, gain_attn, gain_ffn, w_query, w_key, w_value, w_out, w_gate, w_up, w_down, cotangent
):
    k = lax.axis_index("col")
    tokens, width = layer_input.shape
    q_cols, k_cols = w_query.shape[1], w_key.shape[1]
    gain_a, gain_f = gain_attn[None], gain_ffn[None]
    normed, qkv, kvt, wqkv, wo, wg, wu, wd, cos, sin, rstd1 = project(
        layer_input, gain_a, w_query, w_key, w_value, w_out, w_gate, w_up, w_down
    )
    attn, lse, hidden, nf, rstd2, all_dy = attend(qkv, kvt, wo, layer_input, gain_f, cotangent)
    all_f, middle, d_gate, d_up = expand(nf, all_dy, wg, wu, wd)

    def flat(a):
        return a.reshape(4 * tokens, a.shape[-1])

    def grads_of(gathered, right):
        return jnp.stack([weight_grad(flat(gathered[h]), flat(right)) for h in range(2)])

    mid = flat(middle)
    g_down = jnp.stack([weight_grad(mid, flat(all_dy[h])) for h in range(2)])
    down = dp_total(side_by_side(*swap(g_down, k), k, 0))
    gate = dp_total(side_by_side(*swap(grads_of(all_f, d_gate), k), k, 1))
    up = dp_total(side_by_side(*swap(grads_of(all_f, d_up), k), k, 1))

    d_hidden, dya, part_f = contract(d_gate, d_up, wg, wu, hidden, rstd2, gain_f, cotangent)
    all_dya, d_attn = unproject(dya, wo)
    g_out = jnp.stack([weight_grad(flat(attn), flat(all_dya[h])) for h in range(2)])
    d_proj, output, grad_x, part_a = backward(
        qkv, kvt, lse, d_attn, cos, sin, wqkv, middle, wd, hidden, layer_input, rstd1, d_hidden, gain_a
    )
    gains = gains_total(part_a, part_f, lax.axis_size("dp") * 4)

    mine, his = swap(g_out, k)
    n = 2 * LANE
    out = nn(spread(q_cols, n, k * q_cols // 2), mine) + nn(
        spread(q_cols, n, (1 - k) * q_cols // 2), his
    )
    mine, his = swap(grads_of(normed, d_proj), k)

    def columns(core):
        part = [
            jnp.pad(spread_t(n, q_cols, core * q_cols // 2), ((0, 0), (0, 2 * k_cols))),
            jnp.pad(spread_t(LANE, k_cols, core * k_cols // 2), ((0, 0), (q_cols, k_cols))),
            jnp.pad(spread_t(LANE, k_cols, core * k_cols // 2), ((0, 0), (q_cols + k_cols, 0))),
        ]
        return jnp.concatenate(part, 0)

    into = nn(mine, columns(k)) + nn(his, columns(1 - k))
    last = dp_total(jnp.concatenate([out.astype(BF), into.astype(BF)], 0))
    out, into = last[:q_cols].astype(F32), last[q_cols:].astype(F32)
    return (
        output,
        grad_x,
        gains[0],
        gains[1],
        into[:, :q_cols],
        into[:, q_cols : q_cols + k_cols],
        into[:, q_cols + k_cols :],
        out,
        gate.astype(F32),
        up.astype(F32),
        down.astype(F32),
    )


def solution(mesh):
    assert mesh.shape["row"] == 4 and mesh.shape["col"] == 2
    tokens = P(("dp", "row"), "col")
    wide = P("col", "row")
    tall = P("row", "col")
    return jax.shard_map(
        on_device,
        mesh=mesh,
        in_specs=(tokens, P("col"), P("col"), wide, wide, wide, tall, wide, wide, tall, tokens),
        out_specs=(tokens, tokens, P("col"), P("col"), wide, wide, wide, tall, wide, wide, tall),
        check_vma=False,
    )
```

```python
import functools

import jax
import jax.numpy as jnp
import numpy as np
from jax import lax
from jax.experimental import pallas as pl
from jax.experimental.pallas import tpu as pltpu
from jax.sharding import PartitionSpec as P

HD = 96
HALF = HD // 2
LENGTH = 1024
EPS = 1e-05
THETA = 100000.0
SCALE = HD ** (-0.5)
LANE = 128
PIECE = 256

BF = jnp.bfloat16
F32 = jnp.float32
MESH = pl.DeviceIdType.MESH
VM = pl.BlockSpec(memory_space=pltpu.VMEM)
ANY = pl.BlockSpec(memory_space=pl.ANY)
DMA = pltpu.SemaphoreType.DMA


def nn(a, b):
    return lax.dot_general(a, b, (((1,), (0,)), ((), ())), preferred_element_type=F32)


def nt(a, b):
    return lax.dot_general(a, b, (((1,), (1,)), ((), ())), preferred_element_type=F32)


def place():
    r = lax.axis_index("row")
    k = lax.axis_index("col")
    return r, k, r + 1 - 2 * (r % 2), (r + 2) % 4, 3 - r


def tn(a, b):
    return lax.dot_general(a, b, (((0,), (0,)), ((), ())), preferred_element_type=F32)


def line_place():
    n = lax.axis_size("dp")
    z = lax.axis_index("dp")
    left = z < n // 2
    step = jnp.where(left, 1, -1)
    return n, jnp.where(left, z, n - 1 - z), z + step, z - step


def greet(rx, ry, k, line=False, groups=False):
    bar = pltpu.get_barrier_semaphore()

    def hello(device):
        pl.semaphore_signal(bar, inc=1, device_id=device, device_id_type=MESH)

    for device in ({"row": rx}, {"row": ry}, {"col": 1 - k}):
        hello(device)
    if not line:
        pl.semaphore_wait(bar, 3)
        return
    n, s, inward, outward = line_place()
    if groups:
        z = lax.axis_index("dp")

        def one(t, carry):
            hello({"dp": (z + t) % n})
            return carry

        lax.fori_loop(1, n, one, 0)
        pl.semaphore_wait(bar, 3 + n - 1)
        return
    hello({"dp": inward})

    @pl.when(s > 0)
    def _():
        hello({"dp": outward})

    pl.semaphore_wait(bar, jnp.where(s > 0, 5, 4))


def remote(src, dst, send, recv, device):
    return pltpu.make_async_remote_copy(
        src_ref=src, dst_ref=dst, send_sem=send, recv_sem=recv, device_id=device, device_id_type=MESH
    )


def rows_of(half):
    return pl.ds(pl.multiple_of(half * PIECE, PIECE), PIECE)


GATHER_SEMS = [DMA((6,)), DMA((6,)), DMA((8,)), DMA((8,)), DMA]


class Gather:
    def __init__(self, own, buf, sems):
        self.own, self.buf = own, buf
        self.isend, self.irecv, self.dsend, self.drecv, self.lsem = sems
        self.r, self.k, self.rx, self.ry, self.r3 = place()

    def piece(self, i):
        side = jnp.where(i % 2 == 0, self.rx, self.ry)
        row = jnp.where(i < 2, self.r, jnp.where(i < 6, side, self.r3))
        half = jnp.where(i // 2 == 2, 1 - i % 2, i % 2)
        return row, half

    def ici(self, sem, row, half, device, src=None):
        dst = self.buf.at[self.k, row, rows_of(half)]
        return remote(dst if src is None else src, dst, self.isend.at[sem], self.irecv.at[sem], {"row": device})

    def pair(self, i, core, row, half, src=None):
        dst = self.buf.at[core, row, rows_of(half)]
        return remote(dst if src is None else src, dst, self.dsend.at[i], self.drecv.at[i], {"col": 1 - self.k})

    def start(self):
        first, second = self.own.at[pl.ds(0, PIECE)], self.own.at[pl.ds(PIECE, PIECE)]
        self.ici(0, self.r, 0, self.rx, first).start()
        self.ici(1, self.r, 1, self.ry, second).start()
        self.ici(2, self.r, 1, self.rx, second).start()
        self.ici(3, self.r, 0, self.ry, first).start()
        self.pair(0, self.k, self.r, 0, first).start()
        self.pair(1, self.k, self.r, 1, second).start()
        self.local = pltpu.make_async_copy(self.own, self.buf.at[self.k, self.r], self.lsem)
        self.local.start()

    def arrive(self, i):
        row, half = self.piece(i)
        self.ici(i - 2, row, half, self.rx).wait_recv()

        @pl.when(i == 2)
        def _():
            self.ici(4, row, half, self.ry).start()

        @pl.when(i == 3)
        def _():
            self.ici(5, row, half, self.rx).start()

        self.pair(i, self.k, row, half).start()

    def ready(self, i):
        row, half = self.piece(i)
        self.pair(i, 1 - self.k, row, half).wait_recv()

    def run(self, compute, before=None, after=None):
        self.local.wait()

        def pair(q, carry):
            for u in range(2):
                i = 2 * q + u
                self.ready(i)
                row, half = self.piece(i)
                compute(i, row, half)
            if before is not None:
                before(q)

            @pl.when(q < 3)
            def _():
                self.arrive(2 * q + 2)
                self.arrive(2 * q + 3)

            if after is not None:
                after(q)
            return carry

        lax.fori_loop(0, 4, pair, 0)
        self.finish()

    def finish(self):
        for i in range(6):
            self.ici(i, self.r, 0, self.rx).wait_send()
        for i in range(8):
            self.pair(i, self.k, self.r, 0).wait_send()


def sum_scratch(width):
    return [
        pltpu.VMEM((4, PIECE, width), F32),
        pltpu.VMEM((4, PIECE, width), BF),
        pltpu.VMEM((8, PIECE, width), BF),
        pltpu.VMEM((6, PIECE, width), BF),
        pltpu.VMEM((6, PIECE, width), BF),
        DMA((8,)),
        DMA((8,)),
        DMA((6,)),
        DMA((6,)),
    ]


class Sum:
    def __init__(self, scratch):
        self.own, self.ds, self.dr, self.ist, self.irt = scratch[:5]
        self.dsend, self.drecv, self.isend, self.irecv = scratch[5:]
        self.r, self.k, self.rx, self.ry, self.r3 = place()

    def piece(self, j):
        mid = jnp.where(j == 2, self.ry, jnp.where(j == 5, self.ry, self.rx))
        row = jnp.where(j < 2, self.r3, jnp.where(j < 6, mid, self.r))
        return row, j % 2

    def pair(self, j):
        return remote(self.ds.at[j % 4], self.dr.at[j], self.dsend.at[j], self.drecv.at[j], {"col": 1 - self.k})

    def ici(self, j):
        device = jnp.where(j == 0, self.ry, jnp.where(j == 2, self.ry, jnp.where(j == 5, self.ry, self.rx)))
        return remote(self.ist.at[j], self.irt.at[j], self.isend.at[j], self.irecv.at[j], {"row": device})

    def put(self, j, kept, given):
        @pl.when(j >= 4)
        def _():
            self.pair(j - 4).wait_send()

        self.own[j % 4] = kept
        self.ds[j % 4] = given.astype(BF)
        self.pair(j).start()

    def chip(self, j):
        self.pair(j).wait_recv()
        return self.own[j % 4] + self.dr[j].astype(F32)

    def forward(self, j):
        self.ist[j] = self.chip(j).astype(BF)
        self.ici(j).start()

    def relay(self, j):
        value = self.chip(j)
        self.ici(j - 4).wait_recv()
        self.ist[j] = (value + self.irt[j - 4].astype(F32)).astype(BF)
        self.ici(j).start()

    def last(self, j):
        value = self.chip(j)
        self.ici(j - 4).wait_recv()
        value = value + self.irt[j - 4].astype(F32)
        self.ici(j - 2).wait_recv()
        return value + self.irt[j - 2].astype(F32)

    def send_all(self, compute, hook=None):
        def step(j, carry):
            row, half = self.piece(j)
            kept, given = compute(row, half)
            self.put(j, kept, given)

            @pl.when(j > 0)
            def _():
                @pl.when(j < 5)
                def _():
                    self.forward(j - 1)

            if hook is not None:
                hook(j)
            return carry

        lax.fori_loop(0, 8, step, 0)

    def finish(self):
        for j in range(4, 8):
            self.pair(j).wait_send()
        for j in range(6):
            self.ici(j).wait_send()


TALL, WIDE = 128, 768
CHUNK = TALL // 2
DOWN_CHUNKS, MLP_CHUNKS, OUT_CHUNKS, ALL_CHUNKS = 16, 48, 54, 66
RING = 6
LAG = 2


def line_ring(n):
    return LAG * (2 * (n // 2) - 2) + 6


def line_ticks(n):
    return ALL_CHUNKS + LAG * (2 * (n // 2) - 2)


def line_outs(ticks):
    return [sds((ticks, CHUNK, WIDE), BF)] + [sds((LAG, CHUNK, WIDE), BF)] * 2


def line_scratch(n, ticks):
    slots = (RING, line_ring(n), line_ring(n), RING)
    return [pltpu.VMEM((count, CHUNK, WIDE), BF) for count in slots] + [DMA((ticks,))] * 6


class Line:
    def __init__(self, parts, totals, carry, scratch, first, ticks, before=None):
        self.parts, self.totals, self.carry = parts, totals, carry
        self.acc, self.tot, self.rin, self.rxb = scratch[:4]
        self.si, self.ri, self.rx, self.so, self.ro, self.out_sem = scratch[4:]
        self.first, self.ticks = first, ticks
        self.n, self.s, self.inward, self.outward = line_place()
        self.mid = self.n // 2
        self.ring = line_ring(self.n)
        if before is not None:

            @pl.when(self.s > 0)
            def _():
                for b in range(LAG):
                    self.acc[b] = before[0][b]
                    self.tot[b] = before[1][b]

    def valid(self, c):
        return (c >= 0) & (c < ALL_CHUNKS)

    def sends(self, j):
        s, mid, slot, near = self.s, self.mid, j % self.ring, j % RING
        to = {"dp": self.inward}
        c = self.first + j - LAG * s
        moves = []
        inward = (self.rin.at[slot], self.ri.at[j])
        across = (self.rxb.at[near], self.rx.at[j])
        for lo, hi, ref in self.parts:
            ok = (s == 0) & (c >= lo) & (c < hi)
            moves.append((ok, ref, c - lo, across if mid == 1 else inward))
        if mid > 1:
            ok = self.valid(c)
            moves.append((ok & (s == mid - 1), self.acc, near, across))
            if mid > 2:
                moves.append((ok & (s > 0) & (s < mid - 1), self.acc, near, inward))
        out = [
            (cond, lambda ref=ref, at=at, way=way: remote(ref.at[at], way[0], self.si.at[j], way[1], to))
            for cond, ref, at, way in moves
        ]
        if mid > 1:
            c = self.first + j - LAG * (2 * mid - 1 - s)
            out.append(((s > 0) & self.valid(c), lambda: self.outer(j)))
        return out

    def outer(self, j):
        return remote(
            self.tot.at[j % self.ring], self.tot.at[(j + LAG) % self.ring],
            self.so.at[j], self.ro.at[j], {"dp": self.outward},
        )

    def begin(self, j):
        for cond, copy in self.sends(j):

            @pl.when(cond)
            def _(copy=copy):
                copy().start()

    def total_of(self, j):
        copy = lambda: pltpu.make_async_copy(
            self.tot.at[(j + LAG) % self.ring], self.totals.at[j], self.out_sem.at[j]
        )
        return self.valid(self.first + j - LAG * (2 * self.mid - 2 - self.s)), copy

    def settle(self, j):
        for cond, copy in self.sends(j):

            @pl.when(cond)
            def _(copy=copy):
                copy().wait_send()

        cond, copy = self.total_of(j)

        @pl.when(cond)
        def _():
            copy().wait()

    def end(self, j):
        t, s, mid = self.first + j, self.s, self.mid
        slot, later = j % self.ring, (j + LAG) % self.ring
        near, next_near = j % RING, (j + LAG) % RING

        @pl.when(j >= 2)
        def _():
            self.settle(j - 2)

        def came(buf, at, sem):
            remote(buf.at[at], buf.at[at], self.si.at[j], sem.at[j], {"dp": self.inward}).wait_recv()

        def add_part(c, buf, at, dst, to):
            for lo, hi, ref in self.parts:

                @pl.when((c >= lo) & (c < hi))
                def _(ref=ref, lo=lo):
                    dst[to] = (ref[c - lo].astype(F32) + buf[at].astype(F32)).astype(BF)

        if mid > 1:
            c = t - LAG * (s - 1)

            @pl.when((s > 0) & self.valid(c))
            def _():
                came(self.rin, slot, self.ri)
                add_part(c, self.rin, slot, self.acc, next_near)

        @pl.when((s == mid - 1) & self.valid(t - LAG * (mid - 1)))
        def _():
            came(self.rxb, near, self.rx)
            if mid > 1:
                self.tot[later] = (self.acc[near].astype(F32) + self.rxb[near].astype(F32)).astype(BF)
            else:
                add_part(t, self.rxb, near, self.tot, later)

        cond, copy = self.total_of(j)
        if mid > 1:

            @pl.when((s < mid - 1) & cond)
            def _():
                self.outer(j).wait_recv()

        @pl.when(cond)
        def _():
            copy().start()

    def open(self):
        for j in range(min(LAG, self.ticks)):
            self.begin(j)

    def step(self, j):
        self.end(j)

        @pl.when(j + LAG < self.ticks)
        def _():
            self.begin(j + LAG)

    def rest(self, j):
        def one(t, carry):
            self.step(t)
            return carry

        lax.fori_loop(j, self.ticks, one, 0)
        for t in range(max(self.ticks - 2, 0), self.ticks):
            self.settle(t)
        if self.carry is not None:
            for b in range(LAG):
                self.carry[0][b] = self.acc[(self.ticks + b) % RING]
                self.carry[1][b] = self.tot[(self.ticks + b) % self.ring]


def call(kernel, cid, outs, ins, args, scratch, flops, vmem=44, out_specs=None):
    moved = sum(int(np.prod(a.shape)) * a.dtype.itemsize for a in list(args) + list(outs))
    return pl.pallas_call(
        kernel,
        out_shape=outs,
        in_specs=ins,
        out_specs=out_specs or [VM] * len(outs),
        scratch_shapes=scratch,
        compiler_params=pltpu.CompilerParams(
            collective_id=cid, has_side_effects=True, vmem_limit_bytes=vmem << 20
        ),
        cost_estimate=pl.CostEstimate(flops=int(flops), bytes_accessed=moved, transcendentals=0),
    )(*args)


def sds(shape, dtype):
    return jax.ShapeDtypeStruct(shape, dtype)


def head_index(iota):
    head, lane = iota // LANE, iota % LANE
    index = jnp.where(lane < HALF, lane, lane - (LANE // 2 - HALF))
    pad = lane % (LANE // 2) >= HALF
    return jnp.where(pad, -1, head * HD + index)


def spread(rows, cols, first):
    source = head_index(lax.broadcasted_iota(jnp.int32, (rows, cols), 1))
    at = lax.broadcasted_iota(jnp.int32, (rows, cols), 0)
    return jnp.where((source >= 0) & (at == source + first), 1.0, 0.0).astype(BF)


def spread_t(rows, cols, first):
    source = head_index(lax.broadcasted_iota(jnp.int32, (rows, cols), 0))
    at = lax.broadcasted_iota(jnp.int32, (rows, cols), 1)
    return jnp.where((source >= 0) & (at == source + first), 1.0, 0.0).astype(BF)


def angle_tables():
    lane = np.arange(LANE)
    freq = np.where(
        lane % (LANE // 2) < HALF, THETA ** (-2.0 * (lane % (LANE // 2)) / HD), 0.0
    )
    fine = np.arange(32)[:, None] * freq[None]
    coarse = fine * 32.0
    return [f(t).astype(np.float32) for t in (coarse, fine) for f in (np.cos, np.sin)]


def project_kernel(
    x, gain, wq_h, wk_h, wv_h, wo_h, wg, wu, wd, tables,
    normed, qkv, kvt, wqkv_o, wo_o, wg_o, wu_o, wd_o, cos_o, sin_o, rstd_o,
    raw, gains, give_in, give_out, wq, wk, wv, wo, wsem, wrecv, csem, *sems,
):
    r, k, rx, ry, r3 = place()
    width = x.shape[1]
    f_half = wg.shape[1] // 2
    greet(rx, ry, k)
    gather = Gather(x, raw, sems)
    gather.start()
    mate = {"col": 1 - k}
    mine = pl.ds(pl.multiple_of(k * f_half, f_half), f_half)
    his = pl.ds(pl.multiple_of((1 - k) * f_half, f_half), f_half)
    keep = [
        pltpu.make_async_copy(gain, gains.at[k], csem.at[0]),
        pltpu.make_async_copy(wg.at[:, mine], wg_o.at[k], csem.at[1]),
        pltpu.make_async_copy(wu.at[:, mine], wu_o.at[k], csem.at[2]),
        pltpu.make_async_copy(wd.at[mine], wd_o.at[k], csem.at[3]),
    ]
    first = [
        pltpu.make_async_copy(src, dst, csem.at[4 + n])
        for n, (src, dst) in enumerate(((wq_h, wq), (wk_h, wk), (wv_h, wv), (wo_h, wo)))
    ]
    for c in first + keep:
        c.start()

    def give(n, src, dst):
        return remote(src, dst.at[k], wsem.at[n], wrecv.at[n], mate)

    gives = [give(0, gain, gains)]
    gives[0].start()
    heads_q = wq.shape[1] // 2
    heads_k = wk.shape[0] // 2
    nq = heads_q // HD * LANE
    nk = heads_k // HD * LANE
    for c in first:
        c.wait()
    for core, dst_in, dst_out in ((1 - k, give_in, give_out), (k, wqkv_o.at[k], wo_o.at[k])):
        sq = spread(2 * heads_q, nq, core * heads_q)
        sk = spread(2 * heads_k, nk, core * heads_k)
        dst_in[:, 0:nq] = nn(wq[...], sq).astype(BF)
        dst_in[:, nq : nq + nk] = tn(wk[...], sk).astype(BF)
        dst_in[:, nq + nk : nq + 2 * nk] = tn(wv[...], sk).astype(BF)
        dst_out[...] = nn(spread_t(nq, 2 * heads_q, core * heads_q), wo[...]).astype(BF)
    gives += [give(1, give_in, wqkv_o), give(2, give_out, wo_o)]
    gives += [give(3, wg.at[:, his], wg_o), give(4, wu.at[:, his], wu_o), give(5, wd.at[his], wd_o)]
    for g in gives[1:]:
        g.start()
    sign = jnp.where(lax.broadcasted_iota(jnp.int32, (32, LANE), 1) < LANE // 2, -1.0, 1.0)
    cf, sf = tables[2], tables[3]
    for a in range(LENGTH // 32):
        ca, sa = tables[0, a : a + 1, :], tables[1, a : a + 1, :]
        cos_o[a * 32 : a * 32 + 32, :] = ca * cf - sa * sf
        sin_o[a * 32 : a * 32 + 32, :] = (sa * cf + ca * sf) * sign
    for c in keep:
        c.wait()
    for n in range(3):
        gives[n].wait_recv()

    def compute(i, row, half):
        at = rows_of(half)
        x0 = raw[0, row, at, :].astype(F32)
        x1 = raw[1, row, at, :].astype(F32)
        total = jnp.sum(x0 * x0, 1, keepdims=True) + jnp.sum(x1 * x1, 1, keepdims=True)
        rstd = lax.rsqrt(total / (2 * width) + EPS)
        n0 = (x0 * rstd * gains[0]).astype(BF)
        n1 = (x1 * rstd * gains[1]).astype(BF)
        normed[0, row, at, :] = n0
        normed[1, row, at, :] = n1

        @pl.when(i < 2)
        def _():
            rstd_o[at, :] = jnp.broadcast_to(rstd, (PIECE, LANE))

        got = nn(n0, wqkv_o[0]) + nn(n1, wqkv_o[1])
        pos = pl.ds(pl.multiple_of((row % 2) * 2 * PIECE + half * PIECE, PIECE), PIECE)
        out = pl.ds(pl.multiple_of(row * 2 * PIECE + half * PIECE, PIECE), PIECE)
        cos, sin = cos_o[pos, :], sin_o[pos, :]
        for part in range(4):
            u = got[:, part * LANE : (part + 1) * LANE]
            if part < 3:
                u = u * cos + pltpu.roll(u, LANE // 2, 1) * sin
            qkv[part, out, :] = u.astype(BF)
            if part >= 2:
                kvt[part - 2, :, out] = u.T.astype(BF)

    gather.run(compute)
    for g in gives[3:]:
        g.wait_recv()
    for g in gives:
        g.wait_send()


def project(x, gain, wq, wk, wv, wo, wg, wu, wd):
    tokens, width = x.shape
    f_half = wg.shape[1] // 2
    cols = 4 * LANE
    outs = [
        sds((2, 4, tokens, width), BF),
        sds((4, 4 * tokens, LANE), BF),
        sds((2, LANE, 4 * tokens), BF),
        sds((2, width, cols), BF),
        sds((2, 2 * LANE, width), BF),
        sds((2, width, f_half), BF),
        sds((2, width, f_half), BF),
        sds((2, f_half, width), BF),
        sds((LENGTH, LANE), F32),
        sds((LENGTH, LANE), F32),
        sds((tokens, LANE), F32),
    ]
    scratch = [
        pltpu.VMEM((2, 4, tokens, width), BF),
        pltpu.VMEM((2, 1, width), F32),
        pltpu.VMEM((width, cols), BF),
        pltpu.VMEM((2 * LANE, width), BF),
        pltpu.VMEM(wq.shape, BF),
        pltpu.VMEM(wk.shape, BF),
        pltpu.VMEM(wv.shape, BF),
        pltpu.VMEM(wo.shape, BF),
        DMA((6,)),
        DMA((6,)),
        DMA((8,)),
    ] + GATHER_SEMS
    ins = [ANY, VM] + [ANY] * 7 + [VM]
    args = [x, gain, wq, wk, wv, wo, wg, wu, wd, jnp.asarray(np.stack(angle_tables()))]
    return call(project_kernel, 0, outs, ins, args, scratch, 3e10)


def exchange(k, stat, sems):
    copy = remote(stat.at[k], stat.at[k], sems.at[0], sems.at[1], {"col": 1 - k})
    copy.start()
    remote(stat.at[1 - k], stat.at[1 - k], sems.at[0], sems.at[1], {"col": 1 - k}).wait_recv()
    copy.wait_send()
    return stat[0][:, 0:1] + stat[1][:, 0:1]


def causal(shape):
    return lax.broadcasted_iota(jnp.int32, shape, 0) <= lax.broadcasted_iota(jnp.int32, shape, 1)


def attend_kernel(
    qkv, kvt, wo, x, gain, dy,
    attn, lse, hidden, normed, rstd_o, all_dy,
    stat, ssem, *rest,
):
    r, k, rx, ry, r3 = place()
    width = x.shape[1]
    greet(rx, ry, k)
    total = Sum(rest[:9])
    gather = Gather(dy, all_dy, rest[9:])
    gather.start()

    def compute(row, half):
        base = pl.multiple_of(row // 2 * LENGTH, LENGTH)
        at = rows_of(half)
        qrow = pl.ds(pl.multiple_of(row * 2 * PIECE + half * PIECE, PIECE), PIECE)
        order = (row % 2) * 2 + half

        def attend(p):
            span = PIECE * (p + 1)
            for head in range(2):
                keys = qkv[2, pl.ds(base, span), :]
                s = nt(keys, qkv[head, qrow, :])
                tail = jnp.where(causal((PIECE, PIECE)), s[span - PIECE :], -1e30)
                s = tail if p == 0 else jnp.concatenate([s[: span - PIECE], tail], 0)
                top = jnp.max(s, 0, keepdims=True)
                e = jnp.exp((s - top) * SCALE)
                weight = jnp.sum(e, 0, keepdims=True)
                probs = (e * (1.0 / weight)).astype(BF)
                mixed = nn(kvt[1, :, pl.ds(base, span)], probs)
                attn[row, at, head * LANE : (head + 1) * LANE] = mixed.T.astype(BF)
                lse[head, row * 2 + half] = top * SCALE + jnp.log(weight)

        for p in range(4):
            pl.when(order == p)(lambda p=p: attend(p))
        a = attn[row, at, :]
        return nn(a, wo[k]), nn(a, wo[1 - k])

    total.send_all(compute)
    total.relay(4)
    total.relay(5)
    gather.arrive(2)
    gather.arrive(3)
    for half in range(2):
        at = rows_of(half)
        h = x[at, :].astype(F32) + total.last(6 + half)
        hidden[at, :] = h
        stat[k, at, :] = jnp.broadcast_to(jnp.sum(h * h, 1, keepdims=True), (PIECE, LANE))
    rstd = lax.rsqrt(exchange(k, stat, ssem) / (2 * width) + EPS)
    rstd_o[...] = jnp.broadcast_to(rstd, rstd_o.shape)
    normed[...] = (hidden[...] * rstd * gain[...]).astype(BF)
    for i in range(4, 8):
        gather.arrive(i)
    for i in range(8):
        gather.ready(i)
    gather.local.wait()
    gather.finish()
    total.finish()


def attend(qkv, kvt, wo, x, gain, dy):
    tokens, width = x.shape
    outs = [
        sds((4, tokens, 2 * LANE), BF),
        sds((2, 8, 1, PIECE), F32),
        sds((tokens, width), F32),
        sds((tokens, width), BF),
        sds((tokens, LANE), F32),
        sds((2, 4, tokens, width), BF),
    ]
    scratch = [pltpu.VMEM((2, tokens, LANE), F32), DMA((2,))] + sum_scratch(width) + GATHER_SEMS
    return call(
        attend_kernel, 1, outs, [VM] * 5 + [ANY], [qkv, kvt, wo, x, gain, dy], scratch, 3e10
    )


def expand_kernel(
    nf, all_dy, wg, wu, wd, all_f, middle, d_gate, d_up, part, grad, give, gsend, grecv, *sems
):
    r, k, rx, ry, r3 = place()
    greet(rx, ry, k)
    gather = Gather(nf, all_f, sems)
    gather.start()

    def compute(i, row, half):
        at = rows_of(half)
        f0, f1 = all_f[0, row, at, :], all_f[1, row, at, :]
        dy0, dy1 = all_dy[0, row, at, :], all_dy[1, row, at, :]
        gate = nn(f0, wg[0]) + nn(f1, wg[1])
        upper = nn(f0, wu[0]) + nn(f1, wu[1])
        d_mid = nt(dy0, wd[0]) + nt(dy1, wd[1])
        sig = 1.0 / (1.0 + jnp.exp(-gate))
        swish = gate * sig
        mid = (swish * upper).astype(BF)
        middle[row, at, :] = mid
        d_gate[row, at, :] = (d_mid * upper * sig * (1.0 + gate * (1.0 - sig))).astype(BF)
        d_up[row, at, :] = (d_mid * swish).astype(BF)
        g0, g1 = tn(mid, dy0), tn(mid, dy1)

        @pl.when(i == 0)
        def _():
            grad[0] = g0
            grad[1] = g1

        @pl.when(i > 0)
        def _():
            grad[0] += g0
            grad[1] += g1

    gather.run(compute)
    half = DOWN_CHUNKS // 4

    def swap(j, core):
        return remote(give.at[pl.ds(2 * j, 2)], part.at[pl.ds(2 * (half * core + j), 2)], gsend.at[j], grecv.at[j], {"col": 1 - k})

    for j in range(half):
        for h in range(2):
            give[2 * j + h] = grad[1 - k, j * TALL + h * CHUNK : j * TALL + (h + 1) * CHUNK, :].astype(BF)
        swap(j, k).start()
    for j in range(half):
        for h in range(2):
            rows = slice(j * TALL + h * CHUNK, j * TALL + (h + 1) * CHUNK)
            part[2 * (half * k + j) + h] = grad[k, rows, :].astype(BF)
    for j in range(half):
        swap(j, 1 - k).wait_recv()
    for j in range(half):
        swap(j, k).wait_send()


def expand(nf, all_dy, wg, wu, wd):
    tokens, width = nf.shape
    f_half = wg.shape[2]
    outs = [sds((2, 4, tokens, width), BF)] + [sds((4, tokens, f_half), BF)] * 3
    outs += [sds((DOWN_CHUNKS, CHUNK, WIDE), BF)]
    half = DOWN_CHUNKS // 4
    scratch = [pltpu.VMEM((2, f_half, width), F32), pltpu.VMEM((2 * half, CHUNK, WIDE), BF), DMA((half,)), DMA((half,))]
    args = [nf, all_dy, wg, wu, wd]
    return call(expand_kernel, 2, outs, [ANY] + [VM] * 4, args, scratch + GATHER_SEMS, 3e10)


TICKS = 35


def flat(ref, h, m=None):
    got = ref[h] if m is None else ref[h, :, :, pl.ds(pl.multiple_of(m * 256, 256), 256)]
    return got.reshape(-1, got.shape[-1])


def contract_kernel(
    d_gate, d_up, wg, wu, hidden, rstd2, gain, dy, wo, attn, part_d, f_any,
    d_hidden, gains_o, part, part_o, d_attn, totals, acc_c, tot_c,
    stat, ssem, give, gsend, grecv, gathered, dya, grad, give_o, his_o, gsem, fsem, *rest,
):
    r, k, rx, ry, r3 = place()
    width = hidden.shape[1]
    fetch = pltpu.make_async_copy(f_any, gathered, fsem)
    fetch.start()
    greet(rx, ry, k, True)
    total = Sum(rest[:9])
    gather = Gather(dya, gathered, rest[9:14])
    parts = [(0, DOWN_CHUNKS, part_d), (DOWN_CHUNKS, MLP_CHUNKS, part), (MLP_CHUNKS, OUT_CHUNKS, part_o)]
    line = Line(parts, totals, (acc_c, tot_c), rest[14:], 0, TICKS)
    line.open()

    def compute(row, half):
        at = rows_of(half)
        g, u = d_gate[row, at, :], d_up[row, at, :]
        return nt(g, wg[k]) + nt(u, wu[k]), nt(g, wg[1 - k]) + nt(u, wu[1 - k])

    def early(j):
        @pl.when(j % 2 == 1)
        def _():
            line.step(j // 2)

    total.send_all(compute, early)

    def swap(e, core):
        to = part.at[pl.ds(2 * (e // 4 * 8 + 4 * core + e % 4), 2)]
        return remote(give.at[pl.ds(2 * e, 2)], to, gsend.at[e], grecv.at[e], {"col": 1 - k})

    def wide_part(h, right, dst, first):
        def one(m, carry):
            got = tn(flat(gathered, h, m), right[...].reshape(-1, right.shape[2])).astype(BF)
            for b in range(2):
                lanes = pl.ds(pl.multiple_of((2 * m + b) * TALL, TALL), TALL)
                for j in range(4):
                    for u in range(2):
                        rows = slice(b * TALL + u * CHUNK, b * TALL + (u + 1) * CHUNK)
                        dst[2 * (first + j) + u, :, lanes] = got[rows, j * TALL : (j + 1) * TALL]
            return carry

        lax.fori_loop(0, width // 256, one, 0)

    fetch.wait()
    wide_part(1 - k, d_gate, give, 0)
    for e in range(4):
        swap(e, k).start()
    line.step(4)
    wide_part(k, d_gate, part, 4 * k)
    line.step(5)
    wide_part(1 - k, d_up, give, 4)
    for e in range(4, 8):
        swap(e, k).start()
    line.step(6)
    wide_part(k, d_up, part, 8 + 4 * k)
    line.step(7)
    total.relay(4)
    total.relay(5)
    for e in range(8):
        swap(e, 1 - k).wait_recv()
    for j in range(8, 13):
        line.step(j)
    gains = jnp.zeros((1, width), F32)
    for half in range(2):
        at = rows_of(half)
        d_nf = total.last(6 + half)
        h = hidden[at, :]
        gains = gains + jnp.sum(d_nf * h * rstd2[at, 0:1], 0, keepdims=True)
        scaled = d_nf * gain[...]
        d_hidden[at, :] = scaled
        stat[k, at, :] = jnp.broadcast_to(jnp.sum(scaled * h, 1, keepdims=True), (PIECE, LANE))
    gains_o[...] = gains
    inner = exchange(k, stat, ssem) / (2 * width)
    rs = rstd2[:, 0:1]
    value = dy[...].astype(F32) + rs * d_hidden[...] - hidden[...] * (rs * rs * rs * inner)
    d_hidden[...] = value
    dya[...] = value.astype(BF)
    gather.start()

    def piece(i, row, half):
        at = rows_of(half)
        d0, d1 = gathered[0, row, at, :], gathered[1, row, at, :]
        d_attn[row, at, :] = (nt(d0, wo[0]) + nt(d1, wo[1])).astype(BF)
        a = attn[row, at, :]
        g0, g1 = tn(a, d0), tn(a, d1)

        @pl.when(i == 0)
        def _():
            grad[0] = g0
            grad[1] = g1

        @pl.when(i > 0)
        def _():
            grad[0] += g0
            grad[1] += g1

    def before(q):
        @pl.when(q == 0)
        def _():
            for j in range(13, 15):
                line.step(j)

        for j in range(3):
            line.step(15 + 4 * q + j)

    def after(q):
        line.step(18 + 4 * q)

    gather.run(piece, before, after)
    give_o[...] = grad[1 - k].astype(BF)
    give_out = remote(give_o, his_o, gsem.at[0], gsem.at[1], {"col": 1 - k})
    give_out.start()
    q_cols = part_o.shape[0] * CHUNK
    mine = nn(spread(q_cols, 2 * LANE, k * (q_cols // 2)), grad[k].astype(BF))
    give_out.wait_recv()
    out = mine + nn(spread(q_cols, 2 * LANE, (1 - k) * (q_cols // 2)), his_o[...])
    for c in range(q_cols // CHUNK):
        part_o[c] = out[c * CHUNK : (c + 1) * CHUNK].astype(BF)
    line.rest(31)
    for e in range(8):
        swap(e, k).wait_send()
    give_out.wait_send()
    total.finish()


def contract(d_gate, d_up, wg, wu, hidden, rstd2, gain, dy, wo, attn, part_d, all_f):
    tokens, width = hidden.shape
    n = lax.axis_size("dp")
    outs = [sds((tokens, width), F32), sds((1, width), F32)]
    outs += [sds((MLP_CHUNKS - DOWN_CHUNKS, CHUNK, WIDE), BF), sds((OUT_CHUNKS - MLP_CHUNKS, CHUNK, WIDE), BF)]
    outs += [sds((4, tokens, 2 * LANE), BF)] + line_outs(TICKS)
    out_specs = [VM] * 5 + [ANY] + [VM] * 2
    scratch = [pltpu.VMEM((2, tokens, LANE), F32), DMA((2,))]
    scratch += [pltpu.VMEM((16, CHUNK, WIDE), BF), DMA((8,)), DMA((8,))]
    scratch += [pltpu.VMEM((2, 4, tokens, width), BF), pltpu.VMEM((tokens, width), BF)]
    scratch += [pltpu.VMEM((2, 2 * LANE, width), F32)] + [pltpu.VMEM((2 * LANE, width), BF)] * 2
    scratch += [DMA((2,)), DMA]
    scratch += sum_scratch(width) + GATHER_SEMS + line_scratch(n, TICKS)
    args = [d_gate, d_up, wg, wu, hidden, rstd2, gain, dy, wo, attn, part_d, all_f]
    ins = [VM] * 11 + [ANY]
    return call(contract_kernel, 3, outs, ins, args, scratch, 5e10, vmem_limit(n), out_specs)


def vmem_limit(n):
    return 60 if n <= 4 else 63


def columns(rows, cols, core, q_cols, k_cols):
    i = lax.broadcasted_iota(jnp.int32, (rows, cols), 0)
    at = lax.broadcasted_iota(jnp.int32, (rows, cols), 1)
    part, lane = i // LANE, i % LANE
    index = jnp.where(lane < HALF, lane, lane - (LANE // 2 - HALF))
    q = core * (q_cols // 2) + part * HD
    kv = q_cols + (part - 2) * k_cols + core * (k_cols // 2)
    to = jnp.where(part < 2, q, kv) + index
    pad = lane % (LANE // 2) >= HALF
    return jnp.where((at == to) & (pad == False), 1.0, 0.0).astype(BF)


def backward_kernel(
    q_cols, k_cols,
    qkv, kvt, lse, d_attn, cos, sin, middle, wd, hidden, wqkv, x, rstd1, d_hidden, gain, gains_f,
    part_m, part_o, acc_c, tot_c, normed_any,
    output, grad_x, gains_o, totals,
    dk, dv, d_proj, normed, part, mine, give, his, gsem, stat, ssem, free, fsem,
    mine_g, pair_g, slots, gsend, grecv, *rest,
):
    r, k, rx, ry, r3 = place()
    width = x.shape[1]
    n = lax.axis_size("dp")
    z = lax.axis_index("dp")
    fetch = pltpu.make_async_copy(normed_any, normed, fsem)
    fetch.start()
    greet(rx, ry, k, True, True)
    sums = rest[:5]
    down = Sum(sums + rest[5:9])
    into = Sum(sums + rest[9:13])
    ticks = line_ticks(n) - TICKS
    parts = [(DOWN_CHUNKS, MLP_CHUNKS, part_m), (MLP_CHUNKS, OUT_CHUNKS, part_o), (OUT_CHUNKS, ALL_CHUNKS, part)]
    line = Line(parts, totals, None, rest[13:], TICKS, ticks, (acc_c, tot_c))
    line.open()

    def down_piece(row, half):
        m = middle[row, rows_of(half), :]
        return nn(m, wd[k]), nn(m, wd[1 - k])

    def early(j):
        @pl.when(j % 3 == 1)
        def _():
            line.step(j // 3)

    down.send_all(down_piece, early)

    def unrotate(u, p):
        at = pl.ds(p * PIECE, PIECE)
        return u * cos[at, :] - pltpu.roll(u, LANE // 2, 1) * sin[at, :]

    def sequence(seq):
        base = pl.multiple_of(seq * LENGTH, LENGTH)

        def one_head(head, carry):
            for p in range(4):
                span = PIECE * (p + 1)
                row = seq * 2 + p // 2
                at = pl.ds((p % 2) * PIECE, PIECE)
                out = pl.ds(pl.multiple_of(base + p * PIECE, PIECE), PIECE)
                keys = qkv[2, pl.ds(base, span), :]
                q = qkv[head, out, :]
                lane = pl.ds(pl.multiple_of(head * LANE, LANE), LANE)
                do = d_attn[row, at, lane]
                e = jnp.exp(nt(keys, q) * SCALE - lse[head, seq * 4 + p])
                tail = jnp.where(causal((PIECE, PIECE)), e[span - PIECE :], 0.0)
                e = tail if p == 0 else jnp.concatenate([e[: span - PIECE], tail], 0)
                dp = nt(qkv[3, pl.ds(base, span), :], do)
                inner = jnp.sum(e * dp, 0, keepdims=True)
                ds = (e * (dp - inner)).astype(BF)
                dv[0:span, :] += nn(e.astype(BF), do)
                dk[0:span, :] += nn(ds, q)
                dq = nn(kvt[0, :, pl.ds(base, span)], ds).T * SCALE
                d_proj[out, lane] = unrotate(dq, p).astype(BF)
                tick = 3 + seq * 8 + head * 4 + p

                @pl.when(tick < OUT_CHUNKS - LAG - TICKS)
                def _(tick=tick):
                    line.step(tick)

            return carry

        dk[...] = jnp.zeros_like(dk)
        dv[...] = jnp.zeros_like(dv)
        lax.fori_loop(0, 2, one_head, 0)
        for p in range(4):
            at = pl.ds(p * PIECE, PIECE)
            out = pl.ds(pl.multiple_of(base + p * PIECE, PIECE), PIECE)
            d_proj[out, 2 * LANE : 3 * LANE] = unrotate(dk[at, :] * SCALE, p).astype(BF)
            d_proj[out, 3 * LANE : 4 * LANE] = dv[at, :].astype(BF)

    def both(seq, carry):
        sequence(seq)

        @pl.when(seq == 0)
        def _():
            down.relay(4)
            down.relay(5)

        return carry

    lax.fori_loop(0, 2, both, 0)
    for half in range(2):
        at = rows_of(half)
        output[at, :] = hidden[at, :] + down.last(6 + half)
    down.finish()
    for device in ({"row": rx}, {"row": ry}, {"col": 1 - k}):
        pl.semaphore_signal(free, inc=1, device_id=device, device_id_type=MESH)
    pl.semaphore_wait(free, 3)

    fetch.wait()

    def in_part(h, dst):
        def one(m, carry):
            dst[pl.ds(pl.multiple_of(m * 256, 256), 256), :] = tn(flat(normed, h, m), d_proj[...]).astype(BF)
            return carry

        lax.fori_loop(0, width // 256, one, 0)

    in_part(1 - k, give)
    swap = remote(give, his, gsem.at[0], gsem.at[1], {"col": 1 - k})
    swap.start()
    in_part(k, mine)
    cols = q_cols + 2 * k_cols
    got = nn(mine[...], columns(4 * LANE, cols, k, q_cols, k_cols))
    swap.wait_recv()
    got = got + nn(his[...], columns(4 * LANE, cols, 1 - k, q_cols, k_cols))
    for c in range(width // CHUNK):
        part[c] = got[c * CHUNK : (c + 1) * CHUNK].astype(BF)

    def into_piece(row, half):
        d = d_proj[pl.ds(pl.multiple_of(row * 2 * PIECE + half * PIECE, PIECE), PIECE), :]
        return nt(d, wqkv[k]), nt(d, wqkv[1 - k])

    def beside(j):
        @pl.when(j % 2 == 1)
        def _():
            line.step(17 + j // 2)

    into.send_all(into_piece, beside)
    for j in range(21, 24):
        line.step(j)
    into.relay(4)
    into.relay(5)
    for j in range(24, 29):
        line.step(j)
    gains = jnp.zeros((1, width), F32)
    for half in range(2):
        at = rows_of(half)
        d_na = into.last(6 + half)
        xs = x[at, :].astype(F32)
        gains = gains + jnp.sum(d_na * xs * rstd1[at, 0:1], 0, keepdims=True)
        scaled = d_na * gain[...]
        grad_x[at, :] = scaled
        stat[k, at, :] = jnp.broadcast_to(jnp.sum(scaled * xs, 1, keepdims=True), (PIECE, LANE))

    def row_total(step, device):
        copy = remote(mine_g.at[step], pair_g.at[step], gsend.at[n + step], grecv.at[n + step], {"row": device})
        copy.start()
        return copy

    mine_g[0, 0:1] = gains
    mine_g[0, 1:2] = gains_f[...]
    over_x = row_total(0, rx)
    inner = exchange(k, stat, ssem) / (2 * width)
    rs = rstd1[:, 0:1]
    over_x.wait_recv()
    mine_g[1] = mine_g[0] + pair_g[0]
    over_y = row_total(1, ry)
    grad_x[...] = d_hidden[...] + rs * grad_x[...] - x[...].astype(F32) * (rs * rs * rs * inner)
    over_y.wait_recv()
    slots[z] = mine_g[1] + pair_g[1]

    def over_dp(t, mine):
        other = (z + t) % n
        g = z if mine else other
        return remote(slots.at[g], slots.at[g], gsend.at[t], grecv.at[g], {"dp": other})

    def start(t, carry):
        over_dp(t, True).start()
        return carry

    lax.fori_loop(1, n, start, 0)
    line.rest(29)

    def wait(t, carry):
        over_dp(t, False).wait_recv()
        over_dp(t, True).wait_send()
        return carry

    lax.fori_loop(1, n, wait, 0)
    gains_o[...] = lax.fori_loop(1, n, lambda g, total: total + slots[g], slots[0])
    over_x.wait_send()
    over_y.wait_send()
    swap.wait_send()
    into.finish()


def backward(
    qkv, kvt, lse, d_attn, cos, sin, middle, wd, hidden, wqkv, x, rstd1, d_hidden, gain, gains_f,
    part_m, part_o, acc, tot, normed, q_cols, k_cols,
):
    tokens, width = x.shape
    n = lax.axis_size("dp")
    ticks = line_ticks(n) - TICKS
    outs = [sds((tokens, width), F32)] * 2 + [sds((2, width), F32), sds((ticks, CHUNK, WIDE), BF)]
    scratch = [pltpu.VMEM((LENGTH, LANE), F32)] * 2 + [pltpu.VMEM((4 * tokens, 4 * LANE), BF)]
    scratch += [pltpu.VMEM((2, 4, tokens, width), BF), pltpu.VMEM((ALL_CHUNKS - OUT_CHUNKS, CHUNK, WIDE), BF)]
    scratch += [pltpu.VMEM((width, 4 * LANE), BF)] * 3 + [DMA((2,))]
    scratch += [pltpu.VMEM((2, tokens, LANE), F32), DMA((2,)), pltpu.SemaphoreType.REGULAR, DMA]
    scratch += [pltpu.VMEM((2, 2, width), F32)] * 2 + [pltpu.VMEM((n, 2, width), F32)]
    scratch += [DMA((n + 2,)), DMA((n + 2,))]
    both = sum_scratch(width)
    scratch += both + both[5:] + line_scratch(n, ticks)
    args = [qkv, kvt, lse, d_attn, cos, sin, middle, wd, hidden, wqkv, x, rstd1, d_hidden, gain, gains_f]
    args += [part_m, part_o, acc, tot, normed]
    kernel = functools.partial(backward_kernel, q_cols, k_cols)
    ins = [VM] * (len(args) - 1) + [ANY]
    return call(kernel, 5, outs, ins, args, scratch, 5e10, vmem_limit(n), [VM] * 3 + [ANY])


def unpack_kernel(ticks, q_cols, k_cols, *rest):
    tots, (down, gate, up, out, q_o, k_o, v_o), rest = rest[: len(ticks)], rest[len(ticks) : len(ticks) + 7], rest[len(ticks) + 7 :]
    chunks, wide, parts, isem, osem = rest
    n, s, _, _ = line_place()
    mid = n // 2
    off = LAG * (2 * mid - 2 - s)
    offs = [LAG * o for o in range(mid - 1, 2 * mid - 1)]

    def source(t):
        for tot, count in zip(tots, ticks):
            if t < count:
                return tot.at[t]
            t -= count

    def load(c):
        for o in offs:

            @pl.when(off == o)
            def _(o=o):
                for u in range(2):
                    dst = chunks.at[c % 4, pl.ds(u * CHUNK, CHUNK)]
                    pltpu.make_async_copy(source(2 * c + u + o), dst, isem.at[c % 4, u]).start()

    def stored(c):
        slot = c % 4
        buf = wide.at[slot]
        if c < 8:
            return [pltpu.make_async_copy(buf, down.at[pl.ds(c * TALL, TALL)], osem.at[slot, 0])]
        if c < MLP_CHUNKS // 2:
            to, lanes = (gate, up)[c // 8 - 1], pl.ds(c % 8 * TALL, TALL)
            return [
                pltpu.make_async_copy(
                    buf.at[:, pl.ds(b * TALL, TALL)], to.at[pl.ds(b * TALL, TALL), lanes], osem.at[slot, b]
                )
                for b in range(WIDE // TALL)
            ]
        if c < OUT_CHUNKS // 2:
            return [pltpu.make_async_copy(buf, out.at[pl.ds((c - MLP_CHUNKS // 2) * TALL, TALL)], osem.at[slot, 0])]
        rows = pl.ds((c - OUT_CHUNKS // 2) * TALL, TALL)
        return [
            pltpu.make_async_copy(buf.at[:, pl.ds(0, q_cols)], q_o.at[rows], osem.at[slot, 0]),
            pltpu.make_async_copy(parts.at[0, slot], k_o.at[:, rows], osem.at[slot, 1]),
            pltpu.make_async_copy(parts.at[1, slot], v_o.at[:, rows], osem.at[slot, 2]),
        ]

    for c in range(3):
        load(c)
    for c in range(ALL_CHUNKS // 2):
        if c + 3 < ALL_CHUNKS // 2:
            load(c + 3)
        if c >= 4:
            for copy in stored(c - 4):
                copy.wait()
        for u in range(2):
            dst = chunks.at[c % 4, pl.ds(u * CHUNK, CHUNK)]
            pltpu.make_async_copy(dst, dst, isem.at[c % 4, u]).wait()
        value = chunks[c % 4].astype(F32)
        wide[c % 4] = value
        if c >= OUT_CHUNKS // 2:
            parts[0, c % 4] = value[:, q_cols : q_cols + k_cols].T
            parts[1, c % 4] = value[:, q_cols + k_cols :].T
        for copy in stored(c):
            copy.start()
    for c in range(ALL_CHUNKS // 2 - 4, ALL_CHUNKS // 2):
        for copy in stored(c):
            copy.wait()


def unpack(tots, q_cols, k_cols):
    n = lax.axis_size("dp")
    ticks = [TICKS, line_ticks(n) - TICKS]
    outs = [sds((8 * TALL, WIDE), F32), sds((WIDE, 8 * TALL), F32), sds((WIDE, 8 * TALL), F32)]
    outs += [sds((q_cols, WIDE), F32), sds((WIDE, q_cols), F32), sds((k_cols, WIDE), F32), sds((k_cols, WIDE), F32)]
    moved = 6 * ALL_CHUNKS // 2 * TALL * WIDE
    return pl.pallas_call(
        functools.partial(unpack_kernel, ticks, q_cols, k_cols),
        out_shape=outs,
        in_specs=[ANY] * len(tots),
        out_specs=[ANY] * len(outs),
        scratch_shapes=[
            pltpu.VMEM((4, TALL, WIDE), BF),
            pltpu.VMEM((4, TALL, WIDE), F32),
            pltpu.VMEM((2, 4, k_cols, TALL), F32),
            DMA((4, 2)),
            DMA((4, WIDE // TALL)),
        ],
        compiler_params=pltpu.CompilerParams(vmem_limit_bytes=16 << 20),
        cost_estimate=pl.CostEstimate(flops=0, bytes_accessed=moved, transcendentals=0),
    )(*tots)


def on_device(
    layer_input, gain_attn, gain_ffn, w_query, w_key, w_value, w_out, w_gate, w_up, w_down, cotangent
):
    tokens, width = layer_input.shape
    q_cols, k_cols = w_query.shape[1], w_key.shape[1]
    gain_a, gain_f = gain_attn[None], gain_ffn[None]
    normed, qkv, kvt, wqkv, wo, wg, wu, wd, cos, sin, rstd1 = project(
        layer_input, gain_a, w_query, w_key.T, w_value.T, w_out, w_gate, w_up, w_down
    )
    attn, lse, hidden, nf, rstd2, all_dy = attend(qkv, kvt, wo, layer_input, gain_f, cotangent)
    all_f, middle, d_gate, d_up, part_d = expand(nf, all_dy, wg, wu, wd)
    d_hidden, gains_f, part_m, part_o, d_attn, tot1, acc, tot = contract(
        d_gate, d_up, wg, wu, hidden, rstd2, gain_f, cotangent, wo, attn, part_d, all_f
    )
    output, grad_x, gains, tot2 = backward(
        qkv, kvt, lse, d_attn, cos, sin, middle, wd, hidden, wqkv, layer_input, rstd1, d_hidden,
        gain_a, gains_f, part_m, part_o, acc, tot, normed, q_cols, k_cols,
    )
    down, gate, up, out, g_q, g_k, g_v = unpack([tot1, tot2], q_cols, k_cols)
    return output, grad_x, gains[0], gains[1], g_q, g_k.T, g_v.T, out, gate, up, down


def solution(mesh):
    assert mesh.shape["row"] == 4 and mesh.shape["col"] == 2
    tokens = P(("dp", "row"), "col")
    wide = P("col", "row")
    tall = P("row", "col")
    return jax.shard_map(
        on_device,
        mesh=mesh,
        in_specs=(tokens, P("col"), P("col"), wide, wide, wide, tall, wide, wide, tall, tokens),
        out_specs=(tokens, tokens, P("col"), P("col"), wide, wide, wide, tall, wide, wide, tall),
        check_vma=False,
    )
```

```python
import functools

import jax
import jax.numpy as jnp
import numpy as np
from jax import lax
from jax.experimental import pallas as pl
from jax.experimental.pallas import tpu as pltpu
from jax.sharding import PartitionSpec as P

HD = 96
HALF = HD // 2
LENGTH = 1024
EPS = 1e-05
THETA = 100000.0
SCALE = HD ** (-0.5)
LANE = 128
PIECE = 256

BF = jnp.bfloat16
F32 = jnp.float32
MESH = pl.DeviceIdType.MESH
VM = pl.BlockSpec(memory_space=pltpu.VMEM)
ANY = pl.BlockSpec(memory_space=pl.ANY)
DMA = pltpu.SemaphoreType.DMA


def nn(a, b):
    return lax.dot_general(a, b, (((1,), (0,)), ((), ())), preferred_element_type=F32)


def nt(a, b):
    return lax.dot_general(a, b, (((1,), (1,)), ((), ())), preferred_element_type=F32)


def place():
    r = lax.axis_index("row")
    k = lax.axis_index("col")
    return r, k, r + 1 - 2 * (r % 2), (r + 2) % 4, 3 - r


def tn(a, b):
    return lax.dot_general(a, b, (((0,), (0,)), ((), ())), preferred_element_type=F32)


def line_place():
    n = lax.axis_size("dp")
    z = lax.axis_index("dp")
    left = z < n // 2
    step = jnp.where(left, 1, -1)
    return n, jnp.where(left, z, n - 1 - z), z + step, z - step


def greet(rx, ry, k, line=False, groups=False):
    bar = pltpu.get_barrier_semaphore()

    def hello(device):
        pl.semaphore_signal(bar, inc=1, device_id=device, device_id_type=MESH)

    for device in ({"row": rx}, {"row": ry}, {"col": 1 - k}):
        hello(device)
    if not line:
        pl.semaphore_wait(bar, 3)
        return
    n, s, inward, outward = line_place()
    if groups:
        z = lax.axis_index("dp")

        def one(t, carry):
            hello({"dp": (z + t) % n})
            return carry

        lax.fori_loop(1, n, one, 0)
        pl.semaphore_wait(bar, 3 + n - 1)
        return
    hello({"dp": inward})

    @pl.when(s > 0)
    def _():
        hello({"dp": outward})

    pl.semaphore_wait(bar, jnp.where(s > 0, 5, 4))


def remote(src, dst, send, recv, device):
    return pltpu.make_async_remote_copy(
        src_ref=src, dst_ref=dst, send_sem=send, recv_sem=recv, device_id=device, device_id_type=MESH
    )


def rows_of(half):
    return pl.ds(pl.multiple_of(half * PIECE, PIECE), PIECE)


GATHER_SEMS = [DMA((6,)), DMA((6,)), DMA((8,)), DMA((8,)), DMA]


class Gather:
    def __init__(self, own, buf, sems):
        self.own, self.buf = own, buf
        self.isend, self.irecv, self.dsend, self.drecv, self.lsem = sems
        self.r, self.k, self.rx, self.ry, self.r3 = place()

    def piece(self, i):
        side = jnp.where(i % 2 == 0, self.rx, self.ry)
        row = jnp.where(i < 2, self.r, jnp.where(i < 6, side, self.r3))
        half = jnp.where(i // 2 == 2, 1 - i % 2, i % 2)
        return row, half

    def ici(self, sem, row, half, device, src=None):
        dst = self.buf.at[self.k, row, rows_of(half)]
        return remote(dst if src is None else src, dst, self.isend.at[sem], self.irecv.at[sem], {"row": device})

    def pair(self, i, core, row, half, src=None):
        dst = self.buf.at[core, row, rows_of(half)]
        return remote(dst if src is None else src, dst, self.dsend.at[i], self.drecv.at[i], {"col": 1 - self.k})

    def local(self):
        return pltpu.make_async_copy(self.own, self.buf.at[self.k, self.r], self.lsem)

    def start(self):
        own = self.buf.at[self.k, self.r] if self.own is None else self.own
        first, second = own.at[pl.ds(0, PIECE)], own.at[pl.ds(PIECE, PIECE)]
        self.ici(0, self.r, 0, self.rx, first).start()
        self.ici(1, self.r, 1, self.ry, second).start()
        self.ici(2, self.r, 1, self.rx, second).start()
        self.ici(3, self.r, 0, self.ry, first).start()
        self.pair(0, self.k, self.r, 0, first).start()
        self.pair(1, self.k, self.r, 1, second).start()
        if self.own is not None:
            self.local().start()

    def arrive(self, i):
        row, half = self.piece(i)
        self.ici(i - 2, row, half, self.rx).wait_recv()

        @pl.when(i == 2)
        def _():
            self.ici(4, row, half, self.ry).start()

        @pl.when(i == 3)
        def _():
            self.ici(5, row, half, self.rx).start()

        self.pair(i, self.k, row, half).start()

    def ready(self, i):
        row, half = self.piece(i)
        self.pair(i, 1 - self.k, row, half).wait_recv()

    def run(self, compute, before=None, after=None):
        if self.own is not None:
            self.local().wait()

        def pair(q, carry):
            for u in range(2):
                i = 2 * q + u
                self.ready(i)
                row, half = self.piece(i)
                compute(i, row, half)
            if before is not None:
                before(q)

            @pl.when(q < 3)
            def _():
                self.arrive(2 * q + 2)
                self.arrive(2 * q + 3)

            if after is not None:
                after(q)
            return carry

        lax.fori_loop(0, 4, pair, 0)
        self.finish()

    def finish(self):
        for i in range(6):
            self.ici(i, self.r, 0, self.rx).wait_send()
        for i in range(8):
            self.pair(i, self.k, self.r, 0).wait_send()


def sum_scratch(width):
    return [
        pltpu.VMEM((4, PIECE, width), F32),
        pltpu.VMEM((4, PIECE, width), BF),
        pltpu.VMEM((8, PIECE, width), BF),
        pltpu.VMEM((6, PIECE, width), BF),
        pltpu.VMEM((6, PIECE, width), BF),
        DMA((8,)),
        DMA((8,)),
        DMA((6,)),
        DMA((6,)),
    ]


class Sum:
    def __init__(self, scratch):
        self.own, self.ds, self.dr, self.ist, self.irt = scratch[:5]
        self.dsend, self.drecv, self.isend, self.irecv = scratch[5:]
        self.r, self.k, self.rx, self.ry, self.r3 = place()

    def piece(self, j):
        mid = jnp.where(j == 2, self.ry, jnp.where(j == 5, self.ry, self.rx))
        row = jnp.where(j < 2, self.r3, jnp.where(j < 6, mid, self.r))
        return row, j % 2

    def pair(self, j):
        return remote(self.ds.at[j % 4], self.dr.at[j], self.dsend.at[j], self.drecv.at[j], {"col": 1 - self.k})

    def ici(self, j):
        device = jnp.where(j == 0, self.ry, jnp.where(j == 2, self.ry, jnp.where(j == 5, self.ry, self.rx)))
        return remote(self.ist.at[j], self.irt.at[j], self.isend.at[j], self.irecv.at[j], {"row": device})

    def put(self, j, kept, given):
        @pl.when(j >= 4)
        def _():
            self.pair(j - 4).wait_send()

        self.own[j % 4] = kept
        self.ds[j % 4] = given.astype(BF)
        self.pair(j).start()

    def chip(self, j):
        self.pair(j).wait_recv()
        return self.own[j % 4] + self.dr[j].astype(F32)

    def forward(self, j):
        self.ist[j] = self.chip(j).astype(BF)
        self.ici(j).start()

    def relay(self, j):
        value = self.chip(j)
        self.ici(j - 4).wait_recv()
        self.ist[j] = (value + self.irt[j - 4].astype(F32)).astype(BF)
        self.ici(j).start()

    def last(self, j):
        value = self.chip(j)
        self.ici(j - 4).wait_recv()
        value = value + self.irt[j - 4].astype(F32)
        self.ici(j - 2).wait_recv()
        return value + self.irt[j - 2].astype(F32)

    def send_all(self, compute, hook=None):
        def step(j, carry):
            row, half = self.piece(j)
            kept, given = compute(row, half)
            self.put(j, kept, given)

            @pl.when(j > 0)
            def _():
                @pl.when(j < 5)
                def _():
                    self.forward(j - 1)

            if hook is not None:
                hook(j)
            return carry

        lax.fori_loop(0, 8, step, 0)

    def finish(self):
        for j in range(4, 8):
            self.pair(j).wait_send()
        for j in range(6):
            self.ici(j).wait_send()


TALL, WIDE = 128, 768
CHUNK = TALL // 2
DOWN_CHUNKS, MLP_CHUNKS, OUT_CHUNKS, ALL_CHUNKS = 16, 48, 54, 66
RING = 6
LAG = 2


def line_ring(n):
    return LAG * (2 * (n // 2) - 2) + 6


def line_ticks(n):
    return ALL_CHUNKS + LAG * (2 * (n // 2) - 2)


def line_outs(ticks):
    return [sds((ticks, CHUNK, WIDE), BF)] + [sds((LAG, CHUNK, WIDE), BF)] * 2


def line_scratch(n, ticks):
    slots = (RING, line_ring(n), line_ring(n), RING)
    return [pltpu.VMEM((count, CHUNK, WIDE), BF) for count in slots] + [DMA((ticks,))] * 6


class Line:
    def __init__(self, parts, totals, carry, scratch, first, ticks, before=None):
        self.parts, self.totals, self.carry = parts, totals, carry
        self.acc, self.tot, self.rin, self.rxb = scratch[:4]
        self.si, self.ri, self.rx, self.so, self.ro, self.out_sem = scratch[4:]
        self.first, self.ticks = first, ticks
        self.n, self.s, self.inward, self.outward = line_place()
        self.mid = self.n // 2
        self.ring = line_ring(self.n)
        if before is not None:

            @pl.when(self.s > 0)
            def _():
                for b in range(LAG):
                    self.acc[b] = before[0][b]
                    self.tot[b] = before[1][b]

    def valid(self, c):
        return (c >= 0) & (c < ALL_CHUNKS)

    def sends(self, j):
        s, mid, slot, near = self.s, self.mid, j % self.ring, j % RING
        to = {"dp": self.inward}
        c = self.first + j - LAG * s
        moves = []
        inward = (self.rin.at[slot], self.ri.at[j])
        across = (self.rxb.at[near], self.rx.at[j])
        for lo, hi, ref in self.parts:
            ok = (s == 0) & (c >= lo) & (c < hi)
            moves.append((ok, ref, c - lo, across if mid == 1 else inward))
        if mid > 1:
            ok = self.valid(c)
            moves.append((ok & (s == mid - 1), self.acc, near, across))
            if mid > 2:
                moves.append((ok & (s > 0) & (s < mid - 1), self.acc, near, inward))
        out = [
            (cond, lambda ref=ref, at=at, way=way: remote(ref.at[at], way[0], self.si.at[j], way[1], to))
            for cond, ref, at, way in moves
        ]
        if mid > 1:
            c = self.first + j - LAG * (2 * mid - 1 - s)
            out.append(((s > 0) & self.valid(c), lambda: self.outer(j)))
        return out

    def outer(self, j):
        return remote(
            self.tot.at[j % self.ring], self.tot.at[(j + LAG) % self.ring],
            self.so.at[j], self.ro.at[j], {"dp": self.outward},
        )

    def begin(self, j):
        for cond, copy in self.sends(j):

            @pl.when(cond)
            def _(copy=copy):
                copy().start()

    def total_of(self, j):
        copy = lambda: pltpu.make_async_copy(
            self.tot.at[(j + LAG) % self.ring], self.totals.at[j], self.out_sem.at[j]
        )
        return self.valid(self.first + j - LAG * (2 * self.mid - 2 - self.s)), copy

    def settle(self, j):
        for cond, copy in self.sends(j):

            @pl.when(cond)
            def _(copy=copy):
                copy().wait_send()

        cond, copy = self.total_of(j)

        @pl.when(cond)
        def _():
            copy().wait()

    def end(self, j):
        t, s, mid = self.first + j, self.s, self.mid
        slot, later = j % self.ring, (j + LAG) % self.ring
        near, next_near = j % RING, (j + LAG) % RING

        @pl.when(j >= 2)
        def _():
            self.settle(j - 2)

        def came(buf, at, sem):
            remote(buf.at[at], buf.at[at], self.si.at[j], sem.at[j], {"dp": self.inward}).wait_recv()

        def add_part(c, buf, at, dst, to):
            for lo, hi, ref in self.parts:

                @pl.when((c >= lo) & (c < hi))
                def _(ref=ref, lo=lo):
                    dst[to] = (ref[c - lo].astype(F32) + buf[at].astype(F32)).astype(BF)

        if mid > 1:
            c = t - LAG * (s - 1)

            @pl.when((s > 0) & self.valid(c))
            def _():
                came(self.rin, slot, self.ri)
                add_part(c, self.rin, slot, self.acc, next_near)

        @pl.when((s == mid - 1) & self.valid(t - LAG * (mid - 1)))
        def _():
            came(self.rxb, near, self.rx)
            if mid > 1:
                self.tot[later] = (self.acc[near].astype(F32) + self.rxb[near].astype(F32)).astype(BF)
            else:
                add_part(t, self.rxb, near, self.tot, later)

        cond, copy = self.total_of(j)
        if mid > 1:

            @pl.when((s < mid - 1) & cond)
            def _():
                self.outer(j).wait_recv()

        @pl.when(cond)
        def _():
            copy().start()

    def open(self):
        for j in range(min(LAG, self.ticks)):
            self.begin(j)

    def step(self, j):
        self.end(j)

        @pl.when(j + LAG < self.ticks)
        def _():
            self.begin(j + LAG)

    def rest(self, j):
        def one(t, carry):
            self.step(t)
            return carry

        lax.fori_loop(j, self.ticks, one, 0)
        for t in range(max(self.ticks - 2, 0), self.ticks):
            self.settle(t)
        if self.carry is not None:
            for b in range(LAG):
                self.carry[0][b] = self.acc[(self.ticks + b) % RING]
                self.carry[1][b] = self.tot[(self.ticks + b) % self.ring]


def call(kernel, cid, outs, ins, args, scratch, flops, vmem=44, out_specs=None):
    moved = sum(int(np.prod(a.shape)) * a.dtype.itemsize for a in list(args) + list(outs))
    return pl.pallas_call(
        kernel,
        out_shape=outs,
        in_specs=ins,
        out_specs=out_specs or [VM] * len(outs),
        scratch_shapes=scratch,
        compiler_params=pltpu.CompilerParams(
            collective_id=cid, has_side_effects=True, vmem_limit_bytes=vmem << 20
        ),
        cost_estimate=pl.CostEstimate(flops=int(flops), bytes_accessed=moved, transcendentals=0),
    )(*args)


def sds(shape, dtype):
    return jax.ShapeDtypeStruct(shape, dtype)


def head_index(iota):
    head, lane = iota // LANE, iota % LANE
    index = jnp.where(lane < HALF, lane, lane - (LANE // 2 - HALF))
    pad = lane % (LANE // 2) >= HALF
    return jnp.where(pad, -1, head * HD + index)


def spread(rows, cols, first):
    source = head_index(lax.broadcasted_iota(jnp.int32, (rows, cols), 1))
    at = lax.broadcasted_iota(jnp.int32, (rows, cols), 0)
    return jnp.where((source >= 0) & (at == source + first), 1.0, 0.0).astype(BF)


def spread_t(rows, cols, first):
    source = head_index(lax.broadcasted_iota(jnp.int32, (rows, cols), 0))
    at = lax.broadcasted_iota(jnp.int32, (rows, cols), 1)
    return jnp.where((source >= 0) & (at == source + first), 1.0, 0.0).astype(BF)


def angle_tables():
    lane = np.arange(LANE)
    freq = np.where(
        lane % (LANE // 2) < HALF, THETA ** (-2.0 * (lane % (LANE // 2)) / HD), 0.0
    )
    fine = np.arange(32)[:, None] * freq[None]
    coarse = fine * 32.0
    return [f(t).astype(np.float32) for t in (coarse, fine) for f in (np.cos, np.sin)]


def exchange(k, stat, sems):
    copy = remote(stat.at[k], stat.at[k], sems.at[0], sems.at[1], {"col": 1 - k})
    copy.start()
    remote(stat.at[1 - k], stat.at[1 - k], sems.at[0], sems.at[1], {"col": 1 - k}).wait_recv()
    copy.wait_send()
    return stat[0][:, 0:1] + stat[1][:, 0:1]


def causal(shape):
    return lax.broadcasted_iota(jnp.int32, shape, 0) <= lax.broadcasted_iota(jnp.int32, shape, 1)


def front_kernel(
    x, dy, gain, gain_f, wq_h, wk_h, wv_h, wo_h, wg, wu, wd, tables,
    normed_o, f_o, qkv, kvt, wqkv_o, wo_o, wg_o, wu_o, wd_o, cos_o, sin_o, rstd1_o,
    attn, lse, hidden, rstd2_o, middle, d_gate, d_up, part,
    buf, dys, stage, gains, give_in, give_out, wq, wk, wv, wo, wsem, wrecv, csem, nsem, fsem,
    stat, ssem, grad, give, gsend, grecv, *rest,
):
    r, k, rx, ry, r3 = place()
    width = x.shape[1]
    f_half = wg.shape[1] // 2
    mate = {"col": 1 - k}
    mine = pl.ds(pl.multiple_of(k * f_half, f_half), f_half)
    his = pl.ds(pl.multiple_of((1 - k) * f_half, f_half), f_half)
    keep = [
        pltpu.make_async_copy(gain, gains.at[k], csem.at[0]),
        pltpu.make_async_copy(wg.at[:, mine], wg_o.at[k], csem.at[1]),
        pltpu.make_async_copy(wu.at[:, mine], wu_o.at[k], csem.at[2]),
        pltpu.make_async_copy(wd.at[mine], wd_o.at[k], csem.at[3]),
    ]
    first = [
        pltpu.make_async_copy(src, dst, csem.at[4 + n])
        for n, (src, dst) in enumerate(((wq_h, wq), (wk_h, wk), (wv_h, wv), (wo_h, wo)))
    ]
    for c in first + keep:
        c.start()
    greet(rx, ry, k)
    gather = Gather(x, buf, rest[:5])
    gather_dy = Gather(dy, dys, rest[5:10])
    gather_f = Gather(None, buf, rest[10:15])
    total = Sum(rest[15:])
    gather.start()

    def give_to(n, src, dst):
        return remote(src, dst.at[k], wsem.at[n], wrecv.at[n], mate)

    gives = [give_to(0, gain, gains)]
    gives[0].start()
    heads_q = wq.shape[1] // 2
    heads_k = wk.shape[0] // 2
    nq = heads_q // HD * LANE
    nk = heads_k // HD * LANE
    for c in first:
        c.wait()
    for core, dst_in, dst_out in ((1 - k, give_in, give_out), (k, wqkv_o.at[k], wo_o.at[k])):
        sq = spread(2 * heads_q, nq, core * heads_q)
        sk = spread(2 * heads_k, nk, core * heads_k)
        dst_in[:, 0:nq] = nn(wq[...], sq).astype(BF)
        dst_in[:, nq : nq + nk] = tn(wk[...], sk).astype(BF)
        dst_in[:, nq + nk : nq + 2 * nk] = tn(wv[...], sk).astype(BF)
        dst_out[...] = nn(spread_t(nq, 2 * heads_q, core * heads_q), wo[...]).astype(BF)
    gives += [give_to(1, give_in, wqkv_o), give_to(2, give_out, wo_o)]
    gives += [give_to(3, wg.at[:, his], wg_o), give_to(4, wu.at[:, his], wu_o), give_to(5, wd.at[his], wd_o)]
    for g in gives[1:]:
        g.start()
    sign = jnp.where(lax.broadcasted_iota(jnp.int32, (32, LANE), 1) < LANE // 2, -1.0, 1.0)
    cf, sf = tables[2], tables[3]
    for a in range(LENGTH // 32):
        ca, sa = tables[0, a : a + 1, :], tables[1, a : a + 1, :]
        cos_o[a * 32 : a * 32 + 32, :] = ca * cf - sa * sf
        sin_o[a * 32 : a * 32 + 32, :] = (sa * cf + ca * sf) * sign
    for c in keep:
        c.wait()
    for n in range(3):
        gives[n].wait_recv()

    def keep_normed(i):
        row, half = gather.piece(i)
        return pltpu.make_async_copy(stage.at[i % 2], normed_o.at[:, row, rows_of(half)], nsem.at[i])

    def project(i, row, half):
        at = rows_of(half)
        x0 = buf[0, row, at, :].astype(F32)
        x1 = buf[1, row, at, :].astype(F32)
        square = jnp.sum(x0 * x0, 1, keepdims=True) + jnp.sum(x1 * x1, 1, keepdims=True)
        rstd = lax.rsqrt(square / (2 * width) + EPS)
        n0 = (x0 * rstd * gains[0]).astype(BF)
        n1 = (x1 * rstd * gains[1]).astype(BF)

        @pl.when(i >= 2)
        def _():
            keep_normed(i - 2).wait()

        stage[i % 2, 0] = n0
        stage[i % 2, 1] = n1

        @pl.when(i < 2)
        def _():
            rstd1_o[at, :] = jnp.broadcast_to(rstd, (PIECE, LANE))

        got = nn(n0, wqkv_o[0]) + nn(n1, wqkv_o[1])
        keep_normed(i).start()
        pos = pl.ds(pl.multiple_of((row % 2) * 2 * PIECE + half * PIECE, PIECE), PIECE)
        out = pl.ds(pl.multiple_of(row * 2 * PIECE + half * PIECE, PIECE), PIECE)
        cos, sin = cos_o[pos, :], sin_o[pos, :]
        for p in range(4):
            u = got[:, p * LANE : (p + 1) * LANE]
            if p < 3:
                u = u * cos + pltpu.roll(u, LANE // 2, 1) * sin
            qkv[p, out, :] = u.astype(BF)
            if p >= 2:
                kvt[p - 2, :, out] = u.T.astype(BF)

    def dy_too(q):
        @pl.when(q == 0)
        def _():
            gather_dy.start()

    gather.run(project, None, dy_too)
    for i in (6, 7):
        keep_normed(i).wait()

    def attend(row, half):
        base = pl.multiple_of(row // 2 * LENGTH, LENGTH)
        at = rows_of(half)
        qrow = pl.ds(pl.multiple_of(row * 2 * PIECE + half * PIECE, PIECE), PIECE)
        order = (row % 2) * 2 + half

        def queries(p):
            span = PIECE * (p + 1)
            for head in range(2):
                keys = qkv[2, pl.ds(base, span), :]
                s = nt(keys, qkv[head, qrow, :])
                tail = jnp.where(causal((PIECE, PIECE)), s[span - PIECE :], -1e30)
                s = tail if p == 0 else jnp.concatenate([s[: span - PIECE], tail], 0)
                top = jnp.max(s, 0, keepdims=True)
                e = jnp.exp((s - top) * SCALE)
                weight = jnp.sum(e, 0, keepdims=True)
                probs = (e * (1.0 / weight)).astype(BF)
                mixed = nn(kvt[1, :, pl.ds(base, span)], probs)
                attn[row, at, head * LANE : (head + 1) * LANE] = mixed.T.astype(BF)
                lse[head, row * 2 + half] = top * SCALE + jnp.log(weight)

        for p in range(4):
            pl.when(order == p)(lambda p=p: queries(p))
        a = attn[row, at, :]
        return nn(a, wo_o[k]), nn(a, wo_o[1 - k])

    def dy_arrive(j):
        @pl.when(j == 3)
        def _():
            gather_dy.arrive(2)
            gather_dy.arrive(3)

        @pl.when(j == 7)
        def _():
            gather_dy.arrive(4)
            gather_dy.arrive(5)

    total.send_all(attend, dy_arrive)
    for g in gives[3:]:
        g.wait_recv()
    gather_dy.local().wait()

    def mid_pair(q, carry):
        for u in range(2):
            i = 2 * q + u
            gather_dy.ready(i)
            row, half = gather_dy.piece(i)
            at = rows_of(half)
            d_mid = nt(dys[0, row, at, :], wd_o[0]) + nt(dys[1, row, at, :], wd_o[1])
            d_gate[row, at, :] = d_mid.astype(BF)
        return carry

    lax.fori_loop(0, 3, mid_pair, 0)
    gather_dy.arrive(6)
    gather_dy.arrive(7)
    total.relay(4)
    total.relay(5)
    mid_pair(3, 0)
    gather_dy.finish()
    for half in range(2):
        at = rows_of(half)
        h = buf[k, r, at, :].astype(F32) + total.last(6 + half)
        hidden[at, :] = h
        stat[k, at, :] = jnp.broadcast_to(jnp.sum(h * h, 1, keepdims=True), (PIECE, LANE))
    rstd2 = lax.rsqrt(exchange(k, stat, ssem) / (2 * width) + EPS)
    buf[k, r] = (hidden[...] * rstd2 * gain_f[...]).astype(BF)
    rstd2_o[...] = jnp.broadcast_to(rstd2, rstd2_o.shape)
    gather_f.start()

    def keep_f(i):
        row, half = gather_f.piece(i)
        at = rows_of(half)
        return pltpu.make_async_copy(buf.at[:, row, at], f_o.at[:, row, at], fsem.at[i])

    def expand(i, row, half):
        at = rows_of(half)
        keep_f(i).start()
        f0, f1 = buf[0, row, at, :], buf[1, row, at, :]
        dy0, dy1 = dys[0, row, at, :], dys[1, row, at, :]
        gate = nn(f0, wg_o[0]) + nn(f1, wg_o[1])
        upper = nn(f0, wu_o[0]) + nn(f1, wu_o[1])
        d_mid = d_gate[row, at, :].astype(F32)
        sig = 1.0 / (1.0 + jnp.exp(-gate))
        swish = gate * sig
        mid = (swish * upper).astype(BF)
        middle[row, at, :] = mid
        d_gate[row, at, :] = (d_mid * upper * sig * (1.0 + gate * (1.0 - sig))).astype(BF)
        d_up[row, at, :] = (d_mid * swish).astype(BF)
        g0, g1 = tn(mid, dy0), tn(mid, dy1)

        @pl.when(i == 0)
        def _():
            grad[0] = g0
            grad[1] = g1

        @pl.when(i > 0)
        def _():
            grad[0] += g0
            grad[1] += g1

    gather_f.run(expand)
    half = DOWN_CHUNKS // 4

    def swap(j, core):
        return remote(
            give.at[pl.ds(2 * j, 2)], part.at[pl.ds(2 * (half * core + j), 2)], gsend.at[j], grecv.at[j], mate
        )

    for j in range(half):
        for h in range(2):
            give[2 * j + h] = grad[1 - k, j * TALL + h * CHUNK : j * TALL + (h + 1) * CHUNK, :].astype(BF)
        swap(j, k).start()
    for j in range(half):
        for h in range(2):
            rows = slice(j * TALL + h * CHUNK, j * TALL + (h + 1) * CHUNK)
            part[2 * (half * k + j) + h] = grad[k, rows, :].astype(BF)
    for i in range(8):
        keep_f(i).wait()
    for j in range(half):
        swap(j, 1 - k).wait_recv()
    for j in range(half):
        swap(j, k).wait_send()
    for g in gives:
        g.wait_send()
    total.finish()


def front(x, dy, gain, gain_f, wq, wk, wv, wo, wg, wu, wd):
    tokens, width = x.shape
    f_half = wg.shape[1] // 2
    cols = 4 * LANE
    gathered = (2, 4, tokens, width)
    outs = [sds(gathered, BF), sds(gathered, BF)]
    outs += [sds((4, 4 * tokens, LANE), BF), sds((2, LANE, 4 * tokens), BF)]
    outs += [sds((2, width, cols), BF), sds((2, 2 * LANE, width), BF)]
    outs += [sds((2, width, f_half), BF)] * 2 + [sds((2, f_half, width), BF)]
    outs += [sds((LENGTH, LANE), F32)] * 2 + [sds((tokens, LANE), F32)]
    outs += [sds((4, tokens, 2 * LANE), BF), sds((2, 8, 1, PIECE), F32)]
    outs += [sds((tokens, width), F32), sds((tokens, LANE), F32)]
    outs += [sds((4, tokens, f_half), BF)] * 3 + [sds((DOWN_CHUNKS, CHUNK, WIDE), BF)]
    half = DOWN_CHUNKS // 4
    scratch = [pltpu.VMEM(gathered, BF)] * 2 + [pltpu.VMEM((2, 2, PIECE, width), BF)]
    scratch += [pltpu.VMEM((2, 1, width), F32), pltpu.VMEM((width, cols), BF), pltpu.VMEM((2 * LANE, width), BF)]
    scratch += [pltpu.VMEM(w.shape, BF) for w in (wq, wk, wv, wo)]
    scratch += [DMA((6,)), DMA((6,)), DMA((8,)), DMA((8,)), DMA((8,))]
    scratch += [pltpu.VMEM((2, tokens, LANE), F32), DMA((2,)), pltpu.VMEM((2, f_half, width), F32)]
    scratch += [pltpu.VMEM((2 * half, CHUNK, WIDE), BF), DMA((half,)), DMA((half,))]
    scratch += GATHER_SEMS * 3 + sum_scratch(width)
    ins = [ANY] * 2 + [VM] * 2 + [ANY] * 7 + [VM]
    args = [x, dy, gain, gain_f, wq, wk, wv, wo, wg, wu, wd, jnp.asarray(np.stack(angle_tables()))]
    out_specs = [ANY] * 2 + [VM] * (len(outs) - 2)
    return call(front_kernel, 0, outs, ins, args, scratch, 9e10, 60, out_specs)


TICKS = 35


def flat(ref, h, m=None):
    got = ref[h] if m is None else ref[h, :, :, pl.ds(pl.multiple_of(m * 256, 256), 256)]
    return got.reshape(-1, got.shape[-1])


def contract_kernel(
    d_gate, d_up, wg, wu, hidden, rstd2, gain, dy, wo, attn, part_d, f_any,
    d_hidden, gains_o, part, part_o, d_attn, totals, acc_c, tot_c,
    stat, ssem, give, gsend, grecv, gathered, dya, grad, give_o, his_o, gsem, fsem, *rest,
):
    r, k, rx, ry, r3 = place()
    width = hidden.shape[1]
    fetch = pltpu.make_async_copy(f_any, gathered, fsem)
    fetch.start()
    greet(rx, ry, k, True)
    total = Sum(rest[:9])
    gather = Gather(dya, gathered, rest[9:14])
    parts = [(0, DOWN_CHUNKS, part_d), (DOWN_CHUNKS, MLP_CHUNKS, part), (MLP_CHUNKS, OUT_CHUNKS, part_o)]
    line = Line(parts, totals, (acc_c, tot_c), rest[14:], 0, TICKS)
    line.open()

    def compute(row, half):
        at = rows_of(half)
        g, u = d_gate[row, at, :], d_up[row, at, :]
        return nt(g, wg[k]) + nt(u, wu[k]), nt(g, wg[1 - k]) + nt(u, wu[1 - k])

    def early(j):
        @pl.when(j % 2 == 1)
        def _():
            line.step(j // 2)

    total.send_all(compute, early)

    def swap(e, core):
        to = part.at[pl.ds(2 * (e // 4 * 8 + 4 * core + e % 4), 2)]
        return remote(give.at[pl.ds(2 * e, 2)], to, gsend.at[e], grecv.at[e], {"col": 1 - k})

    def wide_part(h, right, dst, first):
        def one(m, carry):
            got = tn(flat(gathered, h, m), right[...].reshape(-1, right.shape[2])).astype(BF)
            for b in range(2):
                lanes = pl.ds(pl.multiple_of((2 * m + b) * TALL, TALL), TALL)
                for j in range(4):
                    for u in range(2):
                        rows = slice(b * TALL + u * CHUNK, b * TALL + (u + 1) * CHUNK)
                        dst[2 * (first + j) + u, :, lanes] = got[rows, j * TALL : (j + 1) * TALL]
            return carry

        lax.fori_loop(0, width // 256, one, 0)

    fetch.wait()
    wide_part(1 - k, d_gate, give, 0)
    for e in range(4):
        swap(e, k).start()
    line.step(4)
    wide_part(k, d_gate, part, 4 * k)
    line.step(5)
    wide_part(1 - k, d_up, give, 4)
    for e in range(4, 8):
        swap(e, k).start()
    line.step(6)
    wide_part(k, d_up, part, 8 + 4 * k)
    line.step(7)
    total.relay(4)
    total.relay(5)
    for e in range(8):
        swap(e, 1 - k).wait_recv()
    for j in range(8, 13):
        line.step(j)
    gains = jnp.zeros((1, width), F32)
    for half in range(2):
        at = rows_of(half)
        d_nf = total.last(6 + half)
        h = hidden[at, :]
        gains = gains + jnp.sum(d_nf * h * rstd2[at, 0:1], 0, keepdims=True)
        scaled = d_nf * gain[...]
        d_hidden[at, :] = scaled
        stat[k, at, :] = jnp.broadcast_to(jnp.sum(scaled * h, 1, keepdims=True), (PIECE, LANE))
    gains_o[...] = gains
    inner = exchange(k, stat, ssem) / (2 * width)
    rs = rstd2[:, 0:1]
    value = dy[...].astype(F32) + rs * d_hidden[...] - hidden[...] * (rs * rs * rs * inner)
    d_hidden[...] = value
    dya[...] = value.astype(BF)
    gather.start()

    def piece(i, row, half):
        at = rows_of(half)
        d0, d1 = gathered[0, row, at, :], gathered[1, row, at, :]
        d_attn[row, at, :] = (nt(d0, wo[0]) + nt(d1, wo[1])).astype(BF)
        a = attn[row, at, :]
        g0, g1 = tn(a, d0), tn(a, d1)

        @pl.when(i == 0)
        def _():
            grad[0] = g0
            grad[1] = g1

        @pl.when(i > 0)
        def _():
            grad[0] += g0
            grad[1] += g1

    def before(q):
        @pl.when(q == 0)
        def _():
            for j in range(13, 15):
                line.step(j)

        for j in range(3):
            line.step(15 + 4 * q + j)

    def after(q):
        line.step(18 + 4 * q)

    gather.run(piece, before, after)
    give_o[...] = grad[1 - k].astype(BF)
    give_out = remote(give_o, his_o, gsem.at[0], gsem.at[1], {"col": 1 - k})
    give_out.start()
    q_cols = part_o.shape[0] * CHUNK
    mine = nn(spread(q_cols, 2 * LANE, k * (q_cols // 2)), grad[k].astype(BF))
    give_out.wait_recv()
    out = mine + nn(spread(q_cols, 2 * LANE, (1 - k) * (q_cols // 2)), his_o[...])
    for c in range(q_cols // CHUNK):
        part_o[c] = out[c * CHUNK : (c + 1) * CHUNK].astype(BF)
    line.rest(31)
    for e in range(8):
        swap(e, k).wait_send()
    give_out.wait_send()
    total.finish()


def contract(d_gate, d_up, wg, wu, hidden, rstd2, gain, dy, wo, attn, part_d, all_f):
    tokens, width = hidden.shape
    n = lax.axis_size("dp")
    outs = [sds((tokens, width), F32), sds((1, width), F32)]
    outs += [sds((MLP_CHUNKS - DOWN_CHUNKS, CHUNK, WIDE), BF), sds((OUT_CHUNKS - MLP_CHUNKS, CHUNK, WIDE), BF)]
    outs += [sds((4, tokens, 2 * LANE), BF)] + line_outs(TICKS)
    out_specs = [VM] * 5 + [ANY] + [VM] * 2
    scratch = [pltpu.VMEM((2, tokens, LANE), F32), DMA((2,))]
    scratch += [pltpu.VMEM((16, CHUNK, WIDE), BF), DMA((8,)), DMA((8,))]
    scratch += [pltpu.VMEM((2, 4, tokens, width), BF), pltpu.VMEM((tokens, width), BF)]
    scratch += [pltpu.VMEM((2, 2 * LANE, width), F32)] + [pltpu.VMEM((2 * LANE, width), BF)] * 2
    scratch += [DMA((2,)), DMA]
    scratch += sum_scratch(width) + GATHER_SEMS + line_scratch(n, TICKS)
    args = [d_gate, d_up, wg, wu, hidden, rstd2, gain, dy, wo, attn, part_d, all_f]
    ins = [VM] * 11 + [ANY]
    return call(contract_kernel, 3, outs, ins, args, scratch, 5e10, vmem_limit(n), out_specs)


def vmem_limit(n):
    return 60 if n <= 4 else 63


def columns(rows, cols, core, q_cols, k_cols):
    i = lax.broadcasted_iota(jnp.int32, (rows, cols), 0)
    at = lax.broadcasted_iota(jnp.int32, (rows, cols), 1)
    part, lane = i // LANE, i % LANE
    index = jnp.where(lane < HALF, lane, lane - (LANE // 2 - HALF))
    q = core * (q_cols // 2) + part * HD
    kv = q_cols + (part - 2) * k_cols + core * (k_cols // 2)
    to = jnp.where(part < 2, q, kv) + index
    pad = lane % (LANE // 2) >= HALF
    return jnp.where((at == to) & (pad == False), 1.0, 0.0).astype(BF)


def backward_kernel(
    q_cols, k_cols,
    qkv, kvt, lse, d_attn, cos, sin, middle, wd, hidden, wqkv, x, rstd1, d_hidden, gain, gains_f,
    part_m, part_o, acc_c, tot_c, normed_any,
    output, grad_x, gains_o, totals,
    dk, dv, d_proj, normed, part, mine, give, his, gsem, stat, ssem, free, fsem,
    mine_g, pair_g, slots, gsend, grecv, *rest,
):
    r, k, rx, ry, r3 = place()
    width = x.shape[1]
    n = lax.axis_size("dp")
    z = lax.axis_index("dp")
    fetch = pltpu.make_async_copy(normed_any, normed, fsem)
    fetch.start()
    greet(rx, ry, k, True, True)
    sums = rest[:5]
    down = Sum(sums + rest[5:9])
    into = Sum(sums + rest[9:13])
    ticks = line_ticks(n) - TICKS
    parts = [(DOWN_CHUNKS, MLP_CHUNKS, part_m), (MLP_CHUNKS, OUT_CHUNKS, part_o), (OUT_CHUNKS, ALL_CHUNKS, part)]
    line = Line(parts, totals, None, rest[13:], TICKS, ticks, (acc_c, tot_c))
    line.open()

    def down_piece(row, half):
        m = middle[row, rows_of(half), :]
        return nn(m, wd[k]), nn(m, wd[1 - k])

    def early(j):
        @pl.when(j % 3 == 1)
        def _():
            line.step(j // 3)

    down.send_all(down_piece, early)

    def unrotate(u, p):
        at = pl.ds(p * PIECE, PIECE)
        return u * cos[at, :] - pltpu.roll(u, LANE // 2, 1) * sin[at, :]

    def sequence(seq):
        base = pl.multiple_of(seq * LENGTH, LENGTH)

        def one_head(head, carry):
            for p in range(4):
                span = PIECE * (p + 1)
                row = seq * 2 + p // 2
                at = pl.ds((p % 2) * PIECE, PIECE)
                out = pl.ds(pl.multiple_of(base + p * PIECE, PIECE), PIECE)
                keys = qkv[2, pl.ds(base, span), :]
                q = qkv[head, out, :]
                lane = pl.ds(pl.multiple_of(head * LANE, LANE), LANE)
                do = d_attn[row, at, lane]
                e = jnp.exp(nt(keys, q) * SCALE - lse[head, seq * 4 + p])
                tail = jnp.where(causal((PIECE, PIECE)), e[span - PIECE :], 0.0)
                e = tail if p == 0 else jnp.concatenate([e[: span - PIECE], tail], 0)
                dp = nt(qkv[3, pl.ds(base, span), :], do)
                inner = jnp.sum(e * dp, 0, keepdims=True)
                ds = (e * (dp - inner)).astype(BF)
                dv[0:span, :] += nn(e.astype(BF), do)
                dk[0:span, :] += nn(ds, q)
                dq = nn(kvt[0, :, pl.ds(base, span)], ds).T * SCALE
                d_proj[out, lane] = unrotate(dq, p).astype(BF)
                tick = 3 + seq * 8 + head * 4 + p

                @pl.when(tick < OUT_CHUNKS - LAG - TICKS)
                def _(tick=tick):
                    line.step(tick)

            return carry

        dk[...] = jnp.zeros_like(dk)
        dv[...] = jnp.zeros_like(dv)
        lax.fori_loop(0, 2, one_head, 0)
        for p in range(4):
            at = pl.ds(p * PIECE, PIECE)
            out = pl.ds(pl.multiple_of(base + p * PIECE, PIECE), PIECE)
            d_proj[out, 2 * LANE : 3 * LANE] = unrotate(dk[at, :] * SCALE, p).astype(BF)
            d_proj[out, 3 * LANE : 4 * LANE] = dv[at, :].astype(BF)

    def both(seq, carry):
        sequence(seq)

        @pl.when(seq == 0)
        def _():
            down.relay(4)
            down.relay(5)

        return carry

    lax.fori_loop(0, 2, both, 0)
    for half in range(2):
        at = rows_of(half)
        output[at, :] = hidden[at, :] + down.last(6 + half)
    down.finish()
    for device in ({"row": rx}, {"row": ry}, {"col": 1 - k}):
        pl.semaphore_signal(free, inc=1, device_id=device, device_id_type=MESH)
    pl.semaphore_wait(free, 3)

    fetch.wait()

    def in_part(h, dst):
        def one(m, carry):
            dst[pl.ds(pl.multiple_of(m * 256, 256), 256), :] = tn(flat(normed, h, m), d_proj[...]).astype(BF)
            return carry

        lax.fori_loop(0, width // 256, one, 0)

    in_part(1 - k, give)
    swap = remote(give, his, gsem.at[0], gsem.at[1], {"col": 1 - k})
    swap.start()
    in_part(k, mine)
    cols = q_cols + 2 * k_cols
    got = nn(mine[...], columns(4 * LANE, cols, k, q_cols, k_cols))
    swap.wait_recv()
    got = got + nn(his[...], columns(4 * LANE, cols, 1 - k, q_cols, k_cols))
    for c in range(width // CHUNK):
        part[c] = got[c * CHUNK : (c + 1) * CHUNK].astype(BF)

    def into_piece(row, half):
        d = d_proj[pl.ds(pl.multiple_of(row * 2 * PIECE + half * PIECE, PIECE), PIECE), :]
        return nt(d, wqkv[k]), nt(d, wqkv[1 - k])

    def beside(j):
        @pl.when(j % 2 == 1)
        def _():
            line.step(17 + j // 2)

    into.send_all(into_piece, beside)
    for j in range(21, 24):
        line.step(j)
    into.relay(4)
    into.relay(5)
    for j in range(24, 29):
        line.step(j)
    gains = jnp.zeros((1, width), F32)
    for half in range(2):
        at = rows_of(half)
        d_na = into.last(6 + half)
        xs = x[at, :].astype(F32)
        gains = gains + jnp.sum(d_na * xs * rstd1[at, 0:1], 0, keepdims=True)
        scaled = d_na * gain[...]
        grad_x[at, :] = scaled
        stat[k, at, :] = jnp.broadcast_to(jnp.sum(scaled * xs, 1, keepdims=True), (PIECE, LANE))

    def row_total(step, device):
        copy = remote(mine_g.at[step], pair_g.at[step], gsend.at[n + step], grecv.at[n + step], {"row": device})
        copy.start()
        return copy

    mine_g[0, 0:1] = gains
    mine_g[0, 1:2] = gains_f[...]
    over_x = row_total(0, rx)
    inner = exchange(k, stat, ssem) / (2 * width)
    rs = rstd1[:, 0:1]
    over_x.wait_recv()
    mine_g[1] = mine_g[0] + pair_g[0]
    over_y = row_total(1, ry)
    grad_x[...] = d_hidden[...] + rs * grad_x[...] - x[...].astype(F32) * (rs * rs * rs * inner)
    over_y.wait_recv()
    slots[z] = mine_g[1] + pair_g[1]

    def over_dp(t, mine):
        other = (z + t) % n
        g = z if mine else other
        return remote(slots.at[g], slots.at[g], gsend.at[t], grecv.at[g], {"dp": other})

    def start(t, carry):
        over_dp(t, True).start()
        return carry

    lax.fori_loop(1, n, start, 0)
    line.rest(29)

    def wait(t, carry):
        over_dp(t, False).wait_recv()
        over_dp(t, True).wait_send()
        return carry

    lax.fori_loop(1, n, wait, 0)
    gains_o[...] = lax.fori_loop(1, n, lambda g, total: total + slots[g], slots[0])
    over_x.wait_send()
    over_y.wait_send()
    swap.wait_send()
    into.finish()


def backward(
    qkv, kvt, lse, d_attn, cos, sin, middle, wd, hidden, wqkv, x, rstd1, d_hidden, gain, gains_f,
    part_m, part_o, acc, tot, normed, q_cols, k_cols,
):
    tokens, width = x.shape
    n = lax.axis_size("dp")
    ticks = line_ticks(n) - TICKS
    outs = [sds((tokens, width), F32)] * 2 + [sds((2, width), F32), sds((ticks, CHUNK, WIDE), BF)]
    scratch = [pltpu.VMEM((LENGTH, LANE), F32)] * 2 + [pltpu.VMEM((4 * tokens, 4 * LANE), BF)]
    scratch += [pltpu.VMEM((2, 4, tokens, width), BF), pltpu.VMEM((ALL_CHUNKS - OUT_CHUNKS, CHUNK, WIDE), BF)]
    scratch += [pltpu.VMEM((width, 4 * LANE), BF)] * 3 + [DMA((2,))]
    scratch += [pltpu.VMEM((2, tokens, LANE), F32), DMA((2,)), pltpu.SemaphoreType.REGULAR, DMA]
    scratch += [pltpu.VMEM((2, 2, width), F32)] * 2 + [pltpu.VMEM((n, 2, width), F32)]
    scratch += [DMA((n + 2,)), DMA((n + 2,))]
    both = sum_scratch(width)
    scratch += both + both[5:] + line_scratch(n, ticks)
    args = [qkv, kvt, lse, d_attn, cos, sin, middle, wd, hidden, wqkv, x, rstd1, d_hidden, gain, gains_f]
    args += [part_m, part_o, acc, tot, normed]
    kernel = functools.partial(backward_kernel, q_cols, k_cols)
    ins = [VM] * (len(args) - 1) + [ANY]
    return call(kernel, 5, outs, ins, args, scratch, 5e10, vmem_limit(n), [VM] * 3 + [ANY])


def unpack_kernel(ticks, q_cols, k_cols, *rest):
    tots, (down, gate, up, out, q_o, k_o, v_o), rest = rest[: len(ticks)], rest[len(ticks) : len(ticks) + 7], rest[len(ticks) + 7 :]
    chunks, wide, parts, isem, osem = rest
    n, s, _, _ = line_place()
    mid = n // 2
    off = LAG * (2 * mid - 2 - s)
    offs = [LAG * o for o in range(mid - 1, 2 * mid - 1)]

    def source(t):
        for tot, count in zip(tots, ticks):
            if t < count:
                return tot.at[t]
            t -= count

    def load(c):
        for o in offs:

            @pl.when(off == o)
            def _(o=o):
                for u in range(2):
                    dst = chunks.at[c % 4, pl.ds(u * CHUNK, CHUNK)]
                    pltpu.make_async_copy(source(2 * c + u + o), dst, isem.at[c % 4, u]).start()

    def stored(c):
        slot = c % 4
        buf = wide.at[slot]
        if c < 8:
            return [pltpu.make_async_copy(buf, down.at[pl.ds(c * TALL, TALL)], osem.at[slot, 0])]
        if c < MLP_CHUNKS // 2:
            to, lanes = (gate, up)[c // 8 - 1], pl.ds(c % 8 * TALL, TALL)
            return [
                pltpu.make_async_copy(
                    buf.at[:, pl.ds(b * TALL, TALL)], to.at[pl.ds(b * TALL, TALL), lanes], osem.at[slot, b]
                )
                for b in range(WIDE // TALL)
            ]
        if c < OUT_CHUNKS // 2:
            return [pltpu.make_async_copy(buf, out.at[pl.ds((c - MLP_CHUNKS // 2) * TALL, TALL)], osem.at[slot, 0])]
        rows = pl.ds((c - OUT_CHUNKS // 2) * TALL, TALL)
        return [
            pltpu.make_async_copy(buf.at[:, pl.ds(0, q_cols)], q_o.at[rows], osem.at[slot, 0]),
            pltpu.make_async_copy(parts.at[0, slot], k_o.at[:, rows], osem.at[slot, 1]),
            pltpu.make_async_copy(parts.at[1, slot], v_o.at[:, rows], osem.at[slot, 2]),
        ]

    for c in range(3):
        load(c)
    for c in range(ALL_CHUNKS // 2):
        if c + 3 < ALL_CHUNKS // 2:
            load(c + 3)
        if c >= 4:
            for copy in stored(c - 4):
                copy.wait()
        for u in range(2):
            dst = chunks.at[c % 4, pl.ds(u * CHUNK, CHUNK)]
            pltpu.make_async_copy(dst, dst, isem.at[c % 4, u]).wait()
        value = chunks[c % 4].astype(F32)
        wide[c % 4] = value
        if c >= OUT_CHUNKS // 2:
            parts[0, c % 4] = value[:, q_cols : q_cols + k_cols].T
            parts[1, c % 4] = value[:, q_cols + k_cols :].T
        for copy in stored(c):
            copy.start()
    for c in range(ALL_CHUNKS // 2 - 4, ALL_CHUNKS // 2):
        for copy in stored(c):
            copy.wait()


def unpack(tots, q_cols, k_cols):
    n = lax.axis_size("dp")
    ticks = [TICKS, line_ticks(n) - TICKS]
    outs = [sds((8 * TALL, WIDE), F32), sds((WIDE, 8 * TALL), F32), sds((WIDE, 8 * TALL), F32)]
    outs += [sds((q_cols, WIDE), F32), sds((WIDE, q_cols), F32), sds((k_cols, WIDE), F32), sds((k_cols, WIDE), F32)]
    moved = 6 * ALL_CHUNKS // 2 * TALL * WIDE
    return pl.pallas_call(
        functools.partial(unpack_kernel, ticks, q_cols, k_cols),
        out_shape=outs,
        in_specs=[ANY] * len(tots),
        out_specs=[ANY] * len(outs),
        scratch_shapes=[
            pltpu.VMEM((4, TALL, WIDE), BF),
            pltpu.VMEM((4, TALL, WIDE), F32),
            pltpu.VMEM((2, 4, k_cols, TALL), F32),
            DMA((4, 2)),
            DMA((4, WIDE // TALL)),
        ],
        compiler_params=pltpu.CompilerParams(vmem_limit_bytes=16 << 20),
        cost_estimate=pl.CostEstimate(flops=0, bytes_accessed=moved, transcendentals=0),
    )(*tots)


def on_device(
    layer_input, gain_attn, gain_ffn, w_query, w_key, w_value, w_out, w_gate, w_up, w_down, cotangent
):
    tokens, width = layer_input.shape
    q_cols, k_cols = w_query.shape[1], w_key.shape[1]
    gain_a, gain_f = gain_attn[None], gain_ffn[None]
    (
        normed, all_f, qkv, kvt, wqkv, wo, wg, wu, wd, cos, sin, rstd1,
        attn, lse, hidden, rstd2, middle, d_gate, d_up, part_d,
    ) = front(
        layer_input, cotangent, gain_a, gain_f,
        w_query, w_key.T, w_value.T, w_out, w_gate, w_up, w_down,
    )
    d_hidden, gains_f, part_m, part_o, d_attn, tot1, acc, tot = contract(
        d_gate, d_up, wg, wu, hidden, rstd2, gain_f, cotangent, wo, attn, part_d, all_f
    )
    output, grad_x, gains, tot2 = backward(
        qkv, kvt, lse, d_attn, cos, sin, middle, wd, hidden, wqkv, layer_input, rstd1, d_hidden,
        gain_a, gains_f, part_m, part_o, acc, tot, normed, q_cols, k_cols,
    )
    down, gate, up, out, g_q, g_k, g_v = unpack([tot1, tot2], q_cols, k_cols)
    return output, grad_x, gains[0], gains[1], g_q, g_k.T, g_v.T, out, gate, up, down


def solution(mesh):
    assert mesh.shape["row"] == 4 and mesh.shape["col"] == 2
    tokens = P(("dp", "row"), "col")
    wide = P("col", "row")
    tall = P("row", "col")
    return jax.shard_map(
        on_device,
        mesh=mesh,
        in_specs=(tokens, P("col"), P("col"), wide, wide, wide, tall, wide, wide, tall, tokens),
        out_specs=(tokens, tokens, P("col"), P("col"), wide, wide, wide, tall, wide, wide, tall),
        check_vma=False,
    )
```

```python
import functools

import jax
import jax.numpy as jnp
import numpy as np
from jax import lax
from jax.experimental import pallas as pl
from jax.experimental.pallas import tpu as pltpu
from jax.sharding import PartitionSpec as P

HD = 96
HALF = HD // 2
LENGTH = 1024
EPS = 1e-05
THETA = 100000.0
SCALE = HD ** (-0.5)
LANE = 128
PIECE = 256

BF = jnp.bfloat16
F32 = jnp.float32
MESH = pl.DeviceIdType.MESH
VM = pl.BlockSpec(memory_space=pltpu.VMEM)
ANY = pl.BlockSpec(memory_space=pl.ANY)
DMA = pltpu.SemaphoreType.DMA


def nn(a, b):
    return lax.dot_general(a, b, (((1,), (0,)), ((), ())), preferred_element_type=F32)


def nt(a, b):
    return lax.dot_general(a, b, (((1,), (1,)), ((), ())), preferred_element_type=F32)


def place():
    r = lax.axis_index("row")
    k = lax.axis_index("col")
    return r, k, r + 1 - 2 * (r % 2), (r + 2) % 4, 3 - r


def tn(a, b):
    return lax.dot_general(a, b, (((0,), (0,)), ((), ())), preferred_element_type=F32)


def line_place():
    n = lax.axis_size("dp")
    z = lax.axis_index("dp")
    left = z < n // 2
    step = jnp.where(left, 1, -1)
    return n, jnp.where(left, z, n - 1 - z), z + step, z - step


def greet(rx, ry, k, line=False, groups=False):
    bar = pltpu.get_barrier_semaphore()

    def hello(device):
        pl.semaphore_signal(bar, inc=1, device_id=device, device_id_type=MESH)

    for device in ({"row": rx}, {"row": ry}, {"col": 1 - k}):
        hello(device)
    if not line:
        pl.semaphore_wait(bar, 3)
        return
    n, s, inward, outward = line_place()
    if groups:
        z = lax.axis_index("dp")

        def one(t, carry):
            hello({"dp": (z + t) % n})
            return carry

        lax.fori_loop(1, n, one, 0)
        pl.semaphore_wait(bar, 3 + n - 1)
        return
    hello({"dp": inward})

    @pl.when(s > 0)
    def _():
        hello({"dp": outward})

    pl.semaphore_wait(bar, jnp.where(s > 0, 5, 4))


def remote(src, dst, send, recv, device):
    return pltpu.make_async_remote_copy(
        src_ref=src, dst_ref=dst, send_sem=send, recv_sem=recv, device_id=device, device_id_type=MESH
    )


def rows_of(half):
    return pl.ds(pl.multiple_of(half * PIECE, PIECE), PIECE)


GATHER_SEMS = [DMA((6,)), DMA((6,)), DMA((8,)), DMA((8,)), DMA]


class Gather:
    def __init__(self, own, buf, sems):
        self.own, self.buf = own, buf
        self.isend, self.irecv, self.dsend, self.drecv, self.lsem = sems
        self.r, self.k, self.rx, self.ry, self.r3 = place()

    def piece(self, i):
        side = jnp.where(i % 2 == 0, self.rx, self.ry)
        row = jnp.where(i < 2, self.r, jnp.where(i < 6, side, self.r3))
        half = jnp.where(i // 2 == 2, 1 - i % 2, i % 2)
        return row, half

    def ici(self, sem, row, half, device, src=None):
        dst = self.buf.at[self.k, row, rows_of(half)]
        return remote(dst if src is None else src, dst, self.isend.at[sem], self.irecv.at[sem], {"row": device})

    def pair(self, i, core, row, half, src=None):
        dst = self.buf.at[core, row, rows_of(half)]
        return remote(dst if src is None else src, dst, self.dsend.at[i], self.drecv.at[i], {"col": 1 - self.k})

    def local(self):
        return pltpu.make_async_copy(self.own, self.buf.at[self.k, self.r], self.lsem)

    def start(self):
        own = self.buf.at[self.k, self.r] if self.own is None else self.own
        first, second = own.at[pl.ds(0, PIECE)], own.at[pl.ds(PIECE, PIECE)]
        self.ici(0, self.r, 0, self.rx, first).start()
        self.ici(1, self.r, 1, self.ry, second).start()
        self.ici(2, self.r, 1, self.rx, second).start()
        self.ici(3, self.r, 0, self.ry, first).start()
        self.pair(0, self.k, self.r, 0, first).start()
        self.pair(1, self.k, self.r, 1, second).start()
        if self.own is not None:
            self.local().start()

    def arrive(self, i):
        row, half = self.piece(i)
        self.ici(i - 2, row, half, self.rx).wait_recv()

        @pl.when(i == 2)
        def _():
            self.ici(4, row, half, self.ry).start()

        @pl.when(i == 3)
        def _():
            self.ici(5, row, half, self.rx).start()

        self.pair(i, self.k, row, half).start()

    def ready(self, i):
        row, half = self.piece(i)
        self.pair(i, 1 - self.k, row, half).wait_recv()

    def run(self, compute, before=None, after=None):
        if self.own is not None:
            self.local().wait()

        def pair(q, carry):
            for u in range(2):
                i = 2 * q + u
                self.ready(i)
                row, half = self.piece(i)
                compute(i, row, half)
            if before is not None:
                before(q)

            @pl.when(q < 3)
            def _():
                self.arrive(2 * q + 2)
                self.arrive(2 * q + 3)

            if after is not None:
                after(q)
            return carry

        lax.fori_loop(0, 4, pair, 0)
        self.finish()

    def finish(self):
        for i in range(6):
            self.ici(i, self.r, 0, self.rx).wait_send()
        for i in range(8):
            self.pair(i, self.k, self.r, 0).wait_send()


def sum_scratch(width):
    return [
        pltpu.VMEM((4, PIECE, width), F32),
        pltpu.VMEM((4, PIECE, width), BF),
        pltpu.VMEM((8, PIECE, width), BF),
        pltpu.VMEM((6, PIECE, width), BF),
        pltpu.VMEM((6, PIECE, width), BF),
        DMA((8,)),
        DMA((8,)),
        DMA((6,)),
        DMA((6,)),
    ]


class Sum:
    def __init__(self, scratch):
        self.own, self.ds, self.dr, self.ist, self.irt = scratch[:5]
        self.dsend, self.drecv, self.isend, self.irecv = scratch[5:]
        self.r, self.k, self.rx, self.ry, self.r3 = place()

    def piece(self, j):
        mid = jnp.where(j == 2, self.ry, jnp.where(j == 5, self.ry, self.rx))
        row = jnp.where(j < 2, self.r3, jnp.where(j < 6, mid, self.r))
        return row, j % 2

    def pair(self, j):
        return remote(self.ds.at[j % 4], self.dr.at[j], self.dsend.at[j], self.drecv.at[j], {"col": 1 - self.k})

    def ici(self, j):
        device = jnp.where(j == 0, self.ry, jnp.where(j == 2, self.ry, jnp.where(j == 5, self.ry, self.rx)))
        return remote(self.ist.at[j], self.irt.at[j], self.isend.at[j], self.irecv.at[j], {"row": device})

    def put(self, j, kept, given):
        @pl.when(j >= 4)
        def _():
            self.pair(j - 4).wait_send()

        self.own[j % 4] = kept
        self.ds[j % 4] = given.astype(BF)
        self.pair(j).start()

    def chip(self, j):
        self.pair(j).wait_recv()
        return self.own[j % 4] + self.dr[j].astype(F32)

    def forward(self, j):
        self.ist[j] = self.chip(j).astype(BF)
        self.ici(j).start()

    def relay(self, j):
        value = self.chip(j)
        self.ici(j - 4).wait_recv()
        self.ist[j] = (value + self.irt[j - 4].astype(F32)).astype(BF)
        self.ici(j).start()

    def last(self, j):
        value = self.chip(j)
        self.ici(j - 4).wait_recv()
        value = value + self.irt[j - 4].astype(F32)
        self.ici(j - 2).wait_recv()
        return value + self.irt[j - 2].astype(F32)

    def send_all(self, compute, hook=None):
        def step(j, carry):
            row, half = self.piece(j)
            kept, given = compute(row, half)
            self.put(j, kept, given)

            @pl.when(j > 0)
            def _():
                @pl.when(j < 5)
                def _():
                    self.forward(j - 1)

            if hook is not None:
                hook(j)
            return carry

        lax.fori_loop(0, 8, step, 0)

    def finish(self):
        for j in range(4, 8):
            self.pair(j).wait_send()
        for j in range(6):
            self.ici(j).wait_send()


TALL, WIDE = 128, 768
CHUNK = TALL // 2
DOWN_CHUNKS, MLP_CHUNKS, OUT_CHUNKS, ALL_CHUNKS = 16, 48, 54, 66
RING = 6
LAG = 2


def line_ring(n):
    return LAG * (2 * (n // 2) - 2) + 6


def line_ticks(n):
    return ALL_CHUNKS + LAG * (2 * (n // 2) - 2)


def line_outs(ticks):
    return [sds((ticks, CHUNK, WIDE), BF)] + [sds((LAG, CHUNK, WIDE), BF)] * 2


def line_scratch(n, ticks):
    slots = (RING, line_ring(n), line_ring(n), RING)
    return [pltpu.VMEM((count, CHUNK, WIDE), BF) for count in slots] + [DMA((ticks,))] * 6


class Line:
    def __init__(self, parts, totals, carry, scratch, first, ticks, before=None):
        self.parts, self.totals, self.carry = parts, totals, carry
        self.acc, self.tot, self.rin, self.rxb = scratch[:4]
        self.si, self.ri, self.rx, self.so, self.ro, self.out_sem = scratch[4:]
        self.first, self.ticks = first, ticks
        self.n, self.s, self.inward, self.outward = line_place()
        self.mid = self.n // 2
        self.ring = line_ring(self.n)
        if before is not None:

            @pl.when(self.s > 0)
            def _():
                for b in range(LAG):
                    self.acc[b] = before[0][b]
                    self.tot[b] = before[1][b]

    def valid(self, c):
        return (c >= 0) & (c < ALL_CHUNKS)

    def sends(self, j):
        s, mid, slot, near = self.s, self.mid, j % self.ring, j % RING
        to = {"dp": self.inward}
        c = self.first + j - LAG * s
        moves = []
        inward = (self.rin.at[slot], self.ri.at[j])
        across = (self.rxb.at[near], self.rx.at[j])
        for lo, hi, ref in self.parts:
            ok = (s == 0) & (c >= lo) & (c < hi)
            moves.append((ok, ref, c - lo, across if mid == 1 else inward))
        if mid > 1:
            ok = self.valid(c)
            moves.append((ok & (s == mid - 1), self.acc, near, across))
            if mid > 2:
                moves.append((ok & (s > 0) & (s < mid - 1), self.acc, near, inward))
        out = [
            (cond, lambda ref=ref, at=at, way=way: remote(ref.at[at], way[0], self.si.at[j], way[1], to))
            for cond, ref, at, way in moves
        ]
        if mid > 1:
            c = self.first + j - LAG * (2 * mid - 1 - s)
            out.append(((s > 0) & self.valid(c), lambda: self.outer(j)))
        return out

    def outer(self, j):
        return remote(
            self.tot.at[j % self.ring], self.tot.at[(j + LAG) % self.ring],
            self.so.at[j], self.ro.at[j], {"dp": self.outward},
        )

    def begin(self, j):
        for cond, copy in self.sends(j):

            @pl.when(cond)
            def _(copy=copy):
                copy().start()

    def total_of(self, j):
        copy = lambda: pltpu.make_async_copy(
            self.tot.at[(j + LAG) % self.ring], self.totals.at[j], self.out_sem.at[j]
        )
        return self.valid(self.first + j - LAG * (2 * self.mid - 2 - self.s)), copy

    def settle(self, j):
        for cond, copy in self.sends(j):

            @pl.when(cond)
            def _(copy=copy):
                copy().wait_send()

        cond, copy = self.total_of(j)

        @pl.when(cond)
        def _():
            copy().wait()

    def end(self, j):
        t, s, mid = self.first + j, self.s, self.mid
        slot, later = j % self.ring, (j + LAG) % self.ring
        near, next_near = j % RING, (j + LAG) % RING

        @pl.when(j >= 2)
        def _():
            self.settle(j - 2)

        def came(buf, at, sem):
            remote(buf.at[at], buf.at[at], self.si.at[j], sem.at[j], {"dp": self.inward}).wait_recv()

        def add_part(c, buf, at, dst, to):
            for lo, hi, ref in self.parts:

                @pl.when((c >= lo) & (c < hi))
                def _(ref=ref, lo=lo):
                    dst[to] = (ref[c - lo].astype(F32) + buf[at].astype(F32)).astype(BF)

        if mid > 1:
            c = t - LAG * (s - 1)

            @pl.when((s > 0) & self.valid(c))
            def _():
                came(self.rin, slot, self.ri)
                add_part(c, self.rin, slot, self.acc, next_near)

        @pl.when((s == mid - 1) & self.valid(t - LAG * (mid - 1)))
        def _():
            came(self.rxb, near, self.rx)
            if mid > 1:
                self.tot[later] = (self.acc[near].astype(F32) + self.rxb[near].astype(F32)).astype(BF)
            else:
                add_part(t, self.rxb, near, self.tot, later)

        cond, copy = self.total_of(j)
        if mid > 1:

            @pl.when((s < mid - 1) & cond)
            def _():
                self.outer(j).wait_recv()

        @pl.when(cond)
        def _():
            copy().start()

    def open(self):
        def one(j, carry):
            self.begin(j)
            return carry

        lax.fori_loop(0, min(LAG, self.ticks), one, 0)

    def step(self, j):
        self.end(j)

        @pl.when(j + LAG < self.ticks)
        def _():
            self.begin(j + LAG)

    def steps(self, start, stop):
        def one(t, carry):
            self.step(t)
            return carry

        lax.fori_loop(start, stop, one, 0)

    def rest(self, j):
        self.steps(j, self.ticks)

        def settle(t, carry):
            self.settle(t)
            return carry

        lax.fori_loop(max(self.ticks - 2, 0), self.ticks, settle, 0)
        if self.carry is not None:
            for b in range(LAG):
                self.carry[0][b] = self.acc[(self.ticks + b) % RING]
                self.carry[1][b] = self.tot[(self.ticks + b) % self.ring]


class Io:
    def __init__(self):
        self.coming, self.later, self.going = [], [], []

    def more(self):
        for entry in self.later:
            entry[1].start()
        self.coming += self.later
        self.later = []

    def need(self, *bufs):
        for buf in bufs:
            for at, (ref, copy) in enumerate(self.coming):
                if ref is buf:
                    copy.wait()
                    del self.coming[at]
                    break

    def spill(self, *bufs):
        for buf in bufs:
            for entry in self.going:
                if entry[0] is buf and not entry[2]:
                    entry[1].start()
                    entry[2] = True

    def finish(self):
        self.more()
        self.need(*[ref for ref, _ in self.coming])
        self.spill(*[entry[0] for entry in self.going])
        for _, copy, _ in self.going:
            copy.wait()


def staged(kernel, n_in, fetch, spill, early):
    def wrapped(*refs):
        refs, sems = list(refs[:-1]), refs[-1]
        count = len(fetch) + len(spill)
        refs, bufs = refs[:-count], refs[-count:]
        io = Io()
        for n, i in enumerate(fetch):
            copy = pltpu.make_async_copy(refs[i], bufs[n], sems.at[n])
            if n < early:
                copy.start()
            (io.coming if n < early else io.later).append((bufs[n], copy))
            refs[i] = bufs[n]
        for n, o in enumerate(spill, len(fetch)):
            io.going.append([bufs[n], pltpu.make_async_copy(bufs[n], refs[n_in + o], sems.at[n]), False])
            refs[n_in + o] = bufs[n]
        kernel(io, *refs)
        io.finish()

    return wrapped


def call(kernel, cid, outs, ins, args, scratch, flops, vmem, out_specs, fetch, spill, early=0):
    moved = sum(int(np.prod(a.shape)) * a.dtype.itemsize for a in list(args) + list(outs))
    ins, out_specs = list(ins), list(out_specs)
    held = [pltpu.VMEM(args[i].shape, args[i].dtype) for i in fetch]
    held += [pltpu.VMEM(outs[o].shape, outs[o].dtype) for o in spill]
    for i in fetch:
        ins[i] = ANY
    for o in spill:
        out_specs[o] = ANY
    return pl.pallas_call(
        staged(kernel, len(args), fetch, spill, early),
        out_shape=outs,
        in_specs=ins,
        out_specs=out_specs,
        scratch_shapes=list(scratch) + held + [DMA((len(held),))],
        compiler_params=pltpu.CompilerParams(
            collective_id=cid, has_side_effects=True, vmem_limit_bytes=vmem << 20
        ),
        cost_estimate=pl.CostEstimate(flops=int(flops), bytes_accessed=moved, transcendentals=0),
    )(*args)


def sds(shape, dtype):
    return jax.ShapeDtypeStruct(shape, dtype)


def head_index(iota):
    head, lane = iota // LANE, iota % LANE
    index = jnp.where(lane < HALF, lane, lane - (LANE // 2 - HALF))
    pad = lane % (LANE // 2) >= HALF
    return jnp.where(pad, -1, head * HD + index)


def spread(rows, cols, first):
    source = head_index(lax.broadcasted_iota(jnp.int32, (rows, cols), 1))
    at = lax.broadcasted_iota(jnp.int32, (rows, cols), 0)
    return jnp.where((source >= 0) & (at == source + first), 1.0, 0.0).astype(BF)


def spread_t(rows, cols, first):
    source = head_index(lax.broadcasted_iota(jnp.int32, (rows, cols), 0))
    at = lax.broadcasted_iota(jnp.int32, (rows, cols), 1)
    return jnp.where((source >= 0) & (at == source + first), 1.0, 0.0).astype(BF)


def angle_tables():
    lane = np.arange(LANE)
    freq = np.where(
        lane % (LANE // 2) < HALF, THETA ** (-2.0 * (lane % (LANE // 2)) / HD), 0.0
    )
    fine = np.arange(32)[:, None] * freq[None]
    coarse = fine * 32.0
    return [f(t).astype(np.float32) for t in (coarse, fine) for f in (np.cos, np.sin)]


def exchange(k, stat, sems):
    copy = remote(stat.at[k], stat.at[k], sems.at[0], sems.at[1], {"col": 1 - k})
    copy.start()
    remote(stat.at[1 - k], stat.at[1 - k], sems.at[0], sems.at[1], {"col": 1 - k}).wait_recv()
    copy.wait_send()
    return stat[0][:, 0:1] + stat[1][:, 0:1]


def causal(shape):
    return lax.broadcasted_iota(jnp.int32, shape, 0) <= lax.broadcasted_iota(jnp.int32, shape, 1)


def front_kernel(
    io,
    x, dy, gain, gain_f, wq_h, wk_h, wv_h, wo_h, wg, wu, wd, tables,
    normed_o, f_o, qkv, kvt, wqkv_o, wo_o, wg_o, wu_o, wd_o, cos_o, sin_o, rstd1_o,
    attn, lse, hidden, rstd2_o, part, mid_o, gate_o, up_o,
    buf, dys, stage, gains, give_in, give_out, wq, wk, wv, wo, wsem, wrecv, csem, nsem, fsem,
    stat, ssem, grad, give, gsend, grecv, middle, d_gate, d_up, msem, *rest,
):
    r, k, rx, ry, r3 = place()
    width = x.shape[1]
    f_half = wg.shape[1] // 2
    mate = {"col": 1 - k}
    mine = pl.ds(pl.multiple_of(k * f_half, f_half), f_half)
    his = pl.ds(pl.multiple_of((1 - k) * f_half, f_half), f_half)
    keep = [
        pltpu.make_async_copy(wg.at[:, mine], wg_o.at[k], csem.at[1]),
        pltpu.make_async_copy(wu.at[:, mine], wu_o.at[k], csem.at[2]),
        pltpu.make_async_copy(wd.at[mine], wd_o.at[k], csem.at[3]),
    ]
    first = [
        pltpu.make_async_copy(src, dst, csem.at[4 + n])
        for n, (src, dst) in enumerate(((wq_h, wq), (wk_h, wk), (wv_h, wv), (wo_h, wo)))
    ]
    for c in first + keep:
        c.start()
    greet(rx, ry, k)
    gather = Gather(x, buf, rest[:5])
    gather_dy = Gather(dy, dys, rest[5:10])
    gather_f = Gather(None, buf, rest[10:15])
    total = Sum(rest[15:])
    gains[k] = gain[...].reshape(1, width)
    gather.start()

    def give_to(n, src, dst):
        return remote(src, dst.at[k], wsem.at[n], wrecv.at[n], mate)

    gives = [give_to(0, gains.at[k], gains)]
    gives[0].start()
    heads_q = wq.shape[1] // 2
    heads_k = wk.shape[0] // 2
    nq = heads_q // HD * LANE
    nk = heads_k // HD * LANE
    for c in first:
        c.wait()
    for core, dst_in, dst_out in ((1 - k, give_in, give_out), (k, wqkv_o.at[k], wo_o.at[k])):
        sq = spread(2 * heads_q, nq, core * heads_q)
        sk = spread(2 * heads_k, nk, core * heads_k)
        dst_in[:, 0:nq] = nn(wq[...], sq).astype(BF)
        dst_in[:, nq : nq + nk] = tn(wk[...], sk).astype(BF)
        dst_in[:, nq + nk : nq + 2 * nk] = tn(wv[...], sk).astype(BF)
        dst_out[...] = nn(spread_t(nq, 2 * heads_q, core * heads_q), wo[...]).astype(BF)
    gives += [give_to(1, give_in, wqkv_o), give_to(2, give_out, wo_o)]
    gives += [give_to(3, wg.at[:, his], wg_o), give_to(4, wu.at[:, his], wu_o), give_to(5, wd.at[his], wd_o)]
    for g in gives[1:]:
        g.start()
    sign = jnp.where(lax.broadcasted_iota(jnp.int32, (32, LANE), 1) < LANE // 2, -1.0, 1.0)
    cf, sf = tables[2], tables[3]
    for a in range(LENGTH // 32):
        ca, sa = tables[0, a : a + 1, :], tables[1, a : a + 1, :]
        cos_o[a * 32 : a * 32 + 32, :] = ca * cf - sa * sf
        sin_o[a * 32 : a * 32 + 32, :] = (sa * cf + ca * sf) * sign
    for c in keep:
        c.wait()
    for n in range(3):
        gives[n].wait_recv()

    def keep_normed(i):
        row, half = gather.piece(i)
        return pltpu.make_async_copy(stage.at[i % 2], normed_o.at[:, row, rows_of(half)], nsem.at[i])

    def project(i, row, half):
        at = rows_of(half)
        x0 = buf[0, row, at, :].astype(F32)
        x1 = buf[1, row, at, :].astype(F32)
        square = jnp.sum(x0 * x0, 1, keepdims=True) + jnp.sum(x1 * x1, 1, keepdims=True)
        rstd = lax.rsqrt(square / (2 * width) + EPS)
        n0 = (x0 * rstd * gains[0]).astype(BF)
        n1 = (x1 * rstd * gains[1]).astype(BF)

        @pl.when(i >= 2)
        def _():
            keep_normed(i - 2).wait()

        stage[i % 2, 0] = n0
        stage[i % 2, 1] = n1

        @pl.when(i < 2)
        def _():
            rstd1_o[at, :] = jnp.broadcast_to(rstd, (PIECE, LANE))

        got = nn(n0, wqkv_o[0]) + nn(n1, wqkv_o[1])
        keep_normed(i).start()
        pos = pl.ds(pl.multiple_of((row % 2) * 2 * PIECE + half * PIECE, PIECE), PIECE)
        out = pl.ds(pl.multiple_of(row * 2 * PIECE + half * PIECE, PIECE), PIECE)
        cos, sin = cos_o[pos, :], sin_o[pos, :]
        for p in range(4):
            u = got[:, p * LANE : (p + 1) * LANE]
            if p < 3:
                u = u * cos + pltpu.roll(u, LANE // 2, 1) * sin
            qkv[p, out, :] = u.astype(BF)
            if p >= 2:
                kvt[p - 2, :, out] = u.T.astype(BF)

    def dy_too(q):
        @pl.when(q == 0)
        def _():
            gather_dy.start()

    gather.run(project, None, dy_too)
    for i in (6, 7):
        keep_normed(i).wait()

    def attend(row, half):
        base = pl.multiple_of(row // 2 * LENGTH, LENGTH)
        at = rows_of(half)
        qrow = pl.ds(pl.multiple_of(row * 2 * PIECE + half * PIECE, PIECE), PIECE)
        order = (row % 2) * 2 + half

        def queries(p):
            span = PIECE * (p + 1)
            for head in range(2):
                keys = qkv[2, pl.ds(base, span), :]
                s = nt(keys, qkv[head, qrow, :])
                tail = jnp.where(causal((PIECE, PIECE)), s[span - PIECE :], -1e30)
                s = tail if p == 0 else jnp.concatenate([s[: span - PIECE], tail], 0)
                top = jnp.max(s, 0, keepdims=True)
                e = jnp.exp((s - top) * SCALE)
                weight = jnp.sum(e, 0, keepdims=True)
                probs = (e * (1.0 / weight)).astype(BF)
                mixed = nn(kvt[1, :, pl.ds(base, span)], probs)
                attn[row, at, head * LANE : (head + 1) * LANE] = mixed.T.astype(BF)
                lse[head, row * 2 + half] = top * SCALE + jnp.log(weight)

        for p in range(4):
            pl.when(order == p)(lambda p=p: queries(p))
        a = attn[row, at, :]
        return nn(a, wo_o[k]), nn(a, wo_o[1 - k])

    def dy_arrive(j):
        @pl.when(j == 3)
        def _():
            gather_dy.arrive(2)
            gather_dy.arrive(3)

        @pl.when(j == 7)
        def _():
            gather_dy.arrive(4)
            gather_dy.arrive(5)

    total.send_all(attend, dy_arrive)
    io.spill(qkv, kvt, cos_o, sin_o, attn, wqkv_o, wo_o)
    for g in gives[3:]:
        g.wait_recv()
    io.spill(wg_o, wu_o, wd_o)
    gather_dy.local().wait()

    def mid_pair(q, carry):
        for u in range(2):
            i = 2 * q + u
            gather_dy.ready(i)
            row, half = gather_dy.piece(i)
            at = rows_of(half)
            d_mid = nt(dys[0, row, at, :], wd_o[0]) + nt(dys[1, row, at, :], wd_o[1])
            d_gate[row, at, :] = d_mid.astype(BF)
        return carry

    lax.fori_loop(0, 3, mid_pair, 0)
    gather_dy.arrive(6)
    gather_dy.arrive(7)
    total.relay(4)
    total.relay(5)
    mid_pair(3, 0)
    gather_dy.finish()
    for half in range(2):
        at = rows_of(half)
        h = buf[k, r, at, :].astype(F32) + total.last(6 + half)
        hidden[at, :] = h
        stat[k, at, :] = jnp.broadcast_to(jnp.sum(h * h, 1, keepdims=True), (PIECE, LANE))
    rstd2 = lax.rsqrt(exchange(k, stat, ssem) / (2 * width) + EPS)
    buf[k, r] = (hidden[...] * rstd2 * gain_f[...].reshape(1, width)).astype(BF)
    rstd2_o[...] = jnp.broadcast_to(rstd2, rstd2_o.shape)
    gather_f.start()
    io.spill(hidden)

    def keep_mids(i):
        row, half = gather_f.piece(i)
        at = rows_of(half)
        return [
            pltpu.make_async_copy(src.at[row, at], dst.at[row, at], msem.at[n, i])
            for n, (src, dst) in enumerate(((middle, mid_o), (d_gate, gate_o), (d_up, up_o)))
        ]

    def keep_f(i):
        row, half = gather_f.piece(i)
        at = rows_of(half)
        return pltpu.make_async_copy(buf.at[:, row, at], f_o.at[:, row, at], fsem.at[i])

    def expand(i, row, half):
        at = rows_of(half)
        keep_f(i).start()

        @pl.when(i > 0)
        def _():
            for c in keep_mids(i - 1):
                c.start()

        f0, f1 = buf[0, row, at, :], buf[1, row, at, :]
        dy0, dy1 = dys[0, row, at, :], dys[1, row, at, :]
        gate = nn(f0, wg_o[0]) + nn(f1, wg_o[1])
        upper = nn(f0, wu_o[0]) + nn(f1, wu_o[1])
        d_mid = d_gate[row, at, :].astype(F32)
        sig = 1.0 / (1.0 + jnp.exp(-gate))
        swish = gate * sig
        mid = (swish * upper).astype(BF)
        middle[row, at, :] = mid
        d_gate[row, at, :] = (d_mid * upper * sig * (1.0 + gate * (1.0 - sig))).astype(BF)
        d_up[row, at, :] = (d_mid * swish).astype(BF)
        g0, g1 = tn(mid, dy0), tn(mid, dy1)

        @pl.when(i == 0)
        def _():
            grad[0] = g0
            grad[1] = g1

        @pl.when(i > 0)
        def _():
            grad[0] += g0
            grad[1] += g1

    gather_f.run(expand)
    for c in keep_mids(7):
        c.start()
    half = DOWN_CHUNKS // 4

    def swap(j, core):
        return remote(
            give.at[pl.ds(2 * j, 2)], part.at[pl.ds(2 * (half * core + j), 2)], gsend.at[j], grecv.at[j], mate
        )

    for j in range(half):
        for h in range(2):
            give[2 * j + h] = grad[1 - k, j * TALL + h * CHUNK : j * TALL + (h + 1) * CHUNK, :].astype(BF)
        swap(j, k).start()
    for j in range(half):
        for h in range(2):
            rows = slice(j * TALL + h * CHUNK, j * TALL + (h + 1) * CHUNK)
            part[2 * (half * k + j) + h] = grad[k, rows, :].astype(BF)
    for j in range(half):
        swap(j, 1 - k).wait_recv()
    io.spill(part)

    def kept(i, carry):
        keep_f(i).wait()
        for c in keep_mids(i):
            c.wait()
        return carry

    lax.fori_loop(0, 8, kept, 0)
    for j in range(half):
        swap(j, k).wait_send()
    for g in gives:
        g.wait_send()
    total.finish()


def front(x, dy, gain, gain_f, wq, wk, wv, wo, wg, wu, wd):
    tokens, width = x.shape
    f_half = wg.shape[1] // 2
    cols = 4 * LANE
    gathered = (2, 4, tokens, width)
    outs = [sds(gathered, BF), sds(gathered, BF)]
    outs += [sds((4, 4 * tokens, LANE), BF), sds((2, LANE, 4 * tokens), BF)]
    outs += [sds((2, width, cols), BF), sds((2, 2 * LANE, width), BF)]
    outs += [sds((2, width, f_half), BF)] * 2 + [sds((2, f_half, width), BF)]
    outs += [sds((LENGTH, LANE), F32)] * 2 + [sds((tokens, LANE), F32)]
    outs += [sds((4, tokens, 2 * LANE), BF), sds((2, 8, 1, PIECE), F32)]
    outs += [sds((tokens, width), F32), sds((tokens, LANE), F32)]
    outs += [sds((DOWN_CHUNKS, CHUNK, WIDE), BF)] + [sds((4, tokens, f_half), BF)] * 3
    half = DOWN_CHUNKS // 4
    scratch = [pltpu.VMEM(gathered, BF)] * 2 + [pltpu.VMEM((2, 2, PIECE, width), BF)]
    scratch += [pltpu.VMEM((2, 1, width), F32), pltpu.VMEM((width, cols), BF), pltpu.VMEM((2 * LANE, width), BF)]
    scratch += [pltpu.VMEM(w.shape, BF) for w in (wq, wk, wv, wo)]
    scratch += [DMA((6,)), DMA((6,)), DMA((8,)), DMA((8,)), DMA((8,))]
    scratch += [pltpu.VMEM((2, tokens, LANE), F32), DMA((2,)), pltpu.VMEM((2, f_half, width), F32)]
    scratch += [pltpu.VMEM((2 * half, CHUNK, WIDE), BF), DMA((half,)), DMA((half,))]
    scratch += [pltpu.VMEM((4, tokens, f_half), BF)] * 3 + [DMA((3, 8))]
    scratch += GATHER_SEMS * 3 + sum_scratch(width)
    ins = [ANY] * 2 + [VM] * 2 + [ANY] * 7 + [VM]
    args = [x, dy, gain, gain_f, wq, wk, wv, wo, wg, wu, wd, jnp.asarray(np.stack(angle_tables()))]
    out_specs = [ANY] * 2 + [VM] * (len(outs) - 5) + [ANY] * 3
    spill = [2, 3, 4, 5, 6, 7, 8, 9, 10, 12, 14, 16]
    return call(front_kernel, 0, outs, ins, args, scratch, 9e10, 61, out_specs, [], spill)


TICKS = 35


def flat(ref, h, m=None):
    got = ref[h] if m is None else ref[h, :, :, pl.ds(pl.multiple_of(m * 256, 256), 256)]
    return got.reshape(-1, got.shape[-1])


def contract_kernel(
    io,
    d_gate, d_up, wg, wu, hidden, rstd2, gain, dy, wo, attn, part_d, f_any,
    d_hidden, gains_o, part, part_o, d_attn, totals, acc_c, tot_c,
    stat, ssem, give, gsend, grecv, gathered, dya, grad, give_o, his_o, gsem, fsem, *rest,
):
    r, k, rx, ry, r3 = place()
    width = hidden.shape[1]
    fetch = pltpu.make_async_copy(f_any, gathered, fsem)
    greet(rx, ry, k, True)
    total = Sum(rest[:9])
    gather = Gather(dya, gathered, rest[9:14])
    parts = [(0, DOWN_CHUNKS, part_d), (DOWN_CHUNKS, MLP_CHUNKS, part), (MLP_CHUNKS, OUT_CHUNKS, part_o)]
    line = Line(parts, totals, (acc_c, tot_c), rest[14:], 0, TICKS)
    io.need(d_gate, d_up, wg, wu, part_d)
    line.open()
    fetch.start()
    io.more()

    def compute(row, half):
        at = rows_of(half)
        g, u = d_gate[row, at, :], d_up[row, at, :]
        return nt(g, wg[k]) + nt(u, wu[k]), nt(g, wg[1 - k]) + nt(u, wu[1 - k])

    def early(j):
        @pl.when(j % 2 == 1)
        def _():
            line.step(j // 2)

    total.send_all(compute, early)

    def swap(e, core):
        to = part.at[pl.ds(2 * (e // 4 * 8 + 4 * core + e % 4), 2)]
        return remote(give.at[pl.ds(2 * e, 2)], to, gsend.at[e], grecv.at[e], {"col": 1 - k})

    def wide_part(h, right, dst, first):
        def one(m, carry):
            got = tn(flat(gathered, h, m), right[...].reshape(-1, right.shape[2])).astype(BF)
            for b in range(2):
                lanes = pl.ds(pl.multiple_of((2 * m + b) * TALL, TALL), TALL)
                for j in range(4):
                    for u in range(2):
                        rows = slice(b * TALL + u * CHUNK, b * TALL + (u + 1) * CHUNK)
                        dst[2 * (first + j) + u, :, lanes] = got[rows, j * TALL : (j + 1) * TALL]
            return carry

        lax.fori_loop(0, width // 256, one, 0)

    fetch.wait()
    wide_part(1 - k, d_gate, give, 0)
    for e in range(4):
        swap(e, k).start()
    wide_part(k, d_gate, part, 4 * k)
    line.steps(4, 6)
    wide_part(1 - k, d_up, give, 4)
    for e in range(4, 8):
        swap(e, k).start()
    wide_part(k, d_up, part, 8 + 4 * k)
    total.relay(4)
    total.relay(5)
    for e in range(8):
        swap(e, 1 - k).wait_recv()
    io.spill(part)
    io.need(hidden, dy, wo, attn)
    line.steps(6, 13)
    gains = jnp.zeros((1, width), F32)
    for half in range(2):
        at = rows_of(half)
        d_nf = total.last(6 + half)
        h = hidden[at, :]
        gains = gains + jnp.sum(d_nf * h * rstd2[at, 0:1], 0, keepdims=True)
        scaled = d_nf * gain[...].reshape(1, width)
        d_hidden[at, :] = scaled
        stat[k, at, :] = jnp.broadcast_to(jnp.sum(scaled * h, 1, keepdims=True), (PIECE, LANE))
    gains_o[...] = gains
    inner = exchange(k, stat, ssem) / (2 * width)
    rs = rstd2[:, 0:1]
    value = dy[...].astype(F32) + rs * d_hidden[...] - hidden[...] * (rs * rs * rs * inner)
    d_hidden[...] = value
    dya[...] = value.astype(BF)
    gather.start()
    io.spill(d_hidden)

    def piece(i, row, half):
        at = rows_of(half)
        d0, d1 = gathered[0, row, at, :], gathered[1, row, at, :]
        d_attn[row, at, :] = (nt(d0, wo[0]) + nt(d1, wo[1])).astype(BF)
        a = attn[row, at, :]
        g0, g1 = tn(a, d0), tn(a, d1)

        @pl.when(i == 0)
        def _():
            grad[0] = g0
            grad[1] = g1

        @pl.when(i > 0)
        def _():
            grad[0] += g0
            grad[1] += g1

    def before(q):
        line.steps(jnp.where(q == 0, 13, 15 + 4 * q), 18 + 4 * q)

    def after(q):
        line.step(18 + 4 * q)

    gather.run(piece, before, after)
    give_o[...] = grad[1 - k].astype(BF)
    give_out = remote(give_o, his_o, gsem.at[0], gsem.at[1], {"col": 1 - k})
    give_out.start()
    q_cols = part_o.shape[0] * CHUNK
    mine = nn(spread(q_cols, 2 * LANE, k * (q_cols // 2)), grad[k].astype(BF))
    give_out.wait_recv()
    out = mine + nn(spread(q_cols, 2 * LANE, (1 - k) * (q_cols // 2)), his_o[...])
    for c in range(q_cols // CHUNK):
        part_o[c] = out[c * CHUNK : (c + 1) * CHUNK].astype(BF)
    line.rest(31)
    for e in range(8):
        swap(e, k).wait_send()
    give_out.wait_send()
    total.finish()


def contract(d_gate, d_up, wg, wu, hidden, rstd2, gain, dy, wo, attn, part_d, all_f):
    tokens, width = hidden.shape
    n = lax.axis_size("dp")
    outs = [sds((tokens, width), F32), sds((1, width), F32)]
    outs += [sds((MLP_CHUNKS - DOWN_CHUNKS, CHUNK, WIDE), BF), sds((OUT_CHUNKS - MLP_CHUNKS, CHUNK, WIDE), BF)]
    outs += [sds((4, tokens, 2 * LANE), BF)] + line_outs(TICKS)
    out_specs = [VM] * 5 + [ANY] + [VM] * 2
    scratch = [pltpu.VMEM((2, tokens, LANE), F32), DMA((2,))]
    scratch += [pltpu.VMEM((16, CHUNK, WIDE), BF), DMA((8,)), DMA((8,))]
    scratch += [pltpu.VMEM((2, 4, tokens, width), BF), pltpu.VMEM((tokens, width), BF)]
    scratch += [pltpu.VMEM((2, 2 * LANE, width), F32)] + [pltpu.VMEM((2 * LANE, width), BF)] * 2
    scratch += [DMA((2,)), DMA]
    scratch += sum_scratch(width) + GATHER_SEMS + line_scratch(n, TICKS)
    args = [d_gate, d_up, wg, wu, hidden, rstd2, gain, dy, wo, attn, part_d, all_f]
    ins = [VM] * 11 + [ANY]
    fetch = [0, 1, 2, 3, 10, 4, 7, 8, 9]
    return call(
        contract_kernel, 1, outs, ins, args, scratch, 5e10, vmem_limit(n), out_specs, fetch, [0, 2, 3, 4], 5
    )


def vmem_limit(n):
    return 60 if n <= 4 else 63


def columns(rows, cols, core, q_cols, k_cols):
    i = lax.broadcasted_iota(jnp.int32, (rows, cols), 0)
    at = lax.broadcasted_iota(jnp.int32, (rows, cols), 1)
    part, lane = i // LANE, i % LANE
    index = jnp.where(lane < HALF, lane, lane - (LANE // 2 - HALF))
    q = core * (q_cols // 2) + part * HD
    kv = q_cols + (part - 2) * k_cols + core * (k_cols // 2)
    to = jnp.where(part < 2, q, kv) + index
    pad = lane % (LANE // 2) >= HALF
    return jnp.where((at == to) & (pad == False), 1.0, 0.0).astype(BF)


def backward_kernel(
    q_cols, k_cols,
    io,
    qkv, kvt, lse, d_attn, cos, sin, middle, wd, hidden, wqkv, x, rstd1, d_hidden, gain, gains_f,
    part_m, part_o, acc_c, tot_c, normed_any,
    output, grad_x, gains_o, totals,
    dk, dv, d_proj, normed, part, mine, give, his, gsem, stat, ssem, free, fsem,
    mine_g, pair_g, slots, gsend, grecv, *rest,
):
    r, k, rx, ry, r3 = place()
    width = x.shape[1]
    n = lax.axis_size("dp")
    z = lax.axis_index("dp")
    fetch = pltpu.make_async_copy(normed_any, normed, fsem)
    greet(rx, ry, k, True, True)
    sums = rest[:5]
    down = Sum(sums + rest[5:9])
    into = Sum(sums + rest[9:13])
    ticks = line_ticks(n) - TICKS
    parts = [(DOWN_CHUNKS, MLP_CHUNKS, part_m), (MLP_CHUNKS, OUT_CHUNKS, part_o), (OUT_CHUNKS, ALL_CHUNKS, part)]
    line = Line(parts, totals, None, rest[13:], TICKS, ticks, (acc_c, tot_c))
    io.need(part_m, part_o, middle, wd)
    line.open()
    io.more()

    def down_piece(row, half):
        m = middle[row, rows_of(half), :]
        return nn(m, wd[k]), nn(m, wd[1 - k])

    def early(j):
        @pl.when(j % 3 == 1)
        def _():
            line.step(j // 3)

    down.send_all(down_piece, early)

    fetch.start()
    io.need(qkv, kvt, d_attn, cos, sin)

    def unrotate(u, p):
        at = pl.ds(p * PIECE, PIECE)
        return u * cos[at, :] - pltpu.roll(u, LANE // 2, 1) * sin[at, :]

    def sequence(seq):
        base = pl.multiple_of(seq * LENGTH, LENGTH)

        def one_head(head, carry):
            for p in range(4):
                span = PIECE * (p + 1)
                row = seq * 2 + p // 2
                at = pl.ds((p % 2) * PIECE, PIECE)
                out = pl.ds(pl.multiple_of(base + p * PIECE, PIECE), PIECE)
                keys = qkv[2, pl.ds(base, span), :]
                q = qkv[head, out, :]
                lane = pl.ds(pl.multiple_of(head * LANE, LANE), LANE)
                do = d_attn[row, at, lane]
                e = jnp.exp(nt(keys, q) * SCALE - lse[head, seq * 4 + p])
                tail = jnp.where(causal((PIECE, PIECE)), e[span - PIECE :], 0.0)
                e = tail if p == 0 else jnp.concatenate([e[: span - PIECE], tail], 0)
                dp = nt(qkv[3, pl.ds(base, span), :], do)
                inner = jnp.sum(e * dp, 0, keepdims=True)
                ds = (e * (dp - inner)).astype(BF)
                dv[0:span, :] += nn(e.astype(BF), do)
                dk[0:span, :] += nn(ds, q)
                dq = nn(kvt[0, :, pl.ds(base, span)], ds).T * SCALE
                d_proj[out, lane] = unrotate(dq, p).astype(BF)
                if p % 2 == 1:
                    tick = 3 + seq * 8 + head * 4 + p - 1
                    line.steps(tick, jnp.minimum(tick + 2, OUT_CHUNKS - LAG - TICKS))
            return carry

        dk[...] = jnp.zeros_like(dk)
        dv[...] = jnp.zeros_like(dv)
        lax.fori_loop(0, 2, one_head, 0)
        for p in range(4):
            at = pl.ds(p * PIECE, PIECE)
            out = pl.ds(pl.multiple_of(base + p * PIECE, PIECE), PIECE)
            d_proj[out, 2 * LANE : 3 * LANE] = unrotate(dk[at, :] * SCALE, p).astype(BF)
            d_proj[out, 3 * LANE : 4 * LANE] = dv[at, :].astype(BF)

    def both(seq, carry):
        sequence(seq)

        @pl.when(seq == 0)
        def _():
            down.relay(4)
            down.relay(5)

        return carry

    lax.fori_loop(0, 2, both, 0)
    io.need(hidden)
    for half in range(2):
        at = rows_of(half)
        output[at, :] = hidden[at, :] + down.last(6 + half)
    down.finish()
    io.spill(output)
    for device in ({"row": rx}, {"row": ry}, {"col": 1 - k}):
        pl.semaphore_signal(free, inc=1, device_id=device, device_id_type=MESH)
    pl.semaphore_wait(free, 3)

    fetch.wait()

    def in_part(h, dst):
        def one(m, carry):
            dst[pl.ds(pl.multiple_of(m * 256, 256), 256), :] = tn(flat(normed, h, m), d_proj[...]).astype(BF)
            return carry

        lax.fori_loop(0, width // 256, one, 0)

    in_part(1 - k, give)
    swap = remote(give, his, gsem.at[0], gsem.at[1], {"col": 1 - k})
    swap.start()
    in_part(k, mine)
    cols = q_cols + 2 * k_cols
    got = nn(mine[...], columns(4 * LANE, cols, k, q_cols, k_cols))
    swap.wait_recv()
    got = got + nn(his[...], columns(4 * LANE, cols, 1 - k, q_cols, k_cols))
    for c in range(width // CHUNK):
        part[c] = got[c * CHUNK : (c + 1) * CHUNK].astype(BF)

    def into_piece(row, half):
        d = d_proj[pl.ds(pl.multiple_of(row * 2 * PIECE + half * PIECE, PIECE), PIECE), :]
        return nt(d, wqkv[k]), nt(d, wqkv[1 - k])

    def beside(j):
        @pl.when(j % 2 == 1)
        def _():
            line.step(17 + j // 2)

    io.need(wqkv)
    into.send_all(into_piece, beside)
    line.steps(21, 24)
    into.relay(4)
    into.relay(5)
    line.steps(24, 29)
    io.need(x, d_hidden)
    gains = jnp.zeros((1, width), F32)
    for half in range(2):
        at = rows_of(half)
        d_na = into.last(6 + half)
        xs = x[at, :].astype(F32)
        gains = gains + jnp.sum(d_na * xs * rstd1[at, 0:1], 0, keepdims=True)
        scaled = d_na * gain[...].reshape(1, width)
        grad_x[at, :] = scaled
        stat[k, at, :] = jnp.broadcast_to(jnp.sum(scaled * xs, 1, keepdims=True), (PIECE, LANE))

    def row_total(step, device):
        copy = remote(mine_g.at[step], pair_g.at[step], gsend.at[n + step], grecv.at[n + step], {"row": device})
        copy.start()
        return copy

    mine_g[0, 0:1] = gains
    mine_g[0, 1:2] = gains_f[...]
    over_x = row_total(0, rx)
    inner = exchange(k, stat, ssem) / (2 * width)
    rs = rstd1[:, 0:1]
    over_x.wait_recv()
    mine_g[1] = mine_g[0] + pair_g[0]
    over_y = row_total(1, ry)
    grad_x[...] = d_hidden[...] + rs * grad_x[...] - x[...].astype(F32) * (rs * rs * rs * inner)
    over_y.wait_recv()
    slots[z] = mine_g[1] + pair_g[1]

    def over_dp(t, mine):
        other = (z + t) % n
        g = z if mine else other
        return remote(slots.at[g], slots.at[g], gsend.at[t], grecv.at[g], {"dp": other})

    def start(t, carry):
        over_dp(t, True).start()
        return carry

    lax.fori_loop(1, n, start, 0)
    io.spill(grad_x)
    line.rest(29)

    def wait(t, carry):
        over_dp(t, False).wait_recv()
        over_dp(t, True).wait_send()
        return carry

    lax.fori_loop(1, n, wait, 0)
    gains_o[...] = lax.fori_loop(1, n, lambda g, total: total + slots[g], slots[0])
    over_x.wait_send()
    over_y.wait_send()
    swap.wait_send()
    into.finish()


def backward(
    qkv, kvt, lse, d_attn, cos, sin, middle, wd, hidden, wqkv, x, rstd1, d_hidden, gain, gains_f,
    part_m, part_o, acc, tot, normed, q_cols, k_cols,
):
    tokens, width = x.shape
    n = lax.axis_size("dp")
    ticks = line_ticks(n) - TICKS
    outs = [sds((tokens, width), F32)] * 2 + [sds((2, width), F32), sds((ticks, CHUNK, WIDE), BF)]
    scratch = [pltpu.VMEM((LENGTH, LANE), F32)] * 2 + [pltpu.VMEM((4 * tokens, 4 * LANE), BF)]
    scratch += [pltpu.VMEM((2, 4, tokens, width), BF), pltpu.VMEM((ALL_CHUNKS - OUT_CHUNKS, CHUNK, WIDE), BF)]
    scratch += [pltpu.VMEM((width, 4 * LANE), BF)] * 3 + [DMA((2,))]
    scratch += [pltpu.VMEM((2, tokens, LANE), F32), DMA((2,)), pltpu.SemaphoreType.REGULAR, DMA]
    scratch += [pltpu.VMEM((2, 2, width), F32)] * 2 + [pltpu.VMEM((n, 2, width), F32)]
    scratch += [DMA((n + 2,)), DMA((n + 2,))]
    both = sum_scratch(width)
    scratch += both + both[5:] + line_scratch(n, ticks)
    args = [qkv, kvt, lse, d_attn, cos, sin, middle, wd, hidden, wqkv, x, rstd1, d_hidden, gain, gains_f]
    args += [part_m, part_o, acc, tot, normed]
    kernel = functools.partial(backward_kernel, q_cols, k_cols)
    ins = [VM] * (len(args) - 1) + [ANY]
    fetch = [15, 16, 6, 7, 0, 1, 3, 4, 5, 8, 9, 10, 12]
    return call(
        kernel, 2, outs, ins, args, scratch, 5e10, vmem_limit(n), [VM] * 3 + [ANY], fetch, [0, 1], 4
    )


def unpack_kernel(ticks, q_cols, k_cols, *rest):
    tots, (down, gate, up, out, q_o, k_o, v_o), rest = rest[: len(ticks)], rest[len(ticks) : len(ticks) + 7], rest[len(ticks) + 7 :]
    chunks, wide, parts, isem, osem = rest
    n, s, _, _ = line_place()
    mid = n // 2
    off = LAG * (2 * mid - 2 - s)
    offs = [LAG * o for o in range(mid - 1, 2 * mid - 1)]

    def source(t):
        for tot, count in zip(tots, ticks):
            if t < count:
                return tot.at[t]
            t -= count

    def load(c):
        for o in offs:

            @pl.when(off == o)
            def _(o=o):
                for u in range(2):
                    dst = chunks.at[c % 4, pl.ds(u * CHUNK, CHUNK)]
                    pltpu.make_async_copy(source(2 * c + u + o), dst, isem.at[c % 4, u]).start()

    def stored(c):
        slot = c % 4
        buf = wide.at[slot]
        if c < 8:
            return [pltpu.make_async_copy(buf, down.at[pl.ds(c * TALL, TALL)], osem.at[slot, 0])]
        if c < MLP_CHUNKS // 2:
            to, lanes = (gate, up)[c // 8 - 1], pl.ds(c % 8 * TALL, TALL)
            return [
                pltpu.make_async_copy(
                    buf.at[:, pl.ds(b * TALL, TALL)], to.at[pl.ds(b * TALL, TALL), lanes], osem.at[slot, b]
                )
                for b in range(WIDE // TALL)
            ]
        if c < OUT_CHUNKS // 2:
            return [pltpu.make_async_copy(buf, out.at[pl.ds((c - MLP_CHUNKS // 2) * TALL, TALL)], osem.at[slot, 0])]
        rows = pl.ds((c - OUT_CHUNKS // 2) * TALL, TALL)
        return [
            pltpu.make_async_copy(buf.at[:, pl.ds(0, q_cols)], q_o.at[rows], osem.at[slot, 0]),
            pltpu.make_async_copy(parts.at[0, slot], k_o.at[:, rows], osem.at[slot, 1]),
            pltpu.make_async_copy(parts.at[1, slot], v_o.at[:, rows], osem.at[slot, 2]),
        ]

    for c in range(3):
        load(c)
    for c in range(ALL_CHUNKS // 2):
        if c + 3 < ALL_CHUNKS // 2:
            load(c + 3)
        if c >= 4:
            for copy in stored(c - 4):
                copy.wait()
        for u in range(2):
            dst = chunks.at[c % 4, pl.ds(u * CHUNK, CHUNK)]
            pltpu.make_async_copy(dst, dst, isem.at[c % 4, u]).wait()
        value = chunks[c % 4].astype(F32)
        wide[c % 4] = value
        if c >= OUT_CHUNKS // 2:
            parts[0, c % 4] = value[:, q_cols : q_cols + k_cols].T
            parts[1, c % 4] = value[:, q_cols + k_cols :].T
        for copy in stored(c):
            copy.start()
    for c in range(ALL_CHUNKS // 2 - 4, ALL_CHUNKS // 2):
        for copy in stored(c):
            copy.wait()


def unpack(tots, q_cols, k_cols):
    n = lax.axis_size("dp")
    ticks = [TICKS, line_ticks(n) - TICKS]
    outs = [sds((8 * TALL, WIDE), F32), sds((WIDE, 8 * TALL), F32), sds((WIDE, 8 * TALL), F32)]
    outs += [sds((q_cols, WIDE), F32), sds((WIDE, q_cols), F32), sds((k_cols, WIDE), F32), sds((k_cols, WIDE), F32)]
    moved = 6 * ALL_CHUNKS // 2 * TALL * WIDE
    return pl.pallas_call(
        functools.partial(unpack_kernel, ticks, q_cols, k_cols),
        out_shape=outs,
        in_specs=[ANY] * len(tots),
        out_specs=[ANY] * len(outs),
        scratch_shapes=[
            pltpu.VMEM((4, TALL, WIDE), BF),
            pltpu.VMEM((4, TALL, WIDE), F32),
            pltpu.VMEM((2, 4, k_cols, TALL), F32),
            DMA((4, 2)),
            DMA((4, WIDE // TALL)),
        ],
        compiler_params=pltpu.CompilerParams(vmem_limit_bytes=16 << 20),
        cost_estimate=pl.CostEstimate(flops=0, bytes_accessed=moved, transcendentals=0),
    )(*tots)


def on_device(
    layer_input, gain_attn, gain_ffn, w_query, w_key, w_value, w_out, w_gate, w_up, w_down, cotangent
):
    tokens, width = layer_input.shape
    q_cols, k_cols = w_query.shape[1], w_key.shape[1]
    gain_a, gain_f = gain_attn, gain_ffn
    (
        normed, all_f, qkv, kvt, wqkv, wo, wg, wu, wd, cos, sin, rstd1,
        attn, lse, hidden, rstd2, part_d, middle, d_gate, d_up,
    ) = front(
        layer_input, cotangent, gain_a, gain_f,
        w_query, w_key.T, w_value.T, w_out, w_gate, w_up, w_down,
    )
    d_hidden, gains_f, part_m, part_o, d_attn, tot1, acc, tot = contract(
        d_gate, d_up, wg, wu, hidden, rstd2, gain_f, cotangent, wo, attn, part_d, all_f
    )
    output, grad_x, gains, tot2 = backward(
        qkv, kvt, lse, d_attn, cos, sin, middle, wd, hidden, wqkv, layer_input, rstd1, d_hidden,
        gain_a, gains_f, part_m, part_o, acc, tot, normed, q_cols, k_cols,
    )
    down, gate, up, out, g_q, g_k, g_v = unpack([tot1, tot2], q_cols, k_cols)
    return output, grad_x, gains[0], gains[1], g_q, g_k.T, g_v.T, out, gate, up, down


def solution(mesh):
    assert mesh.shape["row"] == 4 and mesh.shape["col"] == 2
    tokens = P(("dp", "row"), "col")
    wide = P("col", "row")
    tall = P("row", "col")
    return jax.shard_map(
        on_device,
        mesh=mesh,
        in_specs=(tokens, P("col"), P("col"), wide, wide, wide, tall, wide, wide, tall, tokens),
        out_specs=(tokens, tokens, P("col"), P("col"), wide, wide, wide, tall, wide, wide, tall),
        check_vma=False,
    )
```

```python
import functools

import jax
import jax.numpy as jnp
import numpy as np
from jax import lax
from jax.experimental import pallas as pl
from jax.experimental.pallas import tpu as pltpu
from jax.sharding import PartitionSpec as P

HD = 96
HALF = HD // 2
LENGTH = 1024
EPS = 1e-05
THETA = 100000.0
SCALE = HD ** (-0.5)
LANE = 128
PIECE = 256

BF = jnp.bfloat16
F32 = jnp.float32
MESH = pl.DeviceIdType.MESH
VM = pl.BlockSpec(memory_space=pltpu.VMEM)
ANY = pl.BlockSpec(memory_space=pl.ANY)
DMA = pltpu.SemaphoreType.DMA


def nn(a, b):
    return lax.dot_general(a, b, (((1,), (0,)), ((), ())), preferred_element_type=F32)


def nt(a, b):
    return lax.dot_general(a, b, (((1,), (1,)), ((), ())), preferred_element_type=F32)


def place():
    r = lax.axis_index("row")
    k = lax.axis_index("col")
    return r, k, r + 1 - 2 * (r % 2), (r + 2) % 4, 3 - r


def tn(a, b):
    return lax.dot_general(a, b, (((0,), (0,)), ((), ())), preferred_element_type=F32)


def line_place():
    n = lax.axis_size("dp")
    z = lax.axis_index("dp")
    left = z < n // 2
    step = jnp.where(left, 1, -1)
    return n, jnp.where(left, z, n - 1 - z), z + step, z - step


def greet(rx, ry, k, line=False, groups=False):
    bar = pltpu.get_barrier_semaphore()

    def hello(device):
        pl.semaphore_signal(bar, inc=1, device_id=device, device_id_type=MESH)

    for device in ({"row": rx}, {"row": ry}, {"col": 1 - k}):
        hello(device)
    if not line:
        pl.semaphore_wait(bar, 3)
        return
    n, s, inward, outward = line_place()
    if groups:
        z = lax.axis_index("dp")

        def one(t, carry):
            hello({"dp": (z + t) % n})
            return carry

        lax.fori_loop(1, n, one, 0)
        pl.semaphore_wait(bar, 3 + n - 1)
        return
    hello({"dp": inward})

    @pl.when(s > 0)
    def _():
        hello({"dp": outward})

    pl.semaphore_wait(bar, jnp.where(s > 0, 5, 4))


def remote(src, dst, send, recv, device):
    return pltpu.make_async_remote_copy(
        src_ref=src, dst_ref=dst, send_sem=send, recv_sem=recv, device_id=device, device_id_type=MESH
    )


def rows_of(half):
    return pl.ds(pl.multiple_of(half * PIECE, PIECE), PIECE)


GATHER_SEMS = [DMA((6,)), DMA((6,)), DMA((8,)), DMA((8,)), DMA]


class Gather:
    def __init__(self, own, buf, sems):
        self.own, self.buf = own, buf
        self.isend, self.irecv, self.dsend, self.drecv, self.lsem = sems
        self.r, self.k, self.rx, self.ry, self.r3 = place()

    def piece(self, i):
        side = jnp.where(i % 2 == 0, self.rx, self.ry)
        row = jnp.where(i < 2, self.r, jnp.where(i < 6, side, self.r3))
        half = jnp.where(i // 2 == 2, 1 - i % 2, i % 2)
        return row, half

    def ici(self, sem, row, half, device, src=None):
        dst = self.buf.at[self.k, row, rows_of(half)]
        return remote(dst if src is None else src, dst, self.isend.at[sem], self.irecv.at[sem], {"row": device})

    def pair(self, i, core, row, half, src=None):
        dst = self.buf.at[core, row, rows_of(half)]
        return remote(dst if src is None else src, dst, self.dsend.at[i], self.drecv.at[i], {"col": 1 - self.k})

    def local(self):
        return pltpu.make_async_copy(self.own, self.buf.at[self.k, self.r], self.lsem)

    def start(self):
        own = self.buf.at[self.k, self.r] if self.own is None else self.own
        first, second = own.at[pl.ds(0, PIECE)], own.at[pl.ds(PIECE, PIECE)]
        self.ici(0, self.r, 0, self.rx, first).start()
        self.ici(1, self.r, 1, self.ry, second).start()
        self.ici(2, self.r, 1, self.rx, second).start()
        self.ici(3, self.r, 0, self.ry, first).start()
        self.pair(0, self.k, self.r, 0, first).start()
        self.pair(1, self.k, self.r, 1, second).start()
        if self.own is not None:
            self.local().start()

    def arrive(self, i):
        row, half = self.piece(i)
        self.ici(i - 2, row, half, self.rx).wait_recv()

        @pl.when(i == 2)
        def _():
            self.ici(4, row, half, self.ry).start()

        @pl.when(i == 3)
        def _():
            self.ici(5, row, half, self.rx).start()

        self.pair(i, self.k, row, half).start()

    def ready(self, i):
        row, half = self.piece(i)
        self.pair(i, 1 - self.k, row, half).wait_recv()

    def run(self, compute, before=None, after=None):
        if self.own is not None:
            self.local().wait()

        def pair(q, carry):
            for u in range(2):
                i = 2 * q + u
                self.ready(i)
                row, half = self.piece(i)
                compute(i, row, half)
            if before is not None:
                before(q)

            @pl.when(q < 3)
            def _():
                self.arrive(2 * q + 2)
                self.arrive(2 * q + 3)

            if after is not None:
                after(q)
            return carry

        lax.fori_loop(0, 4, pair, 0)
        self.finish()

    def finish(self):
        for i in range(6):
            self.ici(i, self.r, 0, self.rx).wait_send()
        for i in range(8):
            self.pair(i, self.k, self.r, 0).wait_send()


def sum_scratch(width):
    return [
        pltpu.VMEM((4, PIECE, width), F32),
        pltpu.VMEM((4, PIECE, width), BF),
        pltpu.VMEM((8, PIECE, width), BF),
        pltpu.VMEM((6, PIECE, width), BF),
        pltpu.VMEM((6, PIECE, width), BF),
        DMA((8,)),
        DMA((8,)),
        DMA((6,)),
        DMA((6,)),
    ]


class Sum:
    def __init__(self, scratch):
        self.own, self.ds, self.dr, self.ist, self.irt = scratch[:5]
        self.dsend, self.drecv, self.isend, self.irecv = scratch[5:]
        self.r, self.k, self.rx, self.ry, self.r3 = place()

    def piece(self, j):
        mid = jnp.where(j == 2, self.ry, jnp.where(j == 5, self.ry, self.rx))
        row = jnp.where(j < 2, self.r3, jnp.where(j < 6, mid, self.r))
        return row, j % 2

    def pair(self, j):
        return remote(self.ds.at[j % 4], self.dr.at[j], self.dsend.at[j], self.drecv.at[j], {"col": 1 - self.k})

    def ici(self, j):
        device = jnp.where(j == 0, self.ry, jnp.where(j == 2, self.ry, jnp.where(j == 5, self.ry, self.rx)))
        return remote(self.ist.at[j], self.irt.at[j], self.isend.at[j], self.irecv.at[j], {"row": device})

    def put(self, j, kept, given):
        @pl.when(j >= 4)
        def _():
            self.pair(j - 4).wait_send()

        self.own[j % 4] = kept
        self.ds[j % 4] = given.astype(BF)
        self.pair(j).start()

    def chip(self, j):
        self.pair(j).wait_recv()
        return self.own[j % 4] + self.dr[j].astype(F32)

    def forward(self, j):
        self.ist[j] = self.chip(j).astype(BF)
        self.ici(j).start()

    def relay(self, j):
        value = self.chip(j)
        self.ici(j - 4).wait_recv()
        self.ist[j] = (value + self.irt[j - 4].astype(F32)).astype(BF)
        self.ici(j).start()

    def last(self, j):
        value = self.chip(j)
        self.ici(j - 4).wait_recv()
        value = value + self.irt[j - 4].astype(F32)
        self.ici(j - 2).wait_recv()
        return value + self.irt[j - 2].astype(F32)

    def send_all(self, compute, hook=None):
        def step(j, carry):
            row, half = self.piece(j)
            kept, given = compute(row, half)
            self.put(j, kept, given)

            @pl.when(j > 0)
            def _():
                @pl.when(j < 5)
                def _():
                    self.forward(j - 1)

            if hook is not None:
                hook(j)
            return carry

        lax.fori_loop(0, 8, step, 0)

    def finish(self):
        for j in range(4, 8):
            self.pair(j).wait_send()
        for j in range(6):
            self.ici(j).wait_send()


TALL, WIDE = 128, 768
CHUNK = TALL // 2
DOWN_CHUNKS, MLP_CHUNKS, OUT_CHUNKS, ALL_CHUNKS = 16, 48, 54, 66


def lags(n):
    return (4, 2) if n <= 4 else (2, 1)


def line_ring(n, lag):
    return lag * (2 * (n // 2) - 2) + lag + 4


def line_ticks(n, count, lag):
    return count + lag * (2 * (n // 2) - 2)


def line_outs(ticks, lag):
    return [sds((ticks, CHUNK, WIDE), BF)] + [sds((lag, CHUNK, WIDE), BF)] * 2


def line_scratch(n, ticks, lag):
    near, far = 2 * lag + 2, line_ring(n, lag)
    slots = (near, far, far, near)
    return [pltpu.VMEM((count, CHUNK, WIDE), BF) for count in slots] + [DMA((ticks,))] * 6


class Line:
    def __init__(self, parts, totals, carry, scratch, first, ticks, count, lag, before=None):
        self.parts, self.totals, self.carry = parts, totals, carry
        self.acc, self.tot, self.rin, self.rxb = scratch[:4]
        self.si, self.ri, self.rx, self.so, self.ro, self.out_sem = scratch[4:]
        self.first, self.ticks, self.count, self.lag, self.near = first, ticks, count, lag, 2 * lag + 2
        self.n, self.s, self.inward, self.outward = line_place()
        self.mid = self.n // 2
        self.ring = line_ring(self.n, lag)
        if before is not None:

            @pl.when(self.s > 0)
            def _():
                for b in range(self.lag):
                    self.acc[b] = before[0][b]
                    self.tot[b] = before[1][b]

    def valid(self, c):
        return (c >= 0) & (c < self.count)

    def sends(self, j):
        s, mid, slot, near = self.s, self.mid, j % self.ring, j % self.near
        to = {"dp": self.inward}
        c = self.first + j - self.lag * s
        moves = []
        inward = (self.rin.at[slot], self.ri.at[j])
        across = (self.rxb.at[near], self.rx.at[j])
        for lo, hi, ref in self.parts:
            ok = (s == 0) & (c >= lo) & (c < hi)
            moves.append((ok, ref, c - lo, across if mid == 1 else inward))
        if mid > 1:
            ok = self.valid(c)
            moves.append((ok & (s == mid - 1), self.acc, near, across))
            if mid > 2:
                moves.append((ok & (s > 0) & (s < mid - 1), self.acc, near, inward))
        out = [
            (cond, lambda ref=ref, at=at, way=way: remote(ref.at[at], way[0], self.si.at[j], way[1], to))
            for cond, ref, at, way in moves
        ]
        if mid > 1:
            c = self.first + j - self.lag * (2 * mid - 1 - s)
            out.append(((s > 0) & self.valid(c), lambda: self.outer(j)))
        return out

    def outer(self, j):
        return remote(
            self.tot.at[j % self.ring], self.tot.at[(j + self.lag) % self.ring],
            self.so.at[j], self.ro.at[j], {"dp": self.outward},
        )

    def begin(self, j):
        for cond, copy in self.sends(j):

            @pl.when(cond)
            def _(copy=copy):
                copy().start()

    def total_of(self, j):
        copy = lambda: pltpu.make_async_copy(
            self.tot.at[(j + self.lag) % self.ring], self.totals.at[j], self.out_sem.at[j]
        )
        return self.valid(self.first + j - self.lag * (2 * self.mid - 2 - self.s)), copy

    def settle(self, j):
        for cond, copy in self.sends(j):

            @pl.when(cond)
            def _(copy=copy):
                copy().wait_send()

        cond, copy = self.total_of(j)

        @pl.when(cond)
        def _():
            copy().wait()

    def end(self, j):
        t, s, mid = self.first + j, self.s, self.mid
        slot, later = j % self.ring, (j + self.lag) % self.ring
        near, next_near = j % self.near, (j + self.lag) % self.near

        @pl.when(j >= 2)
        def _():
            self.settle(j - 2)

        def came(buf, at, sem):
            remote(buf.at[at], buf.at[at], self.si.at[j], sem.at[j], {"dp": self.inward}).wait_recv()

        def add_part(c, buf, at, dst, to):
            for lo, hi, ref in self.parts:

                @pl.when((c >= lo) & (c < hi))
                def _(ref=ref, lo=lo):
                    dst[to] = (ref[c - lo].astype(F32) + buf[at].astype(F32)).astype(BF)

        if mid > 1:
            c = t - self.lag * (s - 1)

            @pl.when((s > 0) & self.valid(c))
            def _():
                came(self.rin, slot, self.ri)
                add_part(c, self.rin, slot, self.acc, next_near)

        @pl.when((s == mid - 1) & self.valid(t - self.lag * (mid - 1)))
        def _():
            came(self.rxb, near, self.rx)
            if mid > 1:
                self.tot[later] = (self.acc[near].astype(F32) + self.rxb[near].astype(F32)).astype(BF)
            else:
                add_part(t, self.rxb, near, self.tot, later)

        cond, copy = self.total_of(j)
        if mid > 1:

            @pl.when((s < mid - 1) & cond)
            def _():
                self.outer(j).wait_recv()

        @pl.when(cond)
        def _():
            copy().start()

    def open(self):
        def one(j, carry):
            self.begin(j)
            return carry

        lax.fori_loop(0, min(self.lag, self.ticks), one, 0)

    def step(self, j):
        self.end(j)

        @pl.when(j + self.lag < self.ticks)
        def _():
            self.begin(j + self.lag)

    def steps(self, start, stop):
        def one(t, carry):
            self.step(t)
            return carry

        lax.fori_loop(start, stop, one, 0)

    def rest(self, j):
        self.steps(j, self.ticks)

        def settle(t, carry):
            self.settle(t)
            return carry

        lax.fori_loop(max(self.ticks - 2, 0), self.ticks, settle, 0)
        if self.carry is not None:
            for b in range(self.lag):
                self.carry[0][b] = self.acc[(self.ticks + b) % self.near]
                self.carry[1][b] = self.tot[(self.ticks + b) % self.ring]


class Io:
    def __init__(self):
        self.coming, self.later, self.going = [], [], []

    def more(self):
        for entry in self.later:
            entry[1].start()
        self.coming += self.later
        self.later = []

    def need(self, *bufs):
        for buf in bufs:
            for at, (ref, copy) in enumerate(self.coming):
                if ref is buf:
                    copy.wait()
                    del self.coming[at]
                    break

    def spill(self, *bufs):
        for buf in bufs:
            for entry in self.going:
                if entry[0] is buf and not entry[2]:
                    entry[1].start()
                    entry[2] = True

    def finish(self):
        self.more()
        self.need(*[ref for ref, _ in self.coming])
        self.spill(*[entry[0] for entry in self.going])
        for _, copy, _ in self.going:
            copy.wait()


def staged(kernel, n_in, fetch, spill, early):
    def wrapped(*refs):
        refs, sems = list(refs[:-1]), refs[-1]
        count = len(fetch) + len(spill)
        refs, bufs = refs[:-count], refs[-count:]
        io = Io()
        for n, i in enumerate(fetch):
            copy = pltpu.make_async_copy(refs[i], bufs[n], sems.at[n])
            if n < early:
                copy.start()
            (io.coming if n < early else io.later).append((bufs[n], copy))
            refs[i] = bufs[n]
        for n, o in enumerate(spill, len(fetch)):
            io.going.append([bufs[n], pltpu.make_async_copy(bufs[n], refs[n_in + o], sems.at[n]), False])
            refs[n_in + o] = bufs[n]
        kernel(io, *refs)
        io.finish()

    return wrapped


def call(kernel, cid, outs, ins, args, scratch, flops, vmem, out_specs, fetch, spill, early=0):
    moved = sum(int(np.prod(a.shape)) * a.dtype.itemsize for a in list(args) + list(outs))
    ins, out_specs = list(ins), list(out_specs)
    held = [pltpu.VMEM(args[i].shape, args[i].dtype) for i in fetch]
    held += [pltpu.VMEM(outs[o].shape, outs[o].dtype) for o in spill]
    for i in fetch:
        ins[i] = ANY
    for o in spill:
        out_specs[o] = ANY
    return pl.pallas_call(
        staged(kernel, len(args), fetch, spill, early),
        out_shape=outs,
        in_specs=ins,
        out_specs=out_specs,
        scratch_shapes=list(scratch) + held + [DMA((len(held),))],
        compiler_params=pltpu.CompilerParams(
            collective_id=cid, has_side_effects=True, vmem_limit_bytes=vmem << 20
        ),
        cost_estimate=pl.CostEstimate(flops=int(flops), bytes_accessed=moved, transcendentals=0),
    )(*args)


def sds(shape, dtype):
    return jax.ShapeDtypeStruct(shape, dtype)


def head_index(iota):
    head, lane = iota // LANE, iota % LANE
    index = jnp.where(lane < HALF, lane, lane - (LANE // 2 - HALF))
    pad = lane % (LANE // 2) >= HALF
    return jnp.where(pad, -1, head * HD + index)


def spread(rows, cols, first):
    source = head_index(lax.broadcasted_iota(jnp.int32, (rows, cols), 1))
    at = lax.broadcasted_iota(jnp.int32, (rows, cols), 0)
    return jnp.where((source >= 0) & (at == source + first), 1.0, 0.0).astype(BF)


def spread_t(rows, cols, first):
    source = head_index(lax.broadcasted_iota(jnp.int32, (rows, cols), 0))
    at = lax.broadcasted_iota(jnp.int32, (rows, cols), 1)
    return jnp.where((source >= 0) & (at == source + first), 1.0, 0.0).astype(BF)


def angle_tables():
    lane = np.arange(LANE)
    freq = np.where(
        lane % (LANE // 2) < HALF, THETA ** (-2.0 * (lane % (LANE // 2)) / HD), 0.0
    )
    fine = np.arange(32)[:, None] * freq[None]
    coarse = fine * 32.0
    return [f(t).astype(np.float32) for t in (coarse, fine) for f in (np.cos, np.sin)]


def exchange(k, stat, sems):
    copy = remote(stat.at[k], stat.at[k], sems.at[0], sems.at[1], {"col": 1 - k})
    copy.start()
    remote(stat.at[1 - k], stat.at[1 - k], sems.at[0], sems.at[1], {"col": 1 - k}).wait_recv()
    copy.wait_send()
    return stat[0][:, 0:1] + stat[1][:, 0:1]


def causal(shape):
    return lax.broadcasted_iota(jnp.int32, shape, 0) <= lax.broadcasted_iota(jnp.int32, shape, 1)


def front_kernel(
    io,
    x, dy, gain, gain_f, wq_h, wk_h, wv_h, wo_h, wg, wu, wd, tables,
    normed_o, f_o, qkv, kvt, wqkv_o, wo_o, wg_o, wu_o, wd_o, cos_o, sin_o, rstd1_o,
    attn, lse, hidden, rstd2_o, part, mid_o, gate_o, up_o,
    buf, dys, stage, gains, give_in, give_out, wq, wk, wv, wo, wsem, wrecv, csem, nsem, fsem,
    stat, ssem, grad, give, gsend, grecv, middle, d_gate, d_up, msem, *rest,
):
    r, k, rx, ry, r3 = place()
    width = x.shape[1]
    f_half = wg.shape[1] // 2
    mate = {"col": 1 - k}
    mine = pl.ds(pl.multiple_of(k * f_half, f_half), f_half)
    his = pl.ds(pl.multiple_of((1 - k) * f_half, f_half), f_half)
    keep = [
        pltpu.make_async_copy(wg.at[:, mine], wg_o.at[k], csem.at[1]),
        pltpu.make_async_copy(wu.at[:, mine], wu_o.at[k], csem.at[2]),
        pltpu.make_async_copy(wd.at[mine], wd_o.at[k], csem.at[3]),
    ]
    first = [
        pltpu.make_async_copy(src, dst, csem.at[4 + n])
        for n, (src, dst) in enumerate(((wq_h, wq), (wk_h, wk), (wv_h, wv), (wo_h, wo)))
    ]
    for c in first + keep:
        c.start()
    greet(rx, ry, k)
    gather = Gather(x, buf, rest[:5])
    gather_dy = Gather(dy, dys, rest[5:10])
    gather_f = Gather(None, buf, rest[10:15])
    total = Sum(rest[15:])
    gains[k] = gain[...].reshape(1, width)
    gather.start()

    def give_to(n, src, dst):
        return remote(src, dst.at[k], wsem.at[n], wrecv.at[n], mate)

    gives = [give_to(0, gains.at[k], gains)]
    gives[0].start()
    heads_q = wq.shape[1] // 2
    heads_k = wk.shape[0] // 2
    nq = heads_q // HD * LANE
    nk = heads_k // HD * LANE
    for c in first:
        c.wait()
    for core, dst_in, dst_out in ((1 - k, give_in, give_out), (k, wqkv_o.at[k], wo_o.at[k])):
        sq = spread(2 * heads_q, nq, core * heads_q)
        sk = spread(2 * heads_k, nk, core * heads_k)
        dst_in[:, 0:nq] = nn(wq[...], sq).astype(BF)
        dst_in[:, nq : nq + nk] = tn(wk[...], sk).astype(BF)
        dst_in[:, nq + nk : nq + 2 * nk] = tn(wv[...], sk).astype(BF)
        dst_out[...] = nn(spread_t(nq, 2 * heads_q, core * heads_q), wo[...]).astype(BF)
    gives += [give_to(1, give_in, wqkv_o), give_to(2, give_out, wo_o)]
    gives += [give_to(3, wg.at[:, his], wg_o), give_to(4, wu.at[:, his], wu_o), give_to(5, wd.at[his], wd_o)]
    for g in gives[1:]:
        g.start()
    sign = jnp.where(lax.broadcasted_iota(jnp.int32, (32, LANE), 1) < LANE // 2, -1.0, 1.0)
    cf, sf = tables[2], tables[3]
    for a in range(LENGTH // 32):
        ca, sa = tables[0, a : a + 1, :], tables[1, a : a + 1, :]
        cos_o[a * 32 : a * 32 + 32, :] = ca * cf - sa * sf
        sin_o[a * 32 : a * 32 + 32, :] = (sa * cf + ca * sf) * sign
    for c in keep:
        c.wait()
    for n in range(3):
        gives[n].wait_recv()

    def keep_normed(i):
        row, half = gather.piece(i)
        return pltpu.make_async_copy(stage.at[i % 2], normed_o.at[:, row, rows_of(half)], nsem.at[i])

    def project(i, row, half):
        at = rows_of(half)
        x0 = buf[0, row, at, :].astype(F32)
        x1 = buf[1, row, at, :].astype(F32)
        square = jnp.sum(x0 * x0, 1, keepdims=True) + jnp.sum(x1 * x1, 1, keepdims=True)
        rstd = lax.rsqrt(square / (2 * width) + EPS)
        n0 = (x0 * rstd * gains[0]).astype(BF)
        n1 = (x1 * rstd * gains[1]).astype(BF)

        @pl.when(i >= 2)
        def _():
            keep_normed(i - 2).wait()

        stage[i % 2, 0] = n0
        stage[i % 2, 1] = n1

        @pl.when(i < 2)
        def _():
            rstd1_o[at, :] = jnp.broadcast_to(rstd, (PIECE, LANE))

        got = nn(n0, wqkv_o[0]) + nn(n1, wqkv_o[1])
        keep_normed(i).start()
        pos = pl.ds(pl.multiple_of((row % 2) * 2 * PIECE + half * PIECE, PIECE), PIECE)
        out = pl.ds(pl.multiple_of(row * 2 * PIECE + half * PIECE, PIECE), PIECE)
        cos, sin = cos_o[pos, :], sin_o[pos, :]
        for p in range(4):
            u = got[:, p * LANE : (p + 1) * LANE]
            if p < 3:
                u = u * cos + pltpu.roll(u, LANE // 2, 1) * sin
            qkv[p, out, :] = u.astype(BF)
            if p >= 2:
                kvt[p - 2, :, out] = u.T.astype(BF)

    def dy_too(q):
        @pl.when(q == 0)
        def _():
            gather_dy.start()

    gather.run(project, None, dy_too)
    for i in (6, 7):
        keep_normed(i).wait()

    def attend(row, half):
        base = pl.multiple_of(row // 2 * LENGTH, LENGTH)
        at = rows_of(half)
        qrow = pl.ds(pl.multiple_of(row * 2 * PIECE + half * PIECE, PIECE), PIECE)
        order = (row % 2) * 2 + half

        def queries(p):
            span = PIECE * (p + 1)
            for head in range(2):
                keys = qkv[2, pl.ds(base, span), :]
                s = nt(keys, qkv[head, qrow, :])
                tail = jnp.where(causal((PIECE, PIECE)), s[span - PIECE :], -1e30)
                s = tail if p == 0 else jnp.concatenate([s[: span - PIECE], tail], 0)
                top = jnp.max(s, 0, keepdims=True)
                e = jnp.exp((s - top) * SCALE)
                weight = jnp.sum(e, 0, keepdims=True)
                probs = (e * (1.0 / weight)).astype(BF)
                mixed = nn(kvt[1, :, pl.ds(base, span)], probs)
                attn[row, at, head * LANE : (head + 1) * LANE] = mixed.T.astype(BF)
                lse[head, row * 2 + half] = top * SCALE + jnp.log(weight)

        for p in range(4):
            pl.when(order == p)(lambda p=p: queries(p))
        a = attn[row, at, :]
        return nn(a, wo_o[k]), nn(a, wo_o[1 - k])

    def dy_arrive(j):
        @pl.when(j == 3)
        def _():
            gather_dy.arrive(2)
            gather_dy.arrive(3)

        @pl.when(j == 7)
        def _():
            gather_dy.arrive(4)
            gather_dy.arrive(5)

    total.send_all(attend, dy_arrive)
    io.spill(qkv, kvt, cos_o, sin_o, attn, wqkv_o, wo_o)
    for g in gives[3:]:
        g.wait_recv()
    io.spill(wg_o, wu_o, wd_o)
    gather_dy.local().wait()

    def mid_pair(q, carry):
        for u in range(2):
            i = 2 * q + u
            gather_dy.ready(i)
            row, half = gather_dy.piece(i)
            at = rows_of(half)
            d_mid = nt(dys[0, row, at, :], wd_o[0]) + nt(dys[1, row, at, :], wd_o[1])
            d_gate[row, at, :] = d_mid.astype(BF)
        return carry

    lax.fori_loop(0, 3, mid_pair, 0)
    gather_dy.arrive(6)
    gather_dy.arrive(7)
    total.relay(4)
    total.relay(5)
    mid_pair(3, 0)
    gather_dy.finish()
    for half in range(2):
        at = rows_of(half)
        h = buf[k, r, at, :].astype(F32) + total.last(6 + half)
        hidden[at, :] = h
        stat[k, at, :] = jnp.broadcast_to(jnp.sum(h * h, 1, keepdims=True), (PIECE, LANE))
    rstd2 = lax.rsqrt(exchange(k, stat, ssem) / (2 * width) + EPS)
    buf[k, r] = (hidden[...] * rstd2 * gain_f[...].reshape(1, width)).astype(BF)
    rstd2_o[...] = jnp.broadcast_to(rstd2, rstd2_o.shape)
    gather_f.start()
    io.spill(hidden)

    def keep_mids(i):
        row, half = gather_f.piece(i)
        at = rows_of(half)
        return [
            pltpu.make_async_copy(src.at[row, at], dst.at[row, at], msem.at[n, i])
            for n, (src, dst) in enumerate(((middle, mid_o), (d_gate, gate_o), (d_up, up_o)))
        ]

    def keep_f(i):
        row, half = gather_f.piece(i)
        at = rows_of(half)
        return pltpu.make_async_copy(buf.at[:, row, at], f_o.at[:, row, at], fsem.at[i])

    def expand(i, row, half):
        at = rows_of(half)
        keep_f(i).start()

        @pl.when(i > 0)
        def _():
            for c in keep_mids(i - 1):
                c.start()

        f0, f1 = buf[0, row, at, :], buf[1, row, at, :]
        dy0, dy1 = dys[0, row, at, :], dys[1, row, at, :]
        gate = nn(f0, wg_o[0]) + nn(f1, wg_o[1])
        upper = nn(f0, wu_o[0]) + nn(f1, wu_o[1])
        d_mid = d_gate[row, at, :].astype(F32)
        sig = 1.0 / (1.0 + jnp.exp(-gate))
        swish = gate * sig
        mid = (swish * upper).astype(BF)
        middle[row, at, :] = mid
        d_gate[row, at, :] = (d_mid * upper * sig * (1.0 + gate * (1.0 - sig))).astype(BF)
        d_up[row, at, :] = (d_mid * swish).astype(BF)
        g0, g1 = tn(mid, dy0), tn(mid, dy1)

        @pl.when(i == 0)
        def _():
            grad[0] = g0
            grad[1] = g1

        @pl.when(i > 0)
        def _():
            grad[0] += g0
            grad[1] += g1

    gather_f.run(expand)
    for c in keep_mids(7):
        c.start()
    half = DOWN_CHUNKS // 4

    def swap(j, core):
        return remote(
            give.at[pl.ds(2 * j, 2)], part.at[pl.ds(2 * (half * core + j), 2)], gsend.at[j], grecv.at[j], mate
        )

    for j in range(half):
        for h in range(2):
            give[2 * j + h] = grad[1 - k, j * TALL + h * CHUNK : j * TALL + (h + 1) * CHUNK, :].astype(BF)
        swap(j, k).start()
    for j in range(half):
        for h in range(2):
            rows = slice(j * TALL + h * CHUNK, j * TALL + (h + 1) * CHUNK)
            part[2 * (half * k + j) + h] = grad[k, rows, :].astype(BF)
    for j in range(half):
        swap(j, 1 - k).wait_recv()
    io.spill(part)

    def kept(i, carry):
        keep_f(i).wait()
        for c in keep_mids(i):
            c.wait()
        return carry

    lax.fori_loop(0, 8, kept, 0)
    for j in range(half):
        swap(j, k).wait_send()
    for g in gives:
        g.wait_send()
    total.finish()


def front(x, dy, gain, gain_f, wq, wk, wv, wo, wg, wu, wd):
    tokens, width = x.shape
    f_half = wg.shape[1] // 2
    cols = 4 * LANE
    gathered = (2, 4, tokens, width)
    outs = [sds(gathered, BF), sds(gathered, BF)]
    outs += [sds((4, 4 * tokens, LANE), BF), sds((2, LANE, 4 * tokens), BF)]
    outs += [sds((2, width, cols), BF), sds((2, 2 * LANE, width), BF)]
    outs += [sds((2, width, f_half), BF)] * 2 + [sds((2, f_half, width), BF)]
    outs += [sds((LENGTH, LANE), F32)] * 2 + [sds((tokens, LANE), F32)]
    outs += [sds((4, tokens, 2 * LANE), BF), sds((2, 8, 1, PIECE), F32)]
    outs += [sds((tokens, width), F32), sds((tokens, LANE), F32)]
    outs += [sds((DOWN_CHUNKS, CHUNK, WIDE), BF)] + [sds((4, tokens, f_half), BF)] * 3
    half = DOWN_CHUNKS // 4
    scratch = [pltpu.VMEM(gathered, BF)] * 2 + [pltpu.VMEM((2, 2, PIECE, width), BF)]
    scratch += [pltpu.VMEM((2, 1, width), F32), pltpu.VMEM((width, cols), BF), pltpu.VMEM((2 * LANE, width), BF)]
    scratch += [pltpu.VMEM(w.shape, BF) for w in (wq, wk, wv, wo)]
    scratch += [DMA((6,)), DMA((6,)), DMA((8,)), DMA((8,)), DMA((8,))]
    scratch += [pltpu.VMEM((2, tokens, LANE), F32), DMA((2,)), pltpu.VMEM((2, f_half, width), F32)]
    scratch += [pltpu.VMEM((2 * half, CHUNK, WIDE), BF), DMA((half,)), DMA((half,))]
    scratch += [pltpu.VMEM((4, tokens, f_half), BF)] * 3 + [DMA((3, 8))]
    scratch += GATHER_SEMS * 3 + sum_scratch(width)
    ins = [ANY] * 2 + [VM] * 2 + [ANY] * 7 + [VM]
    args = [x, dy, gain, gain_f, wq, wk, wv, wo, wg, wu, wd, jnp.asarray(np.stack(angle_tables()))]
    out_specs = [ANY] * 2 + [VM] * (len(outs) - 5) + [ANY] * 3
    spill = [2, 3, 4, 5, 6, 7, 8, 9, 10, 12, 14, 16]
    return call(front_kernel, 0, outs, ins, args, scratch, 9e10, 61, out_specs, [], spill)


TICKS = 34


def flat(ref, h, m=None):
    got = ref[h] if m is None else ref[h, :, :, pl.ds(pl.multiple_of(m * 256, 256), 256)]
    return got.reshape(-1, got.shape[-1])


def contract_kernel(
    io,
    d_gate, d_up, wg, wu, hidden, rstd2, gain, dy, wo, attn, part_d, f_any,
    d_hidden, gains_o, part, part_o, d_attn, totals, acc_c, tot_c,
    stat, ssem, give, gsend, grecv, gathered, dya, grad, give_o, his_o, gsem, fsem, *rest,
):
    r, k, rx, ry, r3 = place()
    width = hidden.shape[1]
    fetch = pltpu.make_async_copy(f_any, gathered, fsem)
    greet(rx, ry, k, True)
    total = Sum(rest[:9])
    gather = Gather(dya, gathered, rest[9:14])
    parts = [(0, DOWN_CHUNKS, part_d), (DOWN_CHUNKS, MLP_CHUNKS, part), (MLP_CHUNKS, OUT_CHUNKS, part_o)]
    lag = lags(lax.axis_size("dp"))[0]
    line = Line(parts, totals, (acc_c, tot_c), rest[14:], 0, TICKS, OUT_CHUNKS, lag)
    io.need(d_gate, d_up, wg, wu, part_d)
    line.open()
    fetch.start()
    io.more()

    def compute(row, half):
        at = rows_of(half)
        g, u = d_gate[row, at, :], d_up[row, at, :]
        return nt(g, wg[k]) + nt(u, wu[k]), nt(g, wg[1 - k]) + nt(u, wu[1 - k])

    def early(j):
        @pl.when(j % 2 == 1)
        def _():
            line.step(j // 2)

    total.send_all(compute, early)

    def swap(e, core):
        to = part.at[pl.ds(2 * (e // 4 * 8 + 4 * core + e % 4), 2)]
        return remote(give.at[pl.ds(2 * e, 2)], to, gsend.at[e], grecv.at[e], {"col": 1 - k})

    def wide_part(h, right, dst, first):
        def one(m, carry):
            got = tn(flat(gathered, h, m), right[...].reshape(-1, right.shape[2])).astype(BF)
            for b in range(2):
                lanes = pl.ds(pl.multiple_of((2 * m + b) * TALL, TALL), TALL)
                for j in range(4):
                    for u in range(2):
                        rows = slice(b * TALL + u * CHUNK, b * TALL + (u + 1) * CHUNK)
                        dst[2 * (first + j) + u, :, lanes] = got[rows, j * TALL : (j + 1) * TALL]
            return carry

        lax.fori_loop(0, width // 256, one, 0)

    fetch.wait()
    wide_part(1 - k, d_gate, give, 0)
    for e in range(4):
        swap(e, k).start()
    wide_part(k, d_gate, part, 4 * k)
    line.steps(4, 6)
    wide_part(1 - k, d_up, give, 4)
    for e in range(4, 8):
        swap(e, k).start()
    wide_part(k, d_up, part, 8 + 4 * k)
    total.relay(4)
    total.relay(5)
    for e in range(8):
        swap(e, 1 - k).wait_recv()
    io.spill(part)
    io.need(hidden, dy, wo, attn)
    line.steps(6, 13)
    gains = jnp.zeros((1, width), F32)
    for half in range(2):
        at = rows_of(half)
        d_nf = total.last(6 + half)
        h = hidden[at, :]
        gains = gains + jnp.sum(d_nf * h * rstd2[at, 0:1], 0, keepdims=True)
        scaled = d_nf * gain[...].reshape(1, width)
        d_hidden[at, :] = scaled
        stat[k, at, :] = jnp.broadcast_to(jnp.sum(scaled * h, 1, keepdims=True), (PIECE, LANE))
    gains_o[...] = gains
    inner = exchange(k, stat, ssem) / (2 * width)
    rs = rstd2[:, 0:1]
    value = dy[...].astype(F32) + rs * d_hidden[...] - hidden[...] * (rs * rs * rs * inner)
    d_hidden[...] = value
    dya[...] = value.astype(BF)
    gather.start()
    io.spill(d_hidden)

    def piece(i, row, half):
        at = rows_of(half)
        d0, d1 = gathered[0, row, at, :], gathered[1, row, at, :]
        d_attn[row, at, :] = (nt(d0, wo[0]) + nt(d1, wo[1])).astype(BF)
        a = attn[row, at, :]
        g0, g1 = tn(a, d0), tn(a, d1)

        @pl.when(i == 0)
        def _():
            grad[0] = g0
            grad[1] = g1

        @pl.when(i > 0)
        def _():
            grad[0] += g0
            grad[1] += g1

    def before(q):
        line.steps(jnp.where(q == 0, 13, 15 + 4 * q), 19 + 4 * q)

    gather.run(piece, before)
    give_o[...] = grad[1 - k].astype(BF)
    give_out = remote(give_o, his_o, gsem.at[0], gsem.at[1], {"col": 1 - k})
    give_out.start()
    q_cols = part_o.shape[0] * CHUNK
    mine = nn(spread(q_cols, 2 * LANE, k * (q_cols // 2)), grad[k].astype(BF))
    give_out.wait_recv()
    out = mine + nn(spread(q_cols, 2 * LANE, (1 - k) * (q_cols // 2)), his_o[...])
    for c in range(q_cols // CHUNK):
        part_o[c] = out[c * CHUNK : (c + 1) * CHUNK].astype(BF)
    line.rest(31)
    for e in range(8):
        swap(e, k).wait_send()
    give_out.wait_send()
    total.finish()


def contract(d_gate, d_up, wg, wu, hidden, rstd2, gain, dy, wo, attn, part_d, all_f):
    tokens, width = hidden.shape
    n = lax.axis_size("dp")
    outs = [sds((tokens, width), F32), sds((1, width), F32)]
    outs += [sds((MLP_CHUNKS - DOWN_CHUNKS, CHUNK, WIDE), BF), sds((OUT_CHUNKS - MLP_CHUNKS, CHUNK, WIDE), BF)]
    outs += [sds((4, tokens, 2 * LANE), BF)] + line_outs(TICKS, lags(n)[0])
    out_specs = [VM] * 5 + [ANY] + [VM] * 2
    scratch = [pltpu.VMEM((2, tokens, LANE), F32), DMA((2,))]
    scratch += [pltpu.VMEM((16, CHUNK, WIDE), BF), DMA((8,)), DMA((8,))]
    scratch += [pltpu.VMEM((2, 4, tokens, width), BF), pltpu.VMEM((tokens, width), BF)]
    scratch += [pltpu.VMEM((2, 2 * LANE, width), F32)] + [pltpu.VMEM((2 * LANE, width), BF)] * 2
    scratch += [DMA((2,)), DMA]
    scratch += sum_scratch(width) + GATHER_SEMS + line_scratch(n, TICKS, lags(n)[0])
    args = [d_gate, d_up, wg, wu, hidden, rstd2, gain, dy, wo, attn, part_d, all_f]
    ins = [VM] * 11 + [ANY]
    fetch = [0, 1, 2, 3, 10, 4, 7, 8, 9]
    return call(
        contract_kernel, 1, outs, ins, args, scratch, 5e10, vmem_limit(n), out_specs, fetch, [0, 2, 3, 4], 5
    )


def vmem_limit(n):
    return 60 if n <= 4 else 63


def columns(rows, cols, core, q_cols, k_cols):
    i = lax.broadcasted_iota(jnp.int32, (rows, cols), 0)
    at = lax.broadcasted_iota(jnp.int32, (rows, cols), 1)
    part, lane = i // LANE, i % LANE
    index = jnp.where(lane < HALF, lane, lane - (LANE // 2 - HALF))
    q = core * (q_cols // 2) + part * HD
    kv = q_cols + (part - 2) * k_cols + core * (k_cols // 2)
    to = jnp.where(part < 2, q, kv) + index
    pad = lane % (LANE // 2) >= HALF
    return jnp.where((at == to) & (pad == False), 1.0, 0.0).astype(BF)


def backward_kernel(
    q_cols, k_cols,
    io,
    qkv, kvt, lse, d_attn, cos, sin, middle, wd, hidden, wqkv, x, rstd1, d_hidden, gain, gains_f,
    part_m, part_o, acc_c, tot_c, normed_any,
    output, grad_x, gains_o, totals, totals_in,
    dk, dv, d_proj, normed, part, mine, give, his, gsem, stat, ssem, free, fsem,
    mine_g, pair_g, slots, gsend, grecv, *rest,
):
    r, k, rx, ry, r3 = place()
    width = x.shape[1]
    n = lax.axis_size("dp")
    z = lax.axis_index("dp")
    fetch = pltpu.make_async_copy(normed_any, normed, fsem)
    greet(rx, ry, k, True, True)
    sums = rest[:5]
    down = Sum(sums + rest[5:9])
    into = Sum(sums + rest[9:13])
    lag, lag_in = lags(n)
    count = ALL_CHUNKS - OUT_CHUNKS
    ticks, ticks_in = line_ticks(n, OUT_CHUNKS, lag) - TICKS, line_ticks(n, count, lag_in)
    parts = [(DOWN_CHUNKS, MLP_CHUNKS, part_m), (MLP_CHUNKS, OUT_CHUNKS, part_o)]
    line = Line(parts, totals, None, rest[13:23], TICKS, ticks, OUT_CHUNKS, lag, (acc_c, tot_c))
    line_in = Line([(0, count, part)], totals_in, None, rest[23:], 0, ticks_in, count, lag_in)
    io.need(part_m, part_o, middle, wd)
    line.open()
    io.more()

    def down_piece(row, half):
        m = middle[row, rows_of(half), :]
        return nn(m, wd[k]), nn(m, wd[1 - k])

    def early(j):
        @pl.when(j % 3 == 1)
        def _():
            line.step(j // 3)

    down.send_all(down_piece, early)

    fetch.start()
    io.need(qkv, kvt, d_attn, cos, sin)

    def unrotate(u, p):
        at = pl.ds(p * PIECE, PIECE)
        return u * cos[at, :] - pltpu.roll(u, LANE // 2, 1) * sin[at, :]

    def sequence(seq):
        base = pl.multiple_of(seq * LENGTH, LENGTH)

        def one_head(head, carry):
            for p in range(4):
                span = PIECE * (p + 1)
                row = seq * 2 + p // 2
                at = pl.ds((p % 2) * PIECE, PIECE)
                out = pl.ds(pl.multiple_of(base + p * PIECE, PIECE), PIECE)
                keys = qkv[2, pl.ds(base, span), :]
                q = qkv[head, out, :]
                lane = pl.ds(pl.multiple_of(head * LANE, LANE), LANE)
                do = d_attn[row, at, lane]
                e = jnp.exp(nt(keys, q) * SCALE - lse[head, seq * 4 + p])
                tail = jnp.where(causal((PIECE, PIECE)), e[span - PIECE :], 0.0)
                e = tail if p == 0 else jnp.concatenate([e[: span - PIECE], tail], 0)
                dp = nt(qkv[3, pl.ds(base, span), :], do)
                inner = jnp.sum(e * dp, 0, keepdims=True)
                ds = (e * (dp - inner)).astype(BF)
                dv[0:span, :] += nn(e.astype(BF), do)
                dk[0:span, :] += nn(ds, q)
                dq = nn(kvt[0, :, pl.ds(base, span)], ds).T * SCALE
                d_proj[out, lane] = unrotate(dq, p).astype(BF)
                if p % 2 == 1:
                    tick = 3 + seq * 8 + head * 4 + p - 1
                    line.steps(tick, tick + 2)
            return carry

        dk[...] = jnp.zeros_like(dk)
        dv[...] = jnp.zeros_like(dv)
        lax.fori_loop(0, 2, one_head, 0)
        for p in range(4):
            at = pl.ds(p * PIECE, PIECE)
            out = pl.ds(pl.multiple_of(base + p * PIECE, PIECE), PIECE)
            d_proj[out, 2 * LANE : 3 * LANE] = unrotate(dk[at, :] * SCALE, p).astype(BF)
            d_proj[out, 3 * LANE : 4 * LANE] = dv[at, :].astype(BF)

    def both(seq, carry):
        sequence(seq)

        @pl.when(seq == 0)
        def _():
            down.relay(4)
            down.relay(5)

        return carry

    lax.fori_loop(0, 2, both, 0)
    io.need(hidden)
    for half in range(2):
        at = rows_of(half)
        output[at, :] = hidden[at, :] + down.last(6 + half)
    down.finish()
    io.spill(output)
    for device in ({"row": rx}, {"row": ry}, {"col": 1 - k}):
        pl.semaphore_signal(free, inc=1, device_id=device, device_id_type=MESH)
    pl.semaphore_wait(free, 3)

    fetch.wait()

    def in_part(h, dst):
        def one(m, carry):
            dst[pl.ds(pl.multiple_of(m * 256, 256), 256), :] = tn(flat(normed, h, m), d_proj[...]).astype(BF)
            return carry

        lax.fori_loop(0, width // 256, one, 0)

    in_part(1 - k, give)
    swap = remote(give, his, gsem.at[0], gsem.at[1], {"col": 1 - k})
    swap.start()
    line.steps(19, 21)
    in_part(k, mine)
    line.steps(21, 23)
    cols = q_cols + 2 * k_cols
    got = nn(mine[...], columns(4 * LANE, cols, k, q_cols, k_cols))
    swap.wait_recv()
    got = got + nn(his[...], columns(4 * LANE, cols, 1 - k, q_cols, k_cols))
    for c in range(width // CHUNK):
        part[c] = got[c * CHUNK : (c + 1) * CHUNK].astype(BF)

    def into_piece(row, half):
        d = d_proj[pl.ds(pl.multiple_of(row * 2 * PIECE + half * PIECE, PIECE), PIECE), :]
        return nt(d, wqkv[k]), nt(d, wqkv[1 - k])

    line_in.open()

    def both_lines(t, carry):
        line.step(23 + t)
        line_in.step(t)
        return carry

    def beside(j):
        @pl.when(j % 2 == 1)
        def _():
            both_lines(j // 2, 0)

    io.need(wqkv)
    into.send_all(into_piece, beside)
    lax.fori_loop(4, 5, both_lines, 0)
    line_in.steps(5, 7)
    into.relay(4)
    into.relay(5)
    line_in.steps(7, 12)
    io.need(x, d_hidden)
    gains = jnp.zeros((1, width), F32)
    for half in range(2):
        at = rows_of(half)
        d_na = into.last(6 + half)
        xs = x[at, :].astype(F32)
        gains = gains + jnp.sum(d_na * xs * rstd1[at, 0:1], 0, keepdims=True)
        scaled = d_na * gain[...].reshape(1, width)
        grad_x[at, :] = scaled
        stat[k, at, :] = jnp.broadcast_to(jnp.sum(scaled * xs, 1, keepdims=True), (PIECE, LANE))

    def row_total(step, device):
        copy = remote(mine_g.at[step], pair_g.at[step], gsend.at[n + step], grecv.at[n + step], {"row": device})
        copy.start()
        return copy

    mine_g[0, 0:1] = gains
    mine_g[0, 1:2] = gains_f[...]
    over_x = row_total(0, rx)
    inner = exchange(k, stat, ssem) / (2 * width)
    rs = rstd1[:, 0:1]
    over_x.wait_recv()
    mine_g[1] = mine_g[0] + pair_g[0]
    over_y = row_total(1, ry)
    grad_x[...] = d_hidden[...] + rs * grad_x[...] - x[...].astype(F32) * (rs * rs * rs * inner)
    over_y.wait_recv()
    slots[z] = mine_g[1] + pair_g[1]

    def over_dp(t, mine):
        other = (z + t) % n
        g = z if mine else other
        return remote(slots.at[g], slots.at[g], gsend.at[t], grecv.at[g], {"dp": other})

    def start(t, carry):
        over_dp(t, True).start()
        return carry

    lax.fori_loop(1, n, start, 0)
    io.spill(grad_x)
    line_in.rest(12)
    line.rest(28)

    def wait(t, carry):
        over_dp(t, False).wait_recv()
        over_dp(t, True).wait_send()
        return carry

    lax.fori_loop(1, n, wait, 0)
    gains_o[...] = lax.fori_loop(1, n, lambda g, total: total + slots[g], slots[0])
    over_x.wait_send()
    over_y.wait_send()
    swap.wait_send()
    into.finish()


def backward(
    qkv, kvt, lse, d_attn, cos, sin, middle, wd, hidden, wqkv, x, rstd1, d_hidden, gain, gains_f,
    part_m, part_o, acc, tot, normed, q_cols, k_cols,
):
    tokens, width = x.shape
    n = lax.axis_size("dp")
    lag, lag_in = lags(n)
    ticks = line_ticks(n, OUT_CHUNKS, lag) - TICKS
    ticks_in = line_ticks(n, ALL_CHUNKS - OUT_CHUNKS, lag_in)
    outs = [sds((tokens, width), F32)] * 2 + [sds((2, width), F32)]
    outs += [sds((t, CHUNK, WIDE), BF) for t in (ticks, ticks_in)]
    scratch = [pltpu.VMEM((LENGTH, LANE), F32)] * 2 + [pltpu.VMEM((4 * tokens, 4 * LANE), BF)]
    scratch += [pltpu.VMEM((2, 4, tokens, width), BF), pltpu.VMEM((ALL_CHUNKS - OUT_CHUNKS, CHUNK, WIDE), BF)]
    scratch += [pltpu.VMEM((width, 4 * LANE), BF)] * 3 + [DMA((2,))]
    scratch += [pltpu.VMEM((2, tokens, LANE), F32), DMA((2,)), pltpu.SemaphoreType.REGULAR, DMA]
    scratch += [pltpu.VMEM((2, 2, width), F32)] * 2 + [pltpu.VMEM((n, 2, width), F32)]
    scratch += [DMA((n + 2,)), DMA((n + 2,))]
    both = sum_scratch(width)
    scratch += both + both[5:] + line_scratch(n, ticks, lag) + line_scratch(n, ticks_in, lag_in)
    args = [qkv, kvt, lse, d_attn, cos, sin, middle, wd, hidden, wqkv, x, rstd1, d_hidden, gain, gains_f]
    args += [part_m, part_o, acc, tot, normed]
    kernel = functools.partial(backward_kernel, q_cols, k_cols)
    ins = [VM] * (len(args) - 1) + [ANY]
    fetch = [15, 16, 6, 7, 0, 1, 3, 4, 5, 8, 9, 10, 12]
    return call(
        kernel, 2, outs, ins, args, scratch, 5e10, vmem_limit(n), [VM] * 3 + [ANY] * 2, fetch, [0, 1], 4
    )


SLOTS = 4


def unpack_kernel(q_cols, k_cols, tot1, tot2, tot3, down, gate, up, out, q_o, k_o, v_o, whole, last, wide, turned, isem, osem):
    n, s, _, _ = line_place()
    steps = 2 * (n // 2) - 2 - s
    lag, lag_in = lags(n)
    first = tot1.shape[0]
    loads = [
        pltpu.make_async_copy(tot1, whole.at[pl.ds(0, first)], isem.at[0]),
        pltpu.make_async_copy(tot2, whole.at[pl.ds(first, tot2.shape[0])], isem.at[1]),
        pltpu.make_async_copy(tot3, last, isem.at[2]),
    ]
    for c in loads:
        c.start()
    loads[0].wait()
    late = whole.shape[0] - OUT_CHUNKS > first - DOWN_CHUNKS
    if late:
        loads[1].wait()

    def chunk(c, lanes):
        return whole[c + lag * steps, :, lanes].astype(F32)

    def run(count, make, copies):
        def one(b, carry):
            slot = b % SLOTS

            @pl.when(b >= SLOTS)
            def _():
                for c in copies(b - SLOTS, slot):
                    c.wait()

            make(b, slot)
            for c in copies(b, slot):
                c.start()
            return carry

        lax.fori_loop(0, count, one, 0)

        def drain(b, carry):
            for c in copies(b, b % SLOTS):
                c.wait()
            return carry

        lax.fori_loop(max(count - SLOTS, 0), count, drain, 0)

    def rows(b):
        return pl.ds(pl.multiple_of(b * TALL, TALL), TALL)

    def tall(start, to, count):
        def make(b, slot):
            for u in range(2):
                wide[slot, u * CHUNK : (u + 1) * CHUNK, 0:WIDE] = chunk(start + 2 * b + u, slice(0, WIDE))

        def copies(b, slot):
            return [pltpu.make_async_copy(wide.at[slot, :, pl.ds(0, WIDE)], to.at[rows(b)], osem.at[slot, 0])]

        run(count, make, copies)

    def broad(start, to):
        def make(b, slot):
            for c in range(8):
                for u in range(2):
                    got = chunk(start + 2 * c + u, rows(b))
                    wide[slot, u * CHUNK : (u + 1) * CHUNK, c * TALL : (c + 1) * TALL] = got

        def copies(b, slot):
            return [pltpu.make_async_copy(wide.at[slot], to.at[rows(b)], osem.at[slot, 0])]

        run(WIDE // TALL, make, copies)

    tall(0, down, 8)
    if not late:
        loads[1].wait()
    broad(DOWN_CHUNKS, gate)
    broad(DOWN_CHUNKS + 16, up)
    tall(MLP_CHUNKS, out, q_cols // TALL)
    loads[2].wait()

    def make_in(b, slot):
        for u in range(2):
            got = last[2 * b + u + lag_in * steps].astype(F32)
            wide[slot, u * CHUNK : (u + 1) * CHUNK, 0:WIDE] = got
        turned[slot, 0] = wide[slot, :, q_cols : q_cols + k_cols].T
        turned[slot, 1] = wide[slot, :, q_cols + k_cols : WIDE].T

    def copies_in(b, slot):
        return [
            pltpu.make_async_copy(wide.at[slot, :, pl.ds(0, q_cols)], q_o.at[rows(b)], osem.at[slot, 0]),
            pltpu.make_async_copy(turned.at[slot, 0], k_o.at[:, rows(b)], osem.at[slot, 1]),
            pltpu.make_async_copy(turned.at[slot, 1], v_o.at[:, rows(b)], osem.at[slot, 2]),
        ]

    run(WIDE // TALL, make_in, copies_in)


def unpack(tots, q_cols, k_cols):
    outs = [sds((8 * TALL, WIDE), F32), sds((WIDE, 8 * TALL), F32), sds((WIDE, 8 * TALL), F32)]
    outs += [sds((q_cols, WIDE), F32), sds((WIDE, q_cols), F32), sds((k_cols, WIDE), F32), sds((k_cols, WIDE), F32)]
    return pl.pallas_call(
        functools.partial(unpack_kernel, q_cols, k_cols),
        out_shape=outs,
        in_specs=[ANY] * 3,
        out_specs=[ANY] * len(outs),
        scratch_shapes=[
            pltpu.VMEM((tots[0].shape[0] + tots[1].shape[0], CHUNK, WIDE), BF),
            pltpu.VMEM(tots[2].shape, BF),
            pltpu.VMEM((SLOTS, TALL, 8 * TALL), F32),
            pltpu.VMEM((SLOTS, 2, k_cols, TALL), F32),
            DMA((3,)),
            DMA((SLOTS, 3)),
        ],
        compiler_params=pltpu.CompilerParams(vmem_limit_bytes=62 << 20),
        cost_estimate=pl.CostEstimate(flops=0, bytes_accessed=3 * ALL_CHUNKS * TALL * WIDE, transcendentals=0),
    )(*tots)


def on_device(
    layer_input, gain_attn, gain_ffn, w_query, w_key, w_value, w_out, w_gate, w_up, w_down, cotangent
):
    tokens, width = layer_input.shape
    q_cols, k_cols = w_query.shape[1], w_key.shape[1]
    gain_a, gain_f = gain_attn, gain_ffn
    (
        normed, all_f, qkv, kvt, wqkv, wo, wg, wu, wd, cos, sin, rstd1,
        attn, lse, hidden, rstd2, part_d, middle, d_gate, d_up,
    ) = front(
        layer_input, cotangent, gain_a, gain_f,
        w_query, w_key.T, w_value.T, w_out, w_gate, w_up, w_down,
    )
    d_hidden, gains_f, part_m, part_o, d_attn, tot1, acc, tot = contract(
        d_gate, d_up, wg, wu, hidden, rstd2, gain_f, cotangent, wo, attn, part_d, all_f
    )
    output, grad_x, gains, tot2, tot3 = backward(
        qkv, kvt, lse, d_attn, cos, sin, middle, wd, hidden, wqkv, layer_input, rstd1, d_hidden,
        gain_a, gains_f, part_m, part_o, acc, tot, normed, q_cols, k_cols,
    )
    down, gate, up, out, g_q, g_k, g_v = unpack([tot1, tot2, tot3], q_cols, k_cols)
    return output, grad_x, gains[0], gains[1], g_q, g_k.T, g_v.T, out, gate, up, down


def solution(mesh):
    assert mesh.shape["row"] == 4 and mesh.shape["col"] == 2
    tokens = P(("dp", "row"), "col")
    wide = P("col", "row")
    tall = P("row", "col")
    return jax.shard_map(
        on_device,
        mesh=mesh,
        in_specs=(tokens, P("col"), P("col"), wide, wide, wide, tall, wide, wide, tall, tokens),
        out_specs=(tokens, tokens, P("col"), P("col"), wide, wide, wide, tall, wide, wide, tall),
        check_vma=False,
    )
```

```python
import functools

import jax
import jax.numpy as jnp
import numpy as np
from jax import lax
from jax.experimental import pallas as pl
from jax.experimental.pallas import tpu as pltpu
from jax.sharding import PartitionSpec as P

HD = 96
HALF = HD // 2
LENGTH = 1024
EPS = 1e-05
THETA = 100000.0
SCALE = HD ** (-0.5)
LANE = 128
PIECE = 256

BF = jnp.bfloat16
F32 = jnp.float32
MESH = pl.DeviceIdType.MESH
VM = pl.BlockSpec(memory_space=pltpu.VMEM)
ANY = pl.BlockSpec(memory_space=pl.ANY)
DMA = pltpu.SemaphoreType.DMA


def nn(a, b):
    return lax.dot_general(a, b, (((1,), (0,)), ((), ())), preferred_element_type=F32)


def nt(a, b):
    return lax.dot_general(a, b, (((1,), (1,)), ((), ())), preferred_element_type=F32)


def place():
    r = lax.axis_index("row")
    k = lax.axis_index("col")
    return r, k, r + 1 - 2 * (r % 2), (r + 2) % 4, 3 - r


def tn(a, b):
    return lax.dot_general(a, b, (((0,), (0,)), ((), ())), preferred_element_type=F32)


def line_place():
    n = lax.axis_size("dp")
    z = lax.axis_index("dp")
    left = z < n // 2
    step = jnp.where(left, 1, -1)
    return n, jnp.where(left, z, n - 1 - z), z + step, z - step


def greet(rx, ry, k, line=False, groups=False):
    bar = pltpu.get_barrier_semaphore()

    def hello(device):
        pl.semaphore_signal(bar, inc=1, device_id=device, device_id_type=MESH)

    for device in ({"row": rx}, {"row": ry}, {"col": 1 - k}):
        hello(device)
    if not line:
        pl.semaphore_wait(bar, 3)
        return
    n, s, inward, outward = line_place()
    if groups:
        z = lax.axis_index("dp")

        def one(t, carry):
            hello({"dp": (z + t) % n})
            return carry

        lax.fori_loop(1, n, one, 0)
        pl.semaphore_wait(bar, 3 + n - 1)
        return
    hello({"dp": inward})

    @pl.when(s > 0)
    def _():
        hello({"dp": outward})

    pl.semaphore_wait(bar, jnp.where(s > 0, 5, 4))


def remote(src, dst, send, recv, device):
    return pltpu.make_async_remote_copy(
        src_ref=src, dst_ref=dst, send_sem=send, recv_sem=recv, device_id=device, device_id_type=MESH
    )


def rows_of(half):
    return pl.ds(pl.multiple_of(half * PIECE, PIECE), PIECE)


GATHER_SEMS = [DMA((6,)), DMA((6,)), DMA((8,)), DMA((8,)), DMA]


class Gather:
    def __init__(self, own, buf, sems):
        self.own, self.buf = own, buf
        self.isend, self.irecv, self.dsend, self.drecv, self.lsem = sems
        self.r, self.k, self.rx, self.ry, self.r3 = place()

    def piece(self, i):
        side = jnp.where(i % 2 == 0, self.rx, self.ry)
        row = jnp.where(i < 2, self.r, jnp.where(i < 6, side, self.r3))
        half = jnp.where(i // 2 == 2, 1 - i % 2, i % 2)
        return row, half

    def ici(self, sem, row, half, device, src=None):
        dst = self.buf.at[self.k, row, rows_of(half)]
        return remote(dst if src is None else src, dst, self.isend.at[sem], self.irecv.at[sem], {"row": device})

    def pair(self, i, core, row, half, src=None):
        dst = self.buf.at[core, row, rows_of(half)]
        return remote(dst if src is None else src, dst, self.dsend.at[i], self.drecv.at[i], {"col": 1 - self.k})

    def local(self):
        return pltpu.make_async_copy(self.own, self.buf.at[self.k, self.r], self.lsem)

    def start(self):
        own = self.buf.at[self.k, self.r] if self.own is None else self.own
        first, second = own.at[pl.ds(0, PIECE)], own.at[pl.ds(PIECE, PIECE)]
        self.ici(0, self.r, 0, self.rx, first).start()
        self.ici(1, self.r, 1, self.ry, second).start()
        self.ici(2, self.r, 1, self.rx, second).start()
        self.ici(3, self.r, 0, self.ry, first).start()
        self.pair(0, self.k, self.r, 0, first).start()
        self.pair(1, self.k, self.r, 1, second).start()
        if self.own is not None:
            self.local().start()

    def arrive(self, i):
        row, half = self.piece(i)
        self.ici(i - 2, row, half, self.rx).wait_recv()

        @pl.when(i == 2)
        def _():
            self.ici(4, row, half, self.ry).start()

        @pl.when(i == 3)
        def _():
            self.ici(5, row, half, self.rx).start()

        self.pair(i, self.k, row, half).start()

    def ready(self, i):
        row, half = self.piece(i)
        self.pair(i, 1 - self.k, row, half).wait_recv()

    def run(self, compute, before=None, after=None):
        if self.own is not None:
            self.local().wait()

        def pair(q, carry):
            for u in range(2):
                i = 2 * q + u
                self.ready(i)
                row, half = self.piece(i)
                compute(i, row, half)
            if before is not None:
                before(q)

            @pl.when(q < 3)
            def _():
                self.arrive(2 * q + 2)
                self.arrive(2 * q + 3)

            if after is not None:
                after(q)
            return carry

        lax.fori_loop(0, 4, pair, 0)
        self.finish()

    def finish(self):
        for i in range(6):
            self.ici(i, self.r, 0, self.rx).wait_send()
        for i in range(8):
            self.pair(i, self.k, self.r, 0).wait_send()


def sum_scratch(width):
    return [
        pltpu.VMEM((4, PIECE, width), F32),
        pltpu.VMEM((4, PIECE, width), BF),
        pltpu.VMEM((8, PIECE, width), BF),
        pltpu.VMEM((6, PIECE, width), BF),
        pltpu.VMEM((6, PIECE, width), BF),
        DMA((8,)),
        DMA((8,)),
        DMA((6,)),
        DMA((6,)),
    ]


class Sum:
    def __init__(self, scratch):
        self.own, self.ds, self.dr, self.ist, self.irt = scratch[:5]
        self.dsend, self.drecv, self.isend, self.irecv = scratch[5:]
        self.r, self.k, self.rx, self.ry, self.r3 = place()

    def piece(self, j):
        mid = jnp.where(j == 2, self.ry, jnp.where(j == 5, self.ry, self.rx))
        row = jnp.where(j < 2, self.r3, jnp.where(j < 6, mid, self.r))
        return row, j % 2

    def pair(self, j):
        return remote(self.ds.at[j % 4], self.dr.at[j], self.dsend.at[j], self.drecv.at[j], {"col": 1 - self.k})

    def ici(self, j):
        device = jnp.where(j == 0, self.ry, jnp.where(j == 2, self.ry, jnp.where(j == 5, self.ry, self.rx)))
        return remote(self.ist.at[j], self.irt.at[j], self.isend.at[j], self.irecv.at[j], {"row": device})

    def put(self, j, kept, given):
        @pl.when(j >= 4)
        def _():
            self.pair(j - 4).wait_send()

        self.own[j % 4] = kept
        self.ds[j % 4] = given.astype(BF)
        self.pair(j).start()

    def chip(self, j):
        self.pair(j).wait_recv()
        return self.own[j % 4] + self.dr[j].astype(F32)

    def forward(self, j):
        self.ist[j] = self.chip(j).astype(BF)
        self.ici(j).start()

    def relay(self, j):
        value = self.chip(j)
        self.ici(j - 4).wait_recv()
        self.ist[j] = (value + self.irt[j - 4].astype(F32)).astype(BF)
        self.ici(j).start()

    def last(self, j):
        value = self.chip(j)
        self.ici(j - 4).wait_recv()
        value = value + self.irt[j - 4].astype(F32)
        self.ici(j - 2).wait_recv()
        return value + self.irt[j - 2].astype(F32)

    def send_all(self, compute, hook=None):
        def step(j, carry):
            row, half = self.piece(j)
            kept, given = compute(row, half)
            self.put(j, kept, given)

            @pl.when(j > 0)
            def _():
                @pl.when(j < 5)
                def _():
                    self.forward(j - 1)

            if hook is not None:
                hook(j)
            return carry

        lax.fori_loop(0, 8, step, 0)

    def finish(self):
        for j in range(4, 8):
            self.pair(j).wait_send()
        for j in range(6):
            self.ici(j).wait_send()


TALL, WIDE = 128, 768
CHUNK = TALL // 2
DOWN_CHUNKS, MLP_CHUNKS, OUT_CHUNKS, ALL_CHUNKS = 16, 48, 54, 66


def lags(n):
    return (4, 2) if n <= 4 else (2, 1)


def line_ring(n, lag):
    return lag * (2 * (n // 2) - 2) + lag + 4


def line_ticks(n, count, lag):
    return count + lag * (2 * (n // 2) - 2)


def line_outs(ticks, lag):
    return [sds((ticks, CHUNK, WIDE), BF)] + [sds((lag, CHUNK, WIDE), BF)] * 2


def line_scratch(n, ticks, lag):
    near, far = 2 * lag + 2, line_ring(n, lag)
    slots = (near, far, far, near)
    return [pltpu.VMEM((count, CHUNK, WIDE), BF) for count in slots] + [DMA((ticks,))] * 6


class Line:
    def __init__(self, parts, totals, carry, scratch, first, ticks, count, lag, before=None):
        self.parts, self.totals, self.carry = parts, totals, carry
        self.acc, self.tot, self.rin, self.rxb = scratch[:4]
        self.si, self.ri, self.rx, self.so, self.ro, self.out_sem = scratch[4:]
        self.first, self.ticks, self.count, self.lag, self.near = first, ticks, count, lag, 2 * lag + 2
        self.n, self.s, self.inward, self.outward = line_place()
        self.mid = self.n // 2
        self.ring = line_ring(self.n, lag)
        if before is not None:

            @pl.when(self.s > 0)
            def _():
                for b in range(self.lag):
                    self.acc[b] = before[0][b]
                    self.tot[b] = before[1][b]

    def valid(self, c):
        return (c >= 0) & (c < self.count)

    def sends(self, j):
        s, mid, slot, near = self.s, self.mid, j % self.ring, j % self.near
        to = {"dp": self.inward}
        c = self.first + j - self.lag * s
        moves = []
        inward = (self.rin.at[slot], self.ri.at[j])
        across = (self.rxb.at[near], self.rx.at[j])
        for lo, hi, ref in self.parts:
            ok = (s == 0) & (c >= lo) & (c < hi)
            moves.append((ok, ref, c - lo, across if mid == 1 else inward))
        if mid > 1:
            ok = self.valid(c)
            moves.append((ok & (s == mid - 1), self.acc, near, across))
            if mid > 2:
                moves.append((ok & (s > 0) & (s < mid - 1), self.acc, near, inward))
        out = [
            (cond, lambda ref=ref, at=at, way=way: remote(ref.at[at], way[0], self.si.at[j], way[1], to))
            for cond, ref, at, way in moves
        ]
        if mid > 1:
            c = self.first + j - self.lag * (2 * mid - 1 - s)
            out.append(((s > 0) & self.valid(c), lambda: self.outer(j)))
        return out

    def outer(self, j):
        return remote(
            self.tot.at[j % self.ring], self.tot.at[(j + self.lag) % self.ring],
            self.so.at[j], self.ro.at[j], {"dp": self.outward},
        )

    def begin(self, j):
        for cond, copy in self.sends(j):

            @pl.when(cond)
            def _(copy=copy):
                copy().start()

    def total_of(self, j):
        copy = lambda: pltpu.make_async_copy(
            self.tot.at[(j + self.lag) % self.ring], self.totals.at[j], self.out_sem.at[j]
        )
        return self.valid(self.first + j - self.lag * (2 * self.mid - 2 - self.s)), copy

    def settle(self, j):
        for cond, copy in self.sends(j):

            @pl.when(cond)
            def _(copy=copy):
                copy().wait_send()

        cond, copy = self.total_of(j)

        @pl.when(cond)
        def _():
            copy().wait()

    def end(self, j):
        t, s, mid = self.first + j, self.s, self.mid
        slot, later = j % self.ring, (j + self.lag) % self.ring
        near, next_near = j % self.near, (j + self.lag) % self.near

        @pl.when(j >= 2)
        def _():
            self.settle(j - 2)

        def came(buf, at, sem):
            remote(buf.at[at], buf.at[at], self.si.at[j], sem.at[j], {"dp": self.inward}).wait_recv()

        def add_part(c, buf, at, dst, to):
            for lo, hi, ref in self.parts:

                @pl.when((c >= lo) & (c < hi))
                def _(ref=ref, lo=lo):
                    dst[to] = (ref[c - lo].astype(F32) + buf[at].astype(F32)).astype(BF)

        if mid > 1:
            c = t - self.lag * (s - 1)

            @pl.when((s > 0) & self.valid(c))
            def _():
                came(self.rin, slot, self.ri)
                add_part(c, self.rin, slot, self.acc, next_near)

        @pl.when((s == mid - 1) & self.valid(t - self.lag * (mid - 1)))
        def _():
            came(self.rxb, near, self.rx)
            if mid > 1:
                self.tot[later] = (self.acc[near].astype(F32) + self.rxb[near].astype(F32)).astype(BF)
            else:
                add_part(t, self.rxb, near, self.tot, later)

        cond, copy = self.total_of(j)
        if mid > 1:

            @pl.when((s < mid - 1) & cond)
            def _():
                self.outer(j).wait_recv()

        @pl.when(cond)
        def _():
            copy().start()

    def open(self):
        def one(j, carry):
            self.begin(j)
            return carry

        lax.fori_loop(0, min(self.lag, self.ticks), one, 0)

    def step(self, j):
        self.end(j)

        @pl.when(j + self.lag < self.ticks)
        def _():
            self.begin(j + self.lag)

    def steps(self, start, stop):
        def one(t, carry):
            self.step(t)
            return carry

        lax.fori_loop(start, stop, one, 0)

    def rest(self, j):
        self.steps(j, self.ticks)

        def settle(t, carry):
            self.settle(t)
            return carry

        lax.fori_loop(max(self.ticks - 2, 0), self.ticks, settle, 0)
        if self.carry is not None:
            for b in range(self.lag):
                self.carry[0][b] = self.acc[(self.ticks + b) % self.near]
                self.carry[1][b] = self.tot[(self.ticks + b) % self.ring]


class Io:
    def __init__(self):
        self.coming, self.later, self.going = [], [], []

    def more(self):
        for entry in self.later:
            entry[1].start()
        self.coming += self.later
        self.later = []

    def need(self, *bufs):
        for buf in bufs:
            for at, (ref, copy) in enumerate(self.coming):
                if ref is buf:
                    copy.wait()
                    del self.coming[at]
                    break

    def spill(self, *bufs):
        for buf in bufs:
            for entry in self.going:
                if entry[0] is buf and not entry[2]:
                    entry[1].start()
                    entry[2] = True

    def finish(self):
        self.more()
        self.need(*[ref for ref, _ in self.coming])
        self.spill(*[entry[0] for entry in self.going])
        for _, copy, _ in self.going:
            copy.wait()


def staged(kernel, n_in, fetch, spill, early):
    def wrapped(*refs):
        refs, sems = list(refs[:-1]), refs[-1]
        count = len(fetch) + len(spill)
        refs, bufs = refs[:-count], refs[-count:]
        io = Io()
        for n, i in enumerate(fetch):
            copy = pltpu.make_async_copy(refs[i], bufs[n], sems.at[n])
            if n < early:
                copy.start()
            (io.coming if n < early else io.later).append((bufs[n], copy))
            refs[i] = bufs[n]
        for n, o in enumerate(spill, len(fetch)):
            io.going.append([bufs[n], pltpu.make_async_copy(bufs[n], refs[n_in + o], sems.at[n]), False])
            refs[n_in + o] = bufs[n]
        kernel(io, *refs)
        io.finish()

    return wrapped


def call(kernel, cid, outs, ins, args, scratch, flops, vmem, out_specs, fetch, spill, early=0):
    moved = sum(int(np.prod(a.shape)) * a.dtype.itemsize for a in list(args) + list(outs))
    ins, out_specs = list(ins), list(out_specs)
    held = [pltpu.VMEM(args[i].shape, args[i].dtype) for i in fetch]
    held += [pltpu.VMEM(outs[o].shape, outs[o].dtype) for o in spill]
    for i in fetch:
        ins[i] = ANY
    for o in spill:
        out_specs[o] = ANY
    return pl.pallas_call(
        staged(kernel, len(args), fetch, spill, early),
        out_shape=outs,
        in_specs=ins,
        out_specs=out_specs,
        scratch_shapes=list(scratch) + held + [DMA((len(held),))],
        compiler_params=pltpu.CompilerParams(
            collective_id=cid, has_side_effects=True, vmem_limit_bytes=vmem << 20
        ),
        cost_estimate=pl.CostEstimate(flops=int(flops), bytes_accessed=moved, transcendentals=0),
    )(*args)


def sds(shape, dtype):
    return jax.ShapeDtypeStruct(shape, dtype)


def head_index(iota):
    head, lane = iota // LANE, iota % LANE
    index = jnp.where(lane < HALF, lane, lane - (LANE // 2 - HALF))
    pad = lane % (LANE // 2) >= HALF
    return jnp.where(pad, -1, head * HD + index)


def spread(rows, cols, first):
    source = head_index(lax.broadcasted_iota(jnp.int32, (rows, cols), 1))
    at = lax.broadcasted_iota(jnp.int32, (rows, cols), 0)
    return jnp.where((source >= 0) & (at == source + first), 1.0, 0.0).astype(BF)


def spread_t(rows, cols, first):
    source = head_index(lax.broadcasted_iota(jnp.int32, (rows, cols), 0))
    at = lax.broadcasted_iota(jnp.int32, (rows, cols), 1)
    return jnp.where((source >= 0) & (at == source + first), 1.0, 0.0).astype(BF)


def angle_tables():
    lane = np.arange(LANE)
    freq = np.where(
        lane % (LANE // 2) < HALF, THETA ** (-2.0 * (lane % (LANE // 2)) / HD), 0.0
    )
    fine = np.arange(32)[:, None] * freq[None]
    coarse = fine * 32.0
    return [f(t).astype(np.float32) for t in (coarse, fine) for f in (np.cos, np.sin)]


def exchange(k, stat, sems):
    copy = remote(stat.at[k], stat.at[k], sems.at[0], sems.at[1], {"col": 1 - k})
    copy.start()
    remote(stat.at[1 - k], stat.at[1 - k], sems.at[0], sems.at[1], {"col": 1 - k}).wait_recv()
    copy.wait_send()
    return stat[0][:, 0:1] + stat[1][:, 0:1]


def causal(shape):
    return lax.broadcasted_iota(jnp.int32, shape, 0) <= lax.broadcasted_iota(jnp.int32, shape, 1)


def front_kernel(
    io,
    x, dy, gain, gain_f, wq_h, wk_h, wv_h, wo_h, wg, wu, wd, tables,
    normed_o, f_o, qkv, kvt, wqkv_o, wo_o, wg_o, wu_o, wd_o, cos_o, sin_o, rstd1_o,
    attn, lse, hidden, rstd2_o, part, mid_o, gate_o, up_o,
    buf, dys, stage, gains, give_in, give_out, wq, wk, wv, wo, wsem, wrecv, csem, nsem, fsem,
    stat, ssem, grad, give, gsend, grecv, middle, d_gate, d_up, msem, *rest,
):
    r, k, rx, ry, r3 = place()
    width = x.shape[1]
    f_half = wg.shape[1] // 2
    mate = {"col": 1 - k}
    mine = pl.ds(pl.multiple_of(k * f_half, f_half), f_half)
    his = pl.ds(pl.multiple_of((1 - k) * f_half, f_half), f_half)
    keep = [
        pltpu.make_async_copy(wg.at[:, mine], wg_o.at[k], csem.at[1]),
        pltpu.make_async_copy(wu.at[:, mine], wu_o.at[k], csem.at[2]),
        pltpu.make_async_copy(wd.at[mine], wd_o.at[k], csem.at[3]),
    ]
    first = [
        pltpu.make_async_copy(src, dst, csem.at[4 + n])
        for n, (src, dst) in enumerate(((wq_h, wq), (wk_h, wk), (wv_h, wv), (wo_h, wo)))
    ]
    for c in first + keep:
        c.start()
    greet(rx, ry, k)
    gather = Gather(x, buf, rest[:5])
    gather_dy = Gather(dy, dys, rest[5:10])
    gather_f = Gather(None, buf, rest[10:15])
    total = Sum(rest[15:])
    gains[k] = gain[...].reshape(1, width)
    gather.start()

    def give_to(n, src, dst):
        return remote(src, dst.at[k], wsem.at[n], wrecv.at[n], mate)

    gives = [give_to(0, gains.at[k], gains)]
    gives[0].start()
    heads_q = wq.shape[1] // 2
    heads_k = wk.shape[0] // 2
    nq = heads_q // HD * LANE
    nk = heads_k // HD * LANE
    for c in first:
        c.wait()
    for core, dst_in, dst_out in ((1 - k, give_in, give_out), (k, wqkv_o.at[k], wo_o.at[k])):
        sq = spread(2 * heads_q, nq, core * heads_q)
        sk = spread(2 * heads_k, nk, core * heads_k)
        dst_in[:, 0:nq] = nn(wq[...], sq).astype(BF)
        dst_in[:, nq : nq + nk] = tn(wk[...], sk).astype(BF)
        dst_in[:, nq + nk : nq + 2 * nk] = tn(wv[...], sk).astype(BF)
        dst_out[...] = nn(spread_t(nq, 2 * heads_q, core * heads_q), wo[...]).astype(BF)
    gives += [give_to(1, give_in, wqkv_o), give_to(2, give_out, wo_o)]
    gives += [give_to(3, wg.at[:, his], wg_o), give_to(4, wu.at[:, his], wu_o), give_to(5, wd.at[his], wd_o)]
    for g in gives[1:]:
        g.start()
    sign = jnp.where(lax.broadcasted_iota(jnp.int32, (32, LANE), 1) < LANE // 2, -1.0, 1.0)
    cf, sf = tables[2], tables[3]
    for a in range(LENGTH // 32):
        ca, sa = tables[0, a : a + 1, :], tables[1, a : a + 1, :]
        cos_o[a * 32 : a * 32 + 32, :] = ca * cf - sa * sf
        sin_o[a * 32 : a * 32 + 32, :] = (sa * cf + ca * sf) * sign
    for c in keep:
        c.wait()
    for n in range(3):
        gives[n].wait_recv()

    def keep_normed(i):
        row, half = gather.piece(i)
        return pltpu.make_async_copy(stage.at[i % 2], normed_o.at[:, row, rows_of(half)], nsem.at[i])

    def project(i, row, half):
        at = rows_of(half)
        x0 = buf[0, row, at, :].astype(F32)
        x1 = buf[1, row, at, :].astype(F32)
        square = jnp.sum(x0 * x0, 1, keepdims=True) + jnp.sum(x1 * x1, 1, keepdims=True)
        rstd = lax.rsqrt(square / (2 * width) + EPS)
        n0 = (x0 * rstd * gains[0]).astype(BF)
        n1 = (x1 * rstd * gains[1]).astype(BF)

        @pl.when(i >= 2)
        def _():
            keep_normed(i - 2).wait()

        stage[i % 2, 0] = n0
        stage[i % 2, 1] = n1

        @pl.when(i < 2)
        def _():
            rstd1_o[at, :] = jnp.broadcast_to(rstd, (PIECE, LANE))

        got = nn(n0, wqkv_o[0]) + nn(n1, wqkv_o[1])
        keep_normed(i).start()
        pos = pl.ds(pl.multiple_of((row % 2) * 2 * PIECE + half * PIECE, PIECE), PIECE)
        out = pl.ds(pl.multiple_of(row * 2 * PIECE + half * PIECE, PIECE), PIECE)
        cos, sin = cos_o[pos, :], sin_o[pos, :]
        for p in range(4):
            u = got[:, p * LANE : (p + 1) * LANE]
            if p < 3:
                u = u * cos + pltpu.roll(u, LANE // 2, 1) * sin
            qkv[p, out, :] = u.astype(BF)
            if p >= 2:
                kvt[p - 2, :, out] = u.T.astype(BF)

    def dy_too(q):
        @pl.when(q == 0)
        def _():
            gather_dy.start()

    gather.run(project, None, dy_too)
    for i in (6, 7):
        keep_normed(i).wait()

    def attend(row, half):
        base = pl.multiple_of(row // 2 * LENGTH, LENGTH)
        at = rows_of(half)
        qrow = pl.ds(pl.multiple_of(row * 2 * PIECE + half * PIECE, PIECE), PIECE)
        order = (row % 2) * 2 + half

        def queries(p):
            span = PIECE * (p + 1)
            for head in range(2):
                keys = qkv[2, pl.ds(base, span), :]
                s = nt(keys, qkv[head, qrow, :])
                tail = jnp.where(causal((PIECE, PIECE)), s[span - PIECE :], -1e30)
                s = tail if p == 0 else jnp.concatenate([s[: span - PIECE], tail], 0)
                top = jnp.max(s, 0, keepdims=True)
                e = jnp.exp((s - top) * SCALE)
                weight = jnp.sum(e, 0, keepdims=True)
                probs = (e * (1.0 / weight)).astype(BF)
                mixed = nn(kvt[1, :, pl.ds(base, span)], probs)
                attn[row, at, head * LANE : (head + 1) * LANE] = mixed.T.astype(BF)
                lse[head, row * 2 + half] = top * SCALE + jnp.log(weight)

        for p in range(4):
            pl.when(order == p)(lambda p=p: queries(p))
        a = attn[row, at, :]
        return nn(a, wo_o[k]), nn(a, wo_o[1 - k])

    def dy_arrive(j):
        @pl.when(j == 3)
        def _():
            gather_dy.arrive(2)
            gather_dy.arrive(3)

        @pl.when(j == 7)
        def _():
            gather_dy.arrive(4)
            gather_dy.arrive(5)

    total.send_all(attend, dy_arrive)
    io.spill(qkv, kvt, cos_o, sin_o, attn, wqkv_o, wo_o)
    for g in gives[3:]:
        g.wait_recv()
    io.spill(wg_o, wu_o, wd_o)
    gather_dy.local().wait()

    def mid_pair(q, carry):
        for u in range(2):
            i = 2 * q + u
            gather_dy.ready(i)
            row, half = gather_dy.piece(i)
            at = rows_of(half)
            d_mid = nt(dys[0, row, at, :], wd_o[0]) + nt(dys[1, row, at, :], wd_o[1])
            d_gate[row, at, :] = d_mid.astype(BF)
        return carry

    lax.fori_loop(0, 3, mid_pair, 0)
    gather_dy.arrive(6)
    gather_dy.arrive(7)
    total.relay(4)
    total.relay(5)
    mid_pair(3, 0)
    gather_dy.finish()
    for half in range(2):
        at = rows_of(half)
        h = buf[k, r, at, :].astype(F32) + total.last(6 + half)
        hidden[at, :] = h
        stat[k, at, :] = jnp.broadcast_to(jnp.sum(h * h, 1, keepdims=True), (PIECE, LANE))
    rstd2 = lax.rsqrt(exchange(k, stat, ssem) / (2 * width) + EPS)
    buf[k, r] = (hidden[...] * rstd2 * gain_f[...].reshape(1, width)).astype(BF)
    rstd2_o[...] = jnp.broadcast_to(rstd2, rstd2_o.shape)
    gather_f.start()
    io.spill(hidden)

    def keep_mids(i):
        row, half = gather_f.piece(i)
        at = rows_of(half)
        return [
            pltpu.make_async_copy(src.at[row, at], dst.at[row, at], msem.at[n, i])
            for n, (src, dst) in enumerate(((middle, mid_o), (d_gate, gate_o), (d_up, up_o)))
        ]

    def keep_f(i):
        row, half = gather_f.piece(i)
        at = rows_of(half)
        return pltpu.make_async_copy(buf.at[:, row, at], f_o.at[:, row, at], fsem.at[i])

    def expand(i, row, half):
        at = rows_of(half)
        keep_f(i).start()

        @pl.when(i > 0)
        def _():
            for c in keep_mids(i - 1):
                c.start()

        f0, f1 = buf[0, row, at, :], buf[1, row, at, :]
        dy0, dy1 = dys[0, row, at, :], dys[1, row, at, :]
        gate = nn(f0, wg_o[0]) + nn(f1, wg_o[1])
        upper = nn(f0, wu_o[0]) + nn(f1, wu_o[1])
        d_mid = d_gate[row, at, :].astype(F32)
        sig = 1.0 / (1.0 + jnp.exp(-gate))
        swish = gate * sig
        mid = (swish * upper).astype(BF)
        middle[row, at, :] = mid
        d_gate[row, at, :] = (d_mid * upper * sig * (1.0 + gate * (1.0 - sig))).astype(BF)
        d_up[row, at, :] = (d_mid * swish).astype(BF)
        g0, g1 = tn(mid, dy0), tn(mid, dy1)

        @pl.when(i == 0)
        def _():
            grad[0] = g0
            grad[1] = g1

        @pl.when(i > 0)
        def _():
            grad[0] += g0
            grad[1] += g1

    gather_f.run(expand)
    for c in keep_mids(7):
        c.start()
    half = DOWN_CHUNKS // 4

    def swap(j, core):
        return remote(
            give.at[pl.ds(2 * j, 2)], part.at[pl.ds(2 * (half * core + j), 2)], gsend.at[j], grecv.at[j], mate
        )

    for j in range(half):
        for h in range(2):
            give[2 * j + h] = grad[1 - k, j * TALL + h * CHUNK : j * TALL + (h + 1) * CHUNK, :].astype(BF)
        swap(j, k).start()
    for j in range(half):
        for h in range(2):
            rows = slice(j * TALL + h * CHUNK, j * TALL + (h + 1) * CHUNK)
            part[2 * (half * k + j) + h] = grad[k, rows, :].astype(BF)
    for j in range(half):
        swap(j, 1 - k).wait_recv()
    io.spill(part)

    def kept(i, carry):
        keep_f(i).wait()
        for c in keep_mids(i):
            c.wait()
        return carry

    lax.fori_loop(0, 8, kept, 0)
    for j in range(half):
        swap(j, k).wait_send()
    for g in gives:
        g.wait_send()
    total.finish()


def front(x, dy, gain, gain_f, wq, wk, wv, wo, wg, wu, wd):
    tokens, width = x.shape
    f_half = wg.shape[1] // 2
    cols = 4 * LANE
    gathered = (2, 4, tokens, width)
    outs = [sds(gathered, BF), sds(gathered, BF)]
    outs += [sds((4, 4 * tokens, LANE), BF), sds((2, LANE, 4 * tokens), BF)]
    outs += [sds((2, width, cols), BF), sds((2, 2 * LANE, width), BF)]
    outs += [sds((2, width, f_half), BF)] * 2 + [sds((2, f_half, width), BF)]
    outs += [sds((LENGTH, LANE), F32)] * 2 + [sds((tokens, LANE), F32)]
    outs += [sds((4, tokens, 2 * LANE), BF), sds((2, 8, 1, PIECE), F32)]
    outs += [sds((tokens, width), F32), sds((tokens, LANE), F32)]
    outs += [sds((DOWN_CHUNKS, CHUNK, WIDE), BF)] + [sds((4, tokens, f_half), BF)] * 3
    half = DOWN_CHUNKS // 4
    scratch = [pltpu.VMEM(gathered, BF)] * 2 + [pltpu.VMEM((2, 2, PIECE, width), BF)]
    scratch += [pltpu.VMEM((2, 1, width), F32), pltpu.VMEM((width, cols), BF), pltpu.VMEM((2 * LANE, width), BF)]
    scratch += [pltpu.VMEM(w.shape, BF) for w in (wq, wk, wv, wo)]
    scratch += [DMA((6,)), DMA((6,)), DMA((8,)), DMA((8,)), DMA((8,))]
    scratch += [pltpu.VMEM((2, tokens, LANE), F32), DMA((2,)), pltpu.VMEM((2, f_half, width), F32)]
    scratch += [pltpu.VMEM((2 * half, CHUNK, WIDE), BF), DMA((half,)), DMA((half,))]
    scratch += [pltpu.VMEM((4, tokens, f_half), BF)] * 3 + [DMA((3, 8))]
    scratch += GATHER_SEMS * 3 + sum_scratch(width)
    ins = [ANY] * 2 + [VM] * 2 + [ANY] * 7 + [VM]
    args = [x, dy, gain, gain_f, wq, wk, wv, wo, wg, wu, wd, jnp.asarray(np.stack(angle_tables()))]
    out_specs = [ANY] * 2 + [VM] * (len(outs) - 5) + [ANY] * 3
    spill = [2, 3, 4, 5, 6, 7, 8, 9, 10, 12, 14, 16]
    return call(front_kernel, 0, outs, ins, args, scratch, 9e10, 61, out_specs, [], spill)


TICKS = 34


def flat(ref, h, m=None):
    got = ref[h] if m is None else ref[h, :, :, pl.ds(pl.multiple_of(m * 256, 256), 256)]
    return got.reshape(-1, got.shape[-1])


def contract_kernel(
    io,
    d_gate, d_up, wg, wu, hidden, rstd2, gain, dy, wo, attn, part_d, f_any,
    d_hidden, gains_o, part, part_o, d_attn, totals, acc_c, tot_c,
    stat, ssem, give, gsend, grecv, gathered, dya, grad, give_o, his_o, gsem, fsem, *rest,
):
    r, k, rx, ry, r3 = place()
    width = hidden.shape[1]
    fetch = pltpu.make_async_copy(f_any, gathered, fsem)
    greet(rx, ry, k, True)
    total = Sum(rest[:9])
    gather = Gather(dya, gathered, rest[9:14])
    parts = [(0, DOWN_CHUNKS, part_d), (DOWN_CHUNKS, MLP_CHUNKS, part), (MLP_CHUNKS, OUT_CHUNKS, part_o)]
    lag = lags(lax.axis_size("dp"))[0]
    line = Line(parts, totals, (acc_c, tot_c), rest[14:], 0, TICKS, OUT_CHUNKS, lag)
    io.need(d_gate, d_up, wg, wu, part_d)
    line.open()
    fetch.start()
    io.more()

    def compute(row, half):
        at = rows_of(half)
        g, u = d_gate[row, at, :], d_up[row, at, :]
        return nt(g, wg[k]) + nt(u, wu[k]), nt(g, wg[1 - k]) + nt(u, wu[1 - k])

    def early(j):
        @pl.when(j % 2 == 1)
        def _():
            line.step(j // 2)

    total.send_all(compute, early)

    def swap(e, core):
        to = part.at[pl.ds(2 * (e // 4 * 8 + 4 * core + e % 4), 2)]
        return remote(give.at[pl.ds(2 * e, 2)], to, gsend.at[e], grecv.at[e], {"col": 1 - k})

    def wide_part(h, right, dst, first):
        def one(m, carry):
            got = tn(flat(gathered, h, m), right[...].reshape(-1, right.shape[2])).astype(BF)
            for b in range(2):
                lanes = pl.ds(pl.multiple_of((2 * m + b) * TALL, TALL), TALL)
                for j in range(4):
                    for u in range(2):
                        rows = slice(b * TALL + u * CHUNK, b * TALL + (u + 1) * CHUNK)
                        dst[2 * (first + j) + u, :, lanes] = got[rows, j * TALL : (j + 1) * TALL]
            return carry

        lax.fori_loop(0, width // 256, one, 0)

    fetch.wait()
    wide_part(1 - k, d_gate, give, 0)
    for e in range(4):
        swap(e, k).start()
    wide_part(k, d_gate, part, 4 * k)
    line.steps(4, 6)
    wide_part(1 - k, d_up, give, 4)
    for e in range(4, 8):
        swap(e, k).start()
    wide_part(k, d_up, part, 8 + 4 * k)
    total.relay(4)
    total.relay(5)
    for e in range(8):
        swap(e, 1 - k).wait_recv()
    io.spill(part)
    io.need(hidden, dy, wo, attn)
    line.steps(6, 13)
    gains = jnp.zeros((1, width), F32)
    for half in range(2):
        at = rows_of(half)
        d_nf = total.last(6 + half)
        h = hidden[at, :]
        gains = gains + jnp.sum(d_nf * h * rstd2[at, 0:1], 0, keepdims=True)
        scaled = d_nf * gain[...].reshape(1, width)
        d_hidden[at, :] = scaled
        stat[k, at, :] = jnp.broadcast_to(jnp.sum(scaled * h, 1, keepdims=True), (PIECE, LANE))
    gains_o[...] = gains
    inner = exchange(k, stat, ssem) / (2 * width)
    rs = rstd2[:, 0:1]
    value = dy[...].astype(F32) + rs * d_hidden[...] - hidden[...] * (rs * rs * rs * inner)
    d_hidden[...] = value
    dya[...] = value.astype(BF)
    gather.start()
    io.spill(d_hidden)

    def piece(i, row, half):
        at = rows_of(half)
        d0, d1 = gathered[0, row, at, :], gathered[1, row, at, :]
        d_attn[row, at, :] = (nt(d0, wo[0]) + nt(d1, wo[1])).astype(BF)
        a = attn[row, at, :]
        g0, g1 = tn(a, d0), tn(a, d1)

        @pl.when(i == 0)
        def _():
            grad[0] = g0
            grad[1] = g1

        @pl.when(i > 0)
        def _():
            grad[0] += g0
            grad[1] += g1

    def before(q):
        line.steps(jnp.where(q == 0, 13, 15 + 4 * q), 19 + 4 * q)

    gather.run(piece, before)
    give_o[...] = grad[1 - k].astype(BF)
    give_out = remote(give_o, his_o, gsem.at[0], gsem.at[1], {"col": 1 - k})
    give_out.start()
    q_cols = part_o.shape[0] * CHUNK
    mine = nn(spread(q_cols, 2 * LANE, k * (q_cols // 2)), grad[k].astype(BF))
    give_out.wait_recv()
    out = mine + nn(spread(q_cols, 2 * LANE, (1 - k) * (q_cols // 2)), his_o[...])
    for c in range(q_cols // CHUNK):
        part_o[c] = out[c * CHUNK : (c + 1) * CHUNK].astype(BF)
    line.rest(31)
    for e in range(8):
        swap(e, k).wait_send()
    give_out.wait_send()
    total.finish()


def contract(d_gate, d_up, wg, wu, hidden, rstd2, gain, dy, wo, attn, part_d, all_f):
    tokens, width = hidden.shape
    n = lax.axis_size("dp")
    outs = [sds((tokens, width), F32), sds((1, width), F32)]
    outs += [sds((MLP_CHUNKS - DOWN_CHUNKS, CHUNK, WIDE), BF), sds((OUT_CHUNKS - MLP_CHUNKS, CHUNK, WIDE), BF)]
    outs += [sds((4, tokens, 2 * LANE), BF)] + line_outs(TICKS, lags(n)[0])
    out_specs = [VM] * 5 + [ANY] + [VM] * 2
    scratch = [pltpu.VMEM((2, tokens, LANE), F32), DMA((2,))]
    scratch += [pltpu.VMEM((16, CHUNK, WIDE), BF), DMA((8,)), DMA((8,))]
    scratch += [pltpu.VMEM((2, 4, tokens, width), BF), pltpu.VMEM((tokens, width), BF)]
    scratch += [pltpu.VMEM((2, 2 * LANE, width), F32)] + [pltpu.VMEM((2 * LANE, width), BF)] * 2
    scratch += [DMA((2,)), DMA]
    scratch += sum_scratch(width) + GATHER_SEMS + line_scratch(n, TICKS, lags(n)[0])
    args = [d_gate, d_up, wg, wu, hidden, rstd2, gain, dy, wo, attn, part_d, all_f]
    ins = [VM] * 11 + [ANY]
    fetch = [0, 1, 2, 3, 10, 4, 7, 8, 9]
    return call(
        contract_kernel, 1, outs, ins, args, scratch, 5e10, vmem_limit(n), out_specs, fetch, [0, 2, 3, 4], 5
    )


def vmem_limit(n):
    return 60 if n <= 4 else 63


def columns(rows, cols, core, q_cols, k_cols):
    i = lax.broadcasted_iota(jnp.int32, (rows, cols), 0)
    at = lax.broadcasted_iota(jnp.int32, (rows, cols), 1)
    part, lane = i // LANE, i % LANE
    index = jnp.where(lane < HALF, lane, lane - (LANE // 2 - HALF))
    q = core * (q_cols // 2) + part * HD
    kv = q_cols + (part - 2) * k_cols + core * (k_cols // 2)
    to = jnp.where(part < 2, q, kv) + index
    pad = lane % (LANE // 2) >= HALF
    return jnp.where((at == to) & (pad == False), 1.0, 0.0).astype(BF)


def backward_kernel(
    q_cols, k_cols,
    io,
    qkv, kvt, lse, d_attn, cos, sin, middle, wd, hidden, wqkv, x, rstd1, d_hidden, gain, gains_f,
    part_m, part_o, acc_c, tot_c, normed_any,
    output, grad_x, gains_o, totals, totals_in,
    dk, dv, d_proj, normed, part, mine, give, his, gsem, stat, ssem, free, fsem,
    mine_g, pair_g, slots, gsend, grecv, *rest,
):
    r, k, rx, ry, r3 = place()
    width = x.shape[1]
    n = lax.axis_size("dp")
    z = lax.axis_index("dp")
    fetch = pltpu.make_async_copy(normed_any, normed, fsem)
    greet(rx, ry, k, True, True)
    sums = rest[:5]
    down = Sum(sums + rest[5:9])
    into = Sum(sums + rest[9:13])
    lag, lag_in = lags(n)
    count = ALL_CHUNKS - OUT_CHUNKS
    ticks, ticks_in = line_ticks(n, OUT_CHUNKS, lag) - TICKS, line_ticks(n, count, lag_in)
    parts = [(DOWN_CHUNKS, MLP_CHUNKS, part_m), (MLP_CHUNKS, OUT_CHUNKS, part_o)]
    line = Line(parts, totals, None, rest[13:23], TICKS, ticks, OUT_CHUNKS, lag, (acc_c, tot_c))
    line_in = Line([(0, count, part)], totals_in, None, rest[23:], 0, ticks_in, count, lag_in)
    io.need(part_m, part_o, middle, wd)
    line.open()
    io.more()

    def down_piece(row, half):
        m = middle[row, rows_of(half), :]
        return nn(m, wd[k]), nn(m, wd[1 - k])

    def early(j):
        @pl.when(j % 3 == 1)
        def _():
            line.step(j // 3)

    down.send_all(down_piece, early)

    fetch.start()
    io.need(qkv, kvt, d_attn, cos, sin)

    def unrotate(u, p):
        at = pl.ds(p * PIECE, PIECE)
        return u * cos[at, :] - pltpu.roll(u, LANE // 2, 1) * sin[at, :]

    def sequence(seq):
        base = pl.multiple_of(seq * LENGTH, LENGTH)

        def one_head(head, carry):
            for p in range(4):
                span = PIECE * (p + 1)
                row = seq * 2 + p // 2
                at = pl.ds((p % 2) * PIECE, PIECE)
                out = pl.ds(pl.multiple_of(base + p * PIECE, PIECE), PIECE)
                keys = qkv[2, pl.ds(base, span), :]
                q = qkv[head, out, :]
                lane = pl.ds(pl.multiple_of(head * LANE, LANE), LANE)
                do = d_attn[row, at, lane]
                e = jnp.exp(nt(keys, q) * SCALE - lse[head, seq * 4 + p])
                tail = jnp.where(causal((PIECE, PIECE)), e[span - PIECE :], 0.0)
                e = tail if p == 0 else jnp.concatenate([e[: span - PIECE], tail], 0)
                dp = nt(qkv[3, pl.ds(base, span), :], do)
                inner = jnp.sum(e * dp, 0, keepdims=True)
                ds = (e * (dp - inner)).astype(BF)
                dv[0:span, :] += nn(e.astype(BF), do)
                dk[0:span, :] += nn(ds, q)
                dq = nn(kvt[0, :, pl.ds(base, span)], ds).T * SCALE
                d_proj[out, lane] = unrotate(dq, p).astype(BF)
                if p % 2 == 1:
                    tick = 3 + seq * 8 + head * 4 + p - 1
                    line.steps(tick, tick + 2)
            return carry

        dk[...] = jnp.zeros_like(dk)
        dv[...] = jnp.zeros_like(dv)
        lax.fori_loop(0, 2, one_head, 0)
        for p in range(4):
            at = pl.ds(p * PIECE, PIECE)
            out = pl.ds(pl.multiple_of(base + p * PIECE, PIECE), PIECE)
            d_proj[out, 2 * LANE : 3 * LANE] = unrotate(dk[at, :] * SCALE, p).astype(BF)
            d_proj[out, 3 * LANE : 4 * LANE] = dv[at, :].astype(BF)

    def both(seq, carry):
        sequence(seq)

        @pl.when(seq == 0)
        def _():
            down.relay(4)
            down.relay(5)

        return carry

    lax.fori_loop(0, 2, both, 0)
    io.need(hidden)
    for half in range(2):
        at = rows_of(half)
        output[at, :] = hidden[at, :] + down.last(6 + half)
    down.finish()
    io.spill(output)
    for device in ({"row": rx}, {"row": ry}, {"col": 1 - k}):
        pl.semaphore_signal(free, inc=1, device_id=device, device_id_type=MESH)
    pl.semaphore_wait(free, 3)

    fetch.wait()

    def in_part(h, dst):
        def one(m, carry):
            dst[pl.ds(pl.multiple_of(m * 256, 256), 256), :] = tn(flat(normed, h, m), d_proj[...]).astype(BF)
            return carry

        lax.fori_loop(0, width // 256, one, 0)

    in_part(1 - k, give)
    swap = remote(give, his, gsem.at[0], gsem.at[1], {"col": 1 - k})
    swap.start()
    line.steps(19, 21)
    in_part(k, mine)
    line.steps(21, 23)
    cols = q_cols + 2 * k_cols
    got = nn(mine[...], columns(4 * LANE, cols, k, q_cols, k_cols))
    swap.wait_recv()
    got = got + nn(his[...], columns(4 * LANE, cols, 1 - k, q_cols, k_cols))
    for c in range(width // CHUNK):
        part[c] = got[c * CHUNK : (c + 1) * CHUNK].astype(BF)

    def into_piece(row, half):
        d = d_proj[pl.ds(pl.multiple_of(row * 2 * PIECE + half * PIECE, PIECE), PIECE), :]
        return nt(d, wqkv[k]), nt(d, wqkv[1 - k])

    line_in.open()

    def both_lines(t, carry):
        line.step(23 + t)
        line_in.step(t)
        return carry

    def beside(j):
        @pl.when(j % 2 == 1)
        def _():
            both_lines(j // 2, 0)

    io.need(wqkv)
    into.send_all(into_piece, beside)
    lax.fori_loop(4, 5, both_lines, 0)
    line_in.steps(5, 7)
    into.relay(4)
    into.relay(5)
    line_in.steps(7, 12)
    io.need(x, d_hidden)
    gains = jnp.zeros((1, width), F32)
    for half in range(2):
        at = rows_of(half)
        d_na = into.last(6 + half)
        xs = x[at, :].astype(F32)
        gains = gains + jnp.sum(d_na * xs * rstd1[at, 0:1], 0, keepdims=True)
        scaled = d_na * gain[...].reshape(1, width)
        grad_x[at, :] = scaled
        stat[k, at, :] = jnp.broadcast_to(jnp.sum(scaled * xs, 1, keepdims=True), (PIECE, LANE))

    def row_total(step, device):
        copy = remote(mine_g.at[step], pair_g.at[step], gsend.at[n + step], grecv.at[n + step], {"row": device})
        copy.start()
        return copy

    line_in.step(12)
    mine_g[0, 0:1] = gains
    mine_g[0, 1:2] = gains_f[...]
    over_x = row_total(0, rx)
    inner = exchange(k, stat, ssem) / (2 * width)
    rs = rstd1[:, 0:1]
    line_in.step(13)
    over_x.wait_recv()
    mine_g[1] = mine_g[0] + pair_g[0]
    over_y = row_total(1, ry)
    grad_x[...] = d_hidden[...] + rs * grad_x[...] - x[...].astype(F32) * (rs * rs * rs * inner)
    over_y.wait_recv()
    slots[z] = mine_g[1] + pair_g[1]

    def over_dp(t, mine):
        other = (z + t) % n
        g = z if mine else other
        return remote(slots.at[g], slots.at[g], gsend.at[t], grecv.at[g], {"dp": other})

    def start(t, carry):
        over_dp(t, True).start()
        return carry

    lax.fori_loop(1, n, start, 0)
    io.spill(grad_x)
    line_in.rest(14)
    line.rest(28)

    def wait(t, carry):
        over_dp(t, False).wait_recv()
        over_dp(t, True).wait_send()
        return carry

    lax.fori_loop(1, n, wait, 0)
    gains_o[...] = lax.fori_loop(1, n, lambda g, total: total + slots[g], slots[0])
    over_x.wait_send()
    over_y.wait_send()
    swap.wait_send()
    into.finish()


def backward(
    qkv, kvt, lse, d_attn, cos, sin, middle, wd, hidden, wqkv, x, rstd1, d_hidden, gain, gains_f,
    part_m, part_o, acc, tot, normed, q_cols, k_cols,
):
    tokens, width = x.shape
    n = lax.axis_size("dp")
    lag, lag_in = lags(n)
    ticks = line_ticks(n, OUT_CHUNKS, lag) - TICKS
    ticks_in = line_ticks(n, ALL_CHUNKS - OUT_CHUNKS, lag_in)
    outs = [sds((tokens, width), F32)] * 2 + [sds((2, width), F32)]
    outs += [sds((t, CHUNK, WIDE), BF) for t in (ticks, ticks_in)]
    scratch = [pltpu.VMEM((LENGTH, LANE), F32)] * 2 + [pltpu.VMEM((4 * tokens, 4 * LANE), BF)]
    scratch += [pltpu.VMEM((2, 4, tokens, width), BF), pltpu.VMEM((ALL_CHUNKS - OUT_CHUNKS, CHUNK, WIDE), BF)]
    scratch += [pltpu.VMEM((width, 4 * LANE), BF)] * 3 + [DMA((2,))]
    scratch += [pltpu.VMEM((2, tokens, LANE), F32), DMA((2,)), pltpu.SemaphoreType.REGULAR, DMA]
    scratch += [pltpu.VMEM((2, 2, width), F32)] * 2 + [pltpu.VMEM((n, 2, width), F32)]
    scratch += [DMA((n + 2,)), DMA((n + 2,))]
    both = sum_scratch(width)
    scratch += both + both[5:] + line_scratch(n, ticks, lag) + line_scratch(n, ticks_in, lag_in)
    args = [qkv, kvt, lse, d_attn, cos, sin, middle, wd, hidden, wqkv, x, rstd1, d_hidden, gain, gains_f]
    args += [part_m, part_o, acc, tot, normed]
    kernel = functools.partial(backward_kernel, q_cols, k_cols)
    ins = [VM] * (len(args) - 1) + [ANY]
    fetch = [15, 16, 6, 7, 0, 1, 3, 4, 5, 8, 9, 10, 12]
    return call(
        kernel, 2, outs, ins, args, scratch, 5e10, vmem_limit(n), [VM] * 3 + [ANY] * 2, fetch, [0, 1], 4
    )


SLOTS = 4


def unpack_kernel(q_cols, k_cols, tot1, tot2, tot3, down, gate, up, out, q_o, k_o, v_o, whole, last, wide, turned, isem, osem):
    n, s, _, _ = line_place()
    steps = 2 * (n // 2) - 2 - s
    lag, lag_in = lags(n)
    first = tot1.shape[0]
    loads = [
        pltpu.make_async_copy(tot1, whole.at[pl.ds(0, first)], isem.at[0]),
        pltpu.make_async_copy(tot2, whole.at[pl.ds(first, tot2.shape[0])], isem.at[1]),
        pltpu.make_async_copy(tot3, last, isem.at[2]),
    ]
    for c in loads:
        c.start()
    loads[0].wait()
    late = whole.shape[0] - OUT_CHUNKS > first - DOWN_CHUNKS
    if late:
        loads[1].wait()

    def chunk(c, lanes):
        return whole[c + lag * steps, :, lanes].astype(F32)

    def run(count, make, copies):
        def one(b, carry):
            slot = b % SLOTS

            @pl.when(b >= SLOTS)
            def _():
                for c in copies(b - SLOTS, slot):
                    c.wait()

            make(b, slot)
            for c in copies(b, slot):
                c.start()
            return carry

        lax.fori_loop(0, count, one, 0)

        def drain(b, carry):
            for c in copies(b, b % SLOTS):
                c.wait()
            return carry

        lax.fori_loop(max(count - SLOTS, 0), count, drain, 0)

    def rows(b):
        return pl.ds(pl.multiple_of(b * TALL, TALL), TALL)

    def tall(start, to, count):
        def make(b, slot):
            for u in range(2):
                wide[slot, u * CHUNK : (u + 1) * CHUNK, 0:WIDE] = chunk(start + 2 * b + u, slice(0, WIDE))

        def copies(b, slot):
            return [pltpu.make_async_copy(wide.at[slot, :, pl.ds(0, WIDE)], to.at[rows(b)], osem.at[slot, 0])]

        run(count, make, copies)

    def broad(start, to):
        def make(b, slot):
            for c in range(8):
                for u in range(2):
                    got = chunk(start + 2 * c + u, rows(b))
                    wide[slot, u * CHUNK : (u + 1) * CHUNK, c * TALL : (c + 1) * TALL] = got

        def copies(b, slot):
            return [pltpu.make_async_copy(wide.at[slot], to.at[rows(b)], osem.at[slot, 0])]

        run(WIDE // TALL, make, copies)

    tall(0, down, 8)
    if not late:
        loads[1].wait()
    broad(DOWN_CHUNKS, gate)
    broad(DOWN_CHUNKS + 16, up)
    tall(MLP_CHUNKS, out, q_cols // TALL)
    loads[2].wait()

    def make_in(b, slot):
        for u in range(2):
            got = last[2 * b + u + lag_in * steps].astype(F32)
            wide[slot, u * CHUNK : (u + 1) * CHUNK, 0:WIDE] = got
        turned[slot, 0] = wide[slot, :, q_cols : q_cols + k_cols].T
        turned[slot, 1] = wide[slot, :, q_cols + k_cols : WIDE].T

    def copies_in(b, slot):
        return [
            pltpu.make_async_copy(wide.at[slot, :, pl.ds(0, q_cols)], q_o.at[rows(b)], osem.at[slot, 0]),
            pltpu.make_async_copy(turned.at[slot, 0], k_o.at[:, rows(b)], osem.at[slot, 1]),
            pltpu.make_async_copy(turned.at[slot, 1], v_o.at[:, rows(b)], osem.at[slot, 2]),
        ]

    run(WIDE // TALL, make_in, copies_in)


def unpack(tots, q_cols, k_cols):
    outs = [sds((8 * TALL, WIDE), F32), sds((WIDE, 8 * TALL), F32), sds((WIDE, 8 * TALL), F32)]
    outs += [sds((q_cols, WIDE), F32), sds((WIDE, q_cols), F32), sds((k_cols, WIDE), F32), sds((k_cols, WIDE), F32)]
    return pl.pallas_call(
        functools.partial(unpack_kernel, q_cols, k_cols),
        out_shape=outs,
        in_specs=[ANY] * 3,
        out_specs=[ANY] * len(outs),
        scratch_shapes=[
            pltpu.VMEM((tots[0].shape[0] + tots[1].shape[0], CHUNK, WIDE), BF),
            pltpu.VMEM(tots[2].shape, BF),
            pltpu.VMEM((SLOTS, TALL, 8 * TALL), F32),
            pltpu.VMEM((SLOTS, 2, k_cols, TALL), F32),
            DMA((3,)),
            DMA((SLOTS, 3)),
        ],
        compiler_params=pltpu.CompilerParams(vmem_limit_bytes=62 << 20),
        cost_estimate=pl.CostEstimate(flops=0, bytes_accessed=3 * ALL_CHUNKS * TALL * WIDE, transcendentals=0),
    )(*tots)


def on_device(
    layer_input, gain_attn, gain_ffn, w_query, w_key, w_value, w_out, w_gate, w_up, w_down, cotangent
):
    tokens, width = layer_input.shape
    q_cols, k_cols = w_query.shape[1], w_key.shape[1]
    gain_a, gain_f = gain_attn, gain_ffn
    (
        normed, all_f, qkv, kvt, wqkv, wo, wg, wu, wd, cos, sin, rstd1,
        attn, lse, hidden, rstd2, part_d, middle, d_gate, d_up,
    ) = front(
        layer_input, cotangent, gain_a, gain_f,
        w_query, w_key.T, w_value.T, w_out, w_gate, w_up, w_down,
    )
    d_hidden, gains_f, part_m, part_o, d_attn, tot1, acc, tot = contract(
        d_gate, d_up, wg, wu, hidden, rstd2, gain_f, cotangent, wo, attn, part_d, all_f
    )
    output, grad_x, gains, tot2, tot3 = backward(
        qkv, kvt, lse, d_attn, cos, sin, middle, wd, hidden, wqkv, layer_input, rstd1, d_hidden,
        gain_a, gains_f, part_m, part_o, acc, tot, normed, q_cols, k_cols,
    )
    down, gate, up, out, g_q, g_k, g_v = unpack([tot1, tot2, tot3], q_cols, k_cols)
    return output, grad_x, gains[0], gains[1], g_q, g_k.T, g_v.T, out, gate, up, down


def solution(mesh):
    assert mesh.shape["row"] == 4 and mesh.shape["col"] == 2
    tokens = P(("dp", "row"), "col")
    wide = P("col", "row")
    tall = P("row", "col")
    return jax.shard_map(
        on_device,
        mesh=mesh,
        in_specs=(tokens, P("col"), P("col"), wide, wide, wide, tall, wide, wide, tall, tokens),
        out_specs=(tokens, tokens, P("col"), P("col"), wide, wide, wide, tall, wide, wide, tall),
        check_vma=False,
    )
```

```python
import functools

import jax
import jax.numpy as jnp
import numpy as np
from jax import lax
from jax.experimental import pallas as pl
from jax.experimental.pallas import tpu as pltpu
from jax.sharding import PartitionSpec as P

HD = 96
HALF = HD // 2
LENGTH = 1024
EPS = 1e-05
THETA = 100000.0
SCALE = HD ** (-0.5)
LANE = 128
PIECE = 256

BF = jnp.bfloat16
F32 = jnp.float32
MESH = pl.DeviceIdType.MESH
VM = pl.BlockSpec(memory_space=pltpu.VMEM)
ANY = pl.BlockSpec(memory_space=pl.ANY)
DMA = pltpu.SemaphoreType.DMA


def nn(a, b):
    return lax.dot_general(a, b, (((1,), (0,)), ((), ())), preferred_element_type=F32)


def nt(a, b):
    return lax.dot_general(a, b, (((1,), (1,)), ((), ())), preferred_element_type=F32)


def place():
    r = lax.axis_index("row")
    k = lax.axis_index("col")
    return r, k, r + 1 - 2 * (r % 2), (r + 2) % 4, 3 - r


def tn(a, b):
    return lax.dot_general(a, b, (((0,), (0,)), ((), ())), preferred_element_type=F32)


def line_place():
    n = lax.axis_size("dp")
    z = lax.axis_index("dp")
    left = z < n // 2
    step = jnp.where(left, 1, -1)
    return n, jnp.where(left, z, n - 1 - z), z + step, z - step


def greet(rx, ry, k, line=False, groups=False):
    bar = pltpu.get_barrier_semaphore()

    def hello(device):
        pl.semaphore_signal(bar, inc=1, device_id=device, device_id_type=MESH)

    for device in ({"row": rx}, {"row": ry}, {"col": 1 - k}):
        hello(device)
    if not line:
        pl.semaphore_wait(bar, 3)
        return
    n, s, inward, outward = line_place()
    if groups:
        z = lax.axis_index("dp")

        def one(t, carry):
            hello({"dp": (z + t) % n})
            return carry

        lax.fori_loop(1, n, one, 0)
        pl.semaphore_wait(bar, 3 + n - 1)
        return
    hello({"dp": inward})

    @pl.when(s > 0)
    def _():
        hello({"dp": outward})

    pl.semaphore_wait(bar, jnp.where(s > 0, 5, 4))


def remote(src, dst, send, recv, device):
    return pltpu.make_async_remote_copy(
        src_ref=src, dst_ref=dst, send_sem=send, recv_sem=recv, device_id=device, device_id_type=MESH
    )


def rows_of(half):
    return pl.ds(pl.multiple_of(half * PIECE, PIECE), PIECE)


GATHER_SEMS = [DMA((6,)), DMA((6,)), DMA((8,)), DMA((8,)), DMA]


class Gather:
    def __init__(self, own, buf, sems):
        self.own, self.buf = own, buf
        self.isend, self.irecv, self.dsend, self.drecv, self.lsem = sems
        self.r, self.k, self.rx, self.ry, self.r3 = place()

    def piece(self, i):
        side = jnp.where(i % 2 == 0, self.rx, self.ry)
        row = jnp.where(i < 2, self.r, jnp.where(i < 6, side, self.r3))
        half = jnp.where(i // 2 == 2, 1 - i % 2, i % 2)
        return row, half

    def ici(self, sem, row, half, device, src=None):
        dst = self.buf.at[self.k, row, rows_of(half)]
        return remote(dst if src is None else src, dst, self.isend.at[sem], self.irecv.at[sem], {"row": device})

    def pair(self, i, core, row, half, src=None):
        dst = self.buf.at[core, row, rows_of(half)]
        return remote(dst if src is None else src, dst, self.dsend.at[i], self.drecv.at[i], {"col": 1 - self.k})

    def local(self):
        return pltpu.make_async_copy(self.own, self.buf.at[self.k, self.r], self.lsem)

    def start(self):
        own = self.buf.at[self.k, self.r] if self.own is None else self.own
        first, second = own.at[pl.ds(0, PIECE)], own.at[pl.ds(PIECE, PIECE)]
        self.ici(0, self.r, 0, self.rx, first).start()
        self.ici(1, self.r, 1, self.ry, second).start()
        self.ici(2, self.r, 1, self.rx, second).start()
        self.ici(3, self.r, 0, self.ry, first).start()
        self.pair(0, self.k, self.r, 0, first).start()
        self.pair(1, self.k, self.r, 1, second).start()
        if self.own is not None:
            self.local().start()

    def arrive(self, i):
        row, half = self.piece(i)
        self.ici(i - 2, row, half, self.rx).wait_recv()

        @pl.when(i == 2)
        def _():
            self.ici(4, row, half, self.ry).start()

        @pl.when(i == 3)
        def _():
            self.ici(5, row, half, self.rx).start()

        self.pair(i, self.k, row, half).start()

    def ready(self, i):
        row, half = self.piece(i)
        self.pair(i, 1 - self.k, row, half).wait_recv()

    def run(self, compute, before=None, after=None):
        if self.own is not None:
            self.local().wait()

        def pair(q, carry):
            for u in range(2):
                i = 2 * q + u
                self.ready(i)
                row, half = self.piece(i)
                compute(i, row, half)
            if before is not None:
                before(q)

            @pl.when(q < 3)
            def _():
                self.arrive(2 * q + 2)
                self.arrive(2 * q + 3)

            if after is not None:
                after(q)
            return carry

        lax.fori_loop(0, 4, pair, 0)
        self.finish()

    def finish(self):
        for i in range(6):
            self.ici(i, self.r, 0, self.rx).wait_send()
        for i in range(8):
            self.pair(i, self.k, self.r, 0).wait_send()


def sum_scratch(width):
    return [
        pltpu.VMEM((4, PIECE, width), F32),
        pltpu.VMEM((4, PIECE, width), BF),
        pltpu.VMEM((8, PIECE, width), BF),
        pltpu.VMEM((6, PIECE, width), BF),
        pltpu.VMEM((6, PIECE, width), BF),
        DMA((8,)),
        DMA((8,)),
        DMA((6,)),
        DMA((6,)),
    ]


class Sum:
    def __init__(self, scratch):
        self.own, self.ds, self.dr, self.ist, self.irt = scratch[:5]
        self.dsend, self.drecv, self.isend, self.irecv = scratch[5:]
        self.r, self.k, self.rx, self.ry, self.r3 = place()

    def piece(self, j):
        mid = jnp.where(j == 2, self.ry, jnp.where(j == 5, self.ry, self.rx))
        row = jnp.where(j < 2, self.r3, jnp.where(j < 6, mid, self.r))
        return row, j % 2

    def pair(self, j):
        return remote(self.ds.at[j % 4], self.dr.at[j], self.dsend.at[j], self.drecv.at[j], {"col": 1 - self.k})

    def ici(self, j):
        device = jnp.where(j == 0, self.ry, jnp.where(j == 2, self.ry, jnp.where(j == 5, self.ry, self.rx)))
        return remote(self.ist.at[j], self.irt.at[j], self.isend.at[j], self.irecv.at[j], {"row": device})

    def put(self, j, kept, given):
        @pl.when(j >= 4)
        def _():
            self.pair(j - 4).wait_send()

        self.own[j % 4] = kept
        self.ds[j % 4] = given.astype(BF)
        self.pair(j).start()

    def chip(self, j):
        self.pair(j).wait_recv()
        return self.own[j % 4] + self.dr[j].astype(F32)

    def forward(self, j):
        self.ist[j] = self.chip(j).astype(BF)
        self.ici(j).start()

    def relay(self, j):
        value = self.chip(j)
        self.ici(j - 4).wait_recv()
        self.ist[j] = (value + self.irt[j - 4].astype(F32)).astype(BF)
        self.ici(j).start()

    def last(self, j):
        value = self.chip(j)
        self.ici(j - 4).wait_recv()
        value = value + self.irt[j - 4].astype(F32)
        self.ici(j - 2).wait_recv()
        return value + self.irt[j - 2].astype(F32)

    def send_all(self, compute, hook=None):
        def step(j, carry):
            row, half = self.piece(j)
            kept, given = compute(row, half)
            self.put(j, kept, given)

            @pl.when(j > 0)
            def _():
                @pl.when(j < 5)
                def _():
                    self.forward(j - 1)

            if hook is not None:
                hook(j)
            return carry

        lax.fori_loop(0, 8, step, 0)

    def finish(self):
        for j in range(4, 8):
            self.pair(j).wait_send()
        for j in range(6):
            self.ici(j).wait_send()


TALL, WIDE = 128, 768
CHUNK = TALL // 2
DOWN_CHUNKS, MLP_CHUNKS, OUT_CHUNKS, ALL_CHUNKS = 16, 48, 54, 66


def lags(n):
    return (4, 2) if n <= 4 else (2, 1)


def line_ring(n, lag):
    return lag * (2 * (n // 2) - 2) + lag + 4


def line_ticks(n, count, lag):
    return count + lag * (2 * (n // 2) - 2)


def line_outs(ticks, lag):
    return [sds((ticks, CHUNK, WIDE), BF)] + [sds((lag, CHUNK, WIDE), BF)] * 2


def line_scratch(n, ticks, lag):
    near, far = 2 * lag + 2, line_ring(n, lag)
    slots = (near, far, far, near)
    return [pltpu.VMEM((count, CHUNK, WIDE), BF) for count in slots] + [DMA((ticks,))] * 6


class Line:
    def __init__(self, parts, totals, carry, scratch, first, ticks, count, lag, before=None):
        self.parts, self.totals, self.carry = parts, totals, carry
        self.acc, self.tot, self.rin, self.rxb = scratch[:4]
        self.si, self.ri, self.rx, self.so, self.ro, self.out_sem = scratch[4:]
        self.first, self.ticks, self.count, self.lag, self.near = first, ticks, count, lag, 2 * lag + 2
        self.n, self.s, self.inward, self.outward = line_place()
        self.mid = self.n // 2
        self.ring = line_ring(self.n, lag)
        if before is not None:

            @pl.when(self.s > 0)
            def _():
                for b in range(self.lag):
                    self.acc[b] = before[0][b]
                    self.tot[b] = before[1][b]

    def valid(self, c):
        return (c >= 0) & (c < self.count)

    def sends(self, j):
        s, mid, slot, near = self.s, self.mid, j % self.ring, j % self.near
        to = {"dp": self.inward}
        c = self.first + j - self.lag * s
        moves = []
        inward = (self.rin.at[slot], self.ri.at[j])
        across = (self.rxb.at[near], self.rx.at[j])
        for lo, hi, ref in self.parts:
            ok = (s == 0) & (c >= lo) & (c < hi)
            moves.append((ok, ref, c - lo, across if mid == 1 else inward))
        if mid > 1:
            ok = self.valid(c)
            moves.append((ok & (s == mid - 1), self.acc, near, across))
            if mid > 2:
                moves.append((ok & (s > 0) & (s < mid - 1), self.acc, near, inward))
        out = [
            (cond, lambda ref=ref, at=at, way=way: remote(ref.at[at], way[0], self.si.at[j], way[1], to))
            for cond, ref, at, way in moves
        ]
        if mid > 1:
            c = self.first + j - self.lag * (2 * mid - 1 - s)
            out.append(((s > 0) & self.valid(c), lambda: self.outer(j)))
        return out

    def outer(self, j):
        return remote(
            self.tot.at[j % self.ring], self.tot.at[(j + self.lag) % self.ring],
            self.so.at[j], self.ro.at[j], {"dp": self.outward},
        )

    def begin(self, j):
        for cond, copy in self.sends(j):

            @pl.when(cond)
            def _(copy=copy):
                copy().start()

    def total_of(self, j):
        copy = lambda: pltpu.make_async_copy(
            self.tot.at[(j + self.lag) % self.ring], self.totals.at[j], self.out_sem.at[j]
        )
        return self.valid(self.first + j - self.lag * (2 * self.mid - 2 - self.s)), copy

    def settle(self, j):
        for cond, copy in self.sends(j):

            @pl.when(cond)
            def _(copy=copy):
                copy().wait_send()

        cond, copy = self.total_of(j)

        @pl.when(cond)
        def _():
            copy().wait()

    def end(self, j):
        t, s, mid = self.first + j, self.s, self.mid
        slot, later = j % self.ring, (j + self.lag) % self.ring
        near, next_near = j % self.near, (j + self.lag) % self.near

        @pl.when(j >= 2)
        def _():
            self.settle(j - 2)

        def came(buf, at, sem):
            remote(buf.at[at], buf.at[at], self.si.at[j], sem.at[j], {"dp": self.inward}).wait_recv()

        def add_part(c, buf, at, dst, to):
            for lo, hi, ref in self.parts:

                @pl.when((c >= lo) & (c < hi))
                def _(ref=ref, lo=lo):
                    dst[to] = (ref[c - lo].astype(F32) + buf[at].astype(F32)).astype(BF)

        if mid > 1:
            c = t - self.lag * (s - 1)

            @pl.when((s > 0) & self.valid(c))
            def _():
                came(self.rin, slot, self.ri)
                add_part(c, self.rin, slot, self.acc, next_near)

        @pl.when((s == mid - 1) & self.valid(t - self.lag * (mid - 1)))
        def _():
            came(self.rxb, near, self.rx)
            if mid > 1:
                self.tot[later] = (self.acc[near].astype(F32) + self.rxb[near].astype(F32)).astype(BF)
            else:
                add_part(t, self.rxb, near, self.tot, later)

        cond, copy = self.total_of(j)
        if mid > 1:

            @pl.when((s < mid - 1) & cond)
            def _():
                self.outer(j).wait_recv()

        @pl.when(cond)
        def _():
            copy().start()

    def open(self):
        def one(j, carry):
            self.begin(j)
            return carry

        lax.fori_loop(0, min(self.lag, self.ticks), one, 0)

    def step(self, j):
        self.end(j)

        @pl.when(j + self.lag < self.ticks)
        def _():
            self.begin(j + self.lag)

    def steps(self, start, stop):
        def one(t, carry):
            self.step(t)
            return carry

        lax.fori_loop(start, stop, one, 0)

    def rest(self, j):
        self.steps(j, self.ticks)

        def settle(t, carry):
            self.settle(t)
            return carry

        lax.fori_loop(max(self.ticks - 2, 0), self.ticks, settle, 0)
        if self.carry is not None:
            for b in range(self.lag):
                self.carry[0][b] = self.acc[(self.ticks + b) % self.near]
                self.carry[1][b] = self.tot[(self.ticks + b) % self.ring]


class Io:
    def __init__(self):
        self.coming, self.later, self.going = [], [], []

    def more(self):
        for entry in self.later:
            entry[1].start()
        self.coming += self.later
        self.later = []

    def need(self, *bufs):
        for buf in bufs:
            for at, (ref, copy) in enumerate(self.coming):
                if ref is buf:
                    copy.wait()
                    del self.coming[at]
                    break

    def spill(self, *bufs):
        for buf in bufs:
            for entry in self.going:
                if entry[0] is buf and not entry[2]:
                    entry[1].start()
                    entry[2] = True

    def finish(self):
        self.more()
        self.need(*[ref for ref, _ in self.coming])
        self.spill(*[entry[0] for entry in self.going])
        for _, copy, _ in self.going:
            copy.wait()


def staged(kernel, n_in, fetch, spill, early):
    def wrapped(*refs):
        refs, sems = list(refs[:-1]), refs[-1]
        count = len(fetch) + len(spill)
        refs, bufs = refs[:-count], refs[-count:]
        io = Io()
        for n, i in enumerate(fetch):
            copy = pltpu.make_async_copy(refs[i], bufs[n], sems.at[n])
            if n < early:
                copy.start()
            (io.coming if n < early else io.later).append((bufs[n], copy))
            refs[i] = bufs[n]
        for n, o in enumerate(spill, len(fetch)):
            io.going.append([bufs[n], pltpu.make_async_copy(bufs[n], refs[n_in + o], sems.at[n]), False])
            refs[n_in + o] = bufs[n]
        kernel(io, *refs)
        io.finish()

    return wrapped


def call(kernel, cid, outs, ins, args, scratch, flops, vmem, out_specs, fetch, spill, early=0):
    moved = sum(int(np.prod(a.shape)) * a.dtype.itemsize for a in list(args) + list(outs))
    ins, out_specs = list(ins), list(out_specs)
    held = [pltpu.VMEM(args[i].shape, args[i].dtype) for i in fetch]
    held += [pltpu.VMEM(outs[o].shape, outs[o].dtype) for o in spill]
    for i in fetch:
        ins[i] = ANY
    for o in spill:
        out_specs[o] = ANY
    return pl.pallas_call(
        staged(kernel, len(args), fetch, spill, early),
        out_shape=outs,
        in_specs=ins,
        out_specs=out_specs,
        scratch_shapes=list(scratch) + held + [DMA((len(held),))],
        compiler_params=pltpu.CompilerParams(
            collective_id=cid, has_side_effects=True, vmem_limit_bytes=vmem << 20
        ),
        cost_estimate=pl.CostEstimate(flops=int(flops), bytes_accessed=moved, transcendentals=0),
    )(*args)


def sds(shape, dtype):
    return jax.ShapeDtypeStruct(shape, dtype)


def head_index(iota):
    head, lane = iota // LANE, iota % LANE
    index = jnp.where(lane < HALF, lane, lane - (LANE // 2 - HALF))
    pad = lane % (LANE // 2) >= HALF
    return jnp.where(pad, -1, head * HD + index)


def spread(rows, cols, first):
    source = head_index(lax.broadcasted_iota(jnp.int32, (rows, cols), 1))
    at = lax.broadcasted_iota(jnp.int32, (rows, cols), 0)
    return jnp.where((source >= 0) & (at == source + first), 1.0, 0.0).astype(BF)


def spread_t(rows, cols, first):
    source = head_index(lax.broadcasted_iota(jnp.int32, (rows, cols), 0))
    at = lax.broadcasted_iota(jnp.int32, (rows, cols), 1)
    return jnp.where((source >= 0) & (at == source + first), 1.0, 0.0).astype(BF)


def angle_tables():
    lane = np.arange(LANE)
    freq = np.where(
        lane % (LANE // 2) < HALF, THETA ** (-2.0 * (lane % (LANE // 2)) / HD), 0.0
    )
    fine = np.arange(32)[:, None] * freq[None]
    coarse = fine * 32.0
    return [f(t).astype(np.float32) for t in (coarse, fine) for f in (np.cos, np.sin)]


def exchange(k, stat, sems):
    copy = remote(stat.at[k], stat.at[k], sems.at[0], sems.at[1], {"col": 1 - k})
    copy.start()
    remote(stat.at[1 - k], stat.at[1 - k], sems.at[0], sems.at[1], {"col": 1 - k}).wait_recv()
    copy.wait_send()
    return stat[0][:, 0:1] + stat[1][:, 0:1]


def causal(shape):
    return lax.broadcasted_iota(jnp.int32, shape, 0) <= lax.broadcasted_iota(jnp.int32, shape, 1)


def front_kernel(
    io,
    x, dy, gain, gain_f, wq_h, wk_h, wv_h, wo_h, wg, wu, wd, tables,
    normed_o, f_o, qkv, kvt, wqkv_o, wo_o, wg_o, wu_o, wd_o, cos_o, sin_o, rstd1_o,
    attn, lse, hidden, rstd2_o, part, mid_o, gate_o, up_o,
    buf, dys, stage, gains, give_in, give_out, wq, wk, wv, wo, wsem, wrecv, csem, nsem, fsem,
    stat, ssem, grad, give, gsend, grecv, middle, d_gate, d_up, msem, *rest,
):
    r, k, rx, ry, r3 = place()
    width = x.shape[1]
    f_half = wg.shape[1] // 2
    mate = {"col": 1 - k}
    mine = pl.ds(pl.multiple_of(k * f_half, f_half), f_half)
    his = pl.ds(pl.multiple_of((1 - k) * f_half, f_half), f_half)
    keep = [
        pltpu.make_async_copy(wg.at[:, mine], wg_o.at[k], csem.at[1]),
        pltpu.make_async_copy(wu.at[:, mine], wu_o.at[k], csem.at[2]),
        pltpu.make_async_copy(wd.at[mine], wd_o.at[k], csem.at[3]),
    ]
    first = [
        pltpu.make_async_copy(src, dst, csem.at[4 + n])
        for n, (src, dst) in enumerate(((wq_h, wq), (wk_h, wk), (wv_h, wv), (wo_h, wo)))
    ]
    for c in first + keep:
        c.start()
    greet(rx, ry, k)
    gather = Gather(x, buf, rest[:5])
    gather_dy = Gather(dy, dys, rest[5:10])
    gather_f = Gather(None, buf, rest[10:15])
    total = Sum(rest[15:])
    gains[k] = gain[...].reshape(1, width)
    gather.start()

    def give_to(n, src, dst):
        return remote(src, dst.at[k], wsem.at[n], wrecv.at[n], mate)

    gives = [give_to(0, gains.at[k], gains)]
    gives[0].start()
    heads_q = wq.shape[1] // 2
    heads_k = wk.shape[0] // 2
    nq = heads_q // HD * LANE
    nk = heads_k // HD * LANE
    for c in first:
        c.wait()
    for core, dst_in, dst_out in ((1 - k, give_in, give_out), (k, wqkv_o.at[k], wo_o.at[k])):
        sq = spread(2 * heads_q, nq, core * heads_q)
        sk = spread(2 * heads_k, nk, core * heads_k)
        dst_in[:, 0:nq] = nn(wq[...], sq).astype(BF)
        dst_in[:, nq : nq + nk] = tn(wk[...], sk).astype(BF)
        dst_in[:, nq + nk : nq + 2 * nk] = tn(wv[...], sk).astype(BF)
        dst_out[...] = nn(spread_t(nq, 2 * heads_q, core * heads_q), wo[...]).astype(BF)
    gives += [give_to(1, give_in, wqkv_o), give_to(2, give_out, wo_o)]
    gives += [give_to(3, wg.at[:, his], wg_o), give_to(4, wu.at[:, his], wu_o), give_to(5, wd.at[his], wd_o)]
    for g in gives[1:]:
        g.start()
    sign = jnp.where(lax.broadcasted_iota(jnp.int32, (32, LANE), 1) < LANE // 2, -1.0, 1.0)
    cf, sf = tables[2], tables[3]
    for a in range(LENGTH // 32):
        ca, sa = tables[0, a : a + 1, :], tables[1, a : a + 1, :]
        cos_o[a * 32 : a * 32 + 32, :] = ca * cf - sa * sf
        sin_o[a * 32 : a * 32 + 32, :] = (sa * cf + ca * sf) * sign
    for c in keep:
        c.wait()
    for n in range(3):
        gives[n].wait_recv()

    def keep_normed(i):
        row, half = gather.piece(i)
        return pltpu.make_async_copy(stage.at[i % 2], normed_o.at[:, row, rows_of(half)], nsem.at[i])

    def project(i, row, half):
        at = rows_of(half)
        x0 = buf[0, row, at, :].astype(F32)
        x1 = buf[1, row, at, :].astype(F32)
        square = jnp.sum(x0 * x0, 1, keepdims=True) + jnp.sum(x1 * x1, 1, keepdims=True)
        rstd = lax.rsqrt(square / (2 * width) + EPS)
        n0 = (x0 * rstd * gains[0]).astype(BF)
        n1 = (x1 * rstd * gains[1]).astype(BF)

        @pl.when(i >= 2)
        def _():
            keep_normed(i - 2).wait()

        stage[i % 2, 0] = n0
        stage[i % 2, 1] = n1

        @pl.when(i < 2)
        def _():
            rstd1_o[at, :] = jnp.broadcast_to(rstd, (PIECE, LANE))

        got = nn(n0, wqkv_o[0]) + nn(n1, wqkv_o[1])
        keep_normed(i).start()
        pos = pl.ds(pl.multiple_of((row % 2) * 2 * PIECE + half * PIECE, PIECE), PIECE)
        out = pl.ds(pl.multiple_of(row * 2 * PIECE + half * PIECE, PIECE), PIECE)
        cos, sin = cos_o[pos, :], sin_o[pos, :]
        for p in range(4):
            u = got[:, p * LANE : (p + 1) * LANE]
            if p < 3:
                u = u * cos + pltpu.roll(u, LANE // 2, 1) * sin
            qkv[p, out, :] = u.astype(BF)
            if p >= 2:
                kvt[p - 2, :, out] = u.T.astype(BF)

    def dy_too(q):
        @pl.when(q == 0)
        def _():
            gather_dy.start()

    gather.run(project, None, dy_too)
    for i in (6, 7):
        keep_normed(i).wait()

    def attend(row, half):
        base = pl.multiple_of(row // 2 * LENGTH, LENGTH)
        at = rows_of(half)
        qrow = pl.ds(pl.multiple_of(row * 2 * PIECE + half * PIECE, PIECE), PIECE)
        order = (row % 2) * 2 + half

        def queries(p):
            span = PIECE * (p + 1)
            for head in range(2):
                keys = qkv[2, pl.ds(base, span), :]
                s = nt(keys, qkv[head, qrow, :])
                tail = jnp.where(causal((PIECE, PIECE)), s[span - PIECE :], -1e30)
                s = tail if p == 0 else jnp.concatenate([s[: span - PIECE], tail], 0)
                top = jnp.max(s, 0, keepdims=True)
                e = jnp.exp((s - top) * SCALE)
                weight = jnp.sum(e, 0, keepdims=True)
                probs = (e * (1.0 / weight)).astype(BF)
                mixed = nn(kvt[1, :, pl.ds(base, span)], probs)
                attn[row, at, head * LANE : (head + 1) * LANE] = mixed.T.astype(BF)
                lse[head, row * 2 + half] = top * SCALE + jnp.log(weight)

        for p in range(4):
            pl.when(order == p)(lambda p=p: queries(p))
        a = attn[row, at, :]
        return nn(a, wo_o[k]), nn(a, wo_o[1 - k])

    def dy_arrive(j):
        @pl.when(j == 3)
        def _():
            gather_dy.arrive(2)
            gather_dy.arrive(3)

        @pl.when(j == 7)
        def _():
            gather_dy.arrive(4)
            gather_dy.arrive(5)

    total.send_all(attend, dy_arrive)
    io.spill(qkv, kvt, cos_o, sin_o, attn, wqkv_o, wo_o)
    for g in gives[3:]:
        g.wait_recv()
    io.spill(wg_o, wu_o, wd_o)
    gather_dy.local().wait()

    def mid_pair(q, carry):
        for u in range(2):
            i = 2 * q + u
            gather_dy.ready(i)
            row, half = gather_dy.piece(i)
            at = rows_of(half)
            d_mid = nt(dys[0, row, at, :], wd_o[0]) + nt(dys[1, row, at, :], wd_o[1])
            d_gate[row, at, :] = d_mid.astype(BF)
        return carry

    lax.fori_loop(0, 3, mid_pair, 0)
    gather_dy.arrive(6)
    gather_dy.arrive(7)
    total.relay(4)
    total.relay(5)
    mid_pair(3, 0)
    gather_dy.finish()
    for half in range(2):
        at = rows_of(half)
        h = buf[k, r, at, :].astype(F32) + total.last(6 + half)
        hidden[at, :] = h
        stat[k, at, :] = jnp.broadcast_to(jnp.sum(h * h, 1, keepdims=True), (PIECE, LANE))
    rstd2 = lax.rsqrt(exchange(k, stat, ssem) / (2 * width) + EPS)
    buf[k, r] = (hidden[...] * rstd2 * gain_f[...].reshape(1, width)).astype(BF)
    rstd2_o[...] = jnp.broadcast_to(rstd2, rstd2_o.shape)
    gather_f.start()
    io.spill(hidden)

    def keep_mids(i):
        row, half = gather_f.piece(i)
        at = rows_of(half)
        return [
            pltpu.make_async_copy(src.at[row, at], dst.at[row, at], msem.at[n, i])
            for n, (src, dst) in enumerate(((middle, mid_o), (d_gate, gate_o), (d_up, up_o)))
        ]

    def keep_f(i):
        row, half = gather_f.piece(i)
        at = rows_of(half)
        return pltpu.make_async_copy(buf.at[:, row, at], f_o.at[:, row, at], fsem.at[i])

    def expand(i, row, half):
        at = rows_of(half)
        keep_f(i).start()

        @pl.when(i > 0)
        def _():
            for c in keep_mids(i - 1):
                c.start()

        f0, f1 = buf[0, row, at, :], buf[1, row, at, :]
        dy0, dy1 = dys[0, row, at, :], dys[1, row, at, :]
        gate = nn(f0, wg_o[0]) + nn(f1, wg_o[1])
        upper = nn(f0, wu_o[0]) + nn(f1, wu_o[1])
        d_mid = d_gate[row, at, :].astype(F32)
        sig = 1.0 / (1.0 + jnp.exp(-gate))
        swish = gate * sig
        mid = (swish * upper).astype(BF)
        middle[row, at, :] = mid
        d_gate[row, at, :] = (d_mid * upper * sig * (1.0 + gate * (1.0 - sig))).astype(BF)
        d_up[row, at, :] = (d_mid * swish).astype(BF)
        g0, g1 = tn(mid, dy0), tn(mid, dy1)

        @pl.when(i == 0)
        def _():
            grad[0] = g0
            grad[1] = g1

        @pl.when(i > 0)
        def _():
            grad[0] += g0
            grad[1] += g1

    gather_f.run(expand)
    for c in keep_mids(7):
        c.start()
    half = DOWN_CHUNKS // 4

    def swap(j, core):
        return remote(
            give.at[pl.ds(2 * j, 2)], part.at[pl.ds(2 * (half * core + j), 2)], gsend.at[j], grecv.at[j], mate
        )

    for j in range(half):
        for h in range(2):
            give[2 * j + h] = grad[1 - k, j * TALL + h * CHUNK : j * TALL + (h + 1) * CHUNK, :].astype(BF)
        swap(j, k).start()
    for j in range(half):
        for h in range(2):
            rows = slice(j * TALL + h * CHUNK, j * TALL + (h + 1) * CHUNK)
            part[2 * (half * k + j) + h] = grad[k, rows, :].astype(BF)
    for j in range(half):
        swap(j, 1 - k).wait_recv()
    io.spill(part)

    def kept(i, carry):
        keep_f(i).wait()
        for c in keep_mids(i):
            c.wait()
        return carry

    lax.fori_loop(0, 8, kept, 0)
    for j in range(half):
        swap(j, k).wait_send()
    for g in gives:
        g.wait_send()
    total.finish()


def front(x, dy, gain, gain_f, wq, wk, wv, wo, wg, wu, wd):
    tokens, width = x.shape
    f_half = wg.shape[1] // 2
    cols = 4 * LANE
    gathered = (2, 4, tokens, width)
    outs = [sds(gathered, BF), sds(gathered, BF)]
    outs += [sds((4, 4 * tokens, LANE), BF), sds((2, LANE, 4 * tokens), BF)]
    outs += [sds((2, width, cols), BF), sds((2, 2 * LANE, width), BF)]
    outs += [sds((2, width, f_half), BF)] * 2 + [sds((2, f_half, width), BF)]
    outs += [sds((LENGTH, LANE), F32)] * 2 + [sds((tokens, LANE), F32)]
    outs += [sds((4, tokens, 2 * LANE), BF), sds((2, 8, 1, PIECE), F32)]
    outs += [sds((tokens, width), F32), sds((tokens, LANE), F32)]
    outs += [sds((DOWN_CHUNKS, CHUNK, WIDE), BF)] + [sds((4, tokens, f_half), BF)] * 3
    half = DOWN_CHUNKS // 4
    scratch = [pltpu.VMEM(gathered, BF)] * 2 + [pltpu.VMEM((2, 2, PIECE, width), BF)]
    scratch += [pltpu.VMEM((2, 1, width), F32), pltpu.VMEM((width, cols), BF), pltpu.VMEM((2 * LANE, width), BF)]
    scratch += [pltpu.VMEM(w.shape, BF) for w in (wq, wk, wv, wo)]
    scratch += [DMA((6,)), DMA((6,)), DMA((8,)), DMA((8,)), DMA((8,))]
    scratch += [pltpu.VMEM((2, tokens, LANE), F32), DMA((2,)), pltpu.VMEM((2, f_half, width), F32)]
    scratch += [pltpu.VMEM((2 * half, CHUNK, WIDE), BF), DMA((half,)), DMA((half,))]
    scratch += [pltpu.VMEM((4, tokens, f_half), BF)] * 3 + [DMA((3, 8))]
    scratch += GATHER_SEMS * 3 + sum_scratch(width)
    ins = [ANY] * 2 + [VM] * 2 + [ANY] * 7 + [VM]
    args = [x, dy, gain, gain_f, wq, wk, wv, wo, wg, wu, wd, jnp.asarray(np.stack(angle_tables()))]
    out_specs = [ANY] * 2 + [VM] * (len(outs) - 5) + [ANY] * 3
    spill = [2, 3, 4, 5, 6, 7, 8, 9, 10, 12, 14, 16]
    return call(front_kernel, 0, outs, ins, args, scratch, 9e10, 61, out_specs, [], spill)


TICKS = 34


def flat(ref, h, m=None):
    got = ref[h] if m is None else ref[h, :, :, pl.ds(pl.multiple_of(m * 256, 256), 256)]
    return got.reshape(-1, got.shape[-1])


def contract_kernel(
    io,
    d_gate, d_up, wg, wu, hidden, rstd2, gain, dy, wo, attn, part_d, f_any,
    d_hidden, gains_o, part, part_o, d_attn, totals, acc_c, tot_c,
    stat, ssem, give, gsend, grecv, gathered, dya, grad, give_o, his_o, gsem, fsem, *rest,
):
    r, k, rx, ry, r3 = place()
    width = hidden.shape[1]
    fetch = pltpu.make_async_copy(f_any, gathered, fsem)
    greet(rx, ry, k, True)
    total = Sum(rest[:9])
    gather = Gather(dya, gathered, rest[9:14])
    parts = [(0, DOWN_CHUNKS, part_d), (DOWN_CHUNKS, MLP_CHUNKS, part), (MLP_CHUNKS, OUT_CHUNKS, part_o)]
    lag = lags(lax.axis_size("dp"))[0]
    line = Line(parts, totals, (acc_c, tot_c), rest[14:], 0, TICKS, OUT_CHUNKS, lag)
    io.need(d_gate, d_up, wg, wu, part_d)
    line.open()
    fetch.start()
    io.more()

    def compute(row, half):
        at = rows_of(half)
        g, u = d_gate[row, at, :], d_up[row, at, :]
        return nt(g, wg[k]) + nt(u, wu[k]), nt(g, wg[1 - k]) + nt(u, wu[1 - k])

    def early(j):
        @pl.when(j % 2 == 1)
        def _():
            line.step(j // 2)

    total.send_all(compute, early)

    def swap(e, core):
        to = part.at[pl.ds(2 * (e // 4 * 8 + 4 * core + e % 4), 2)]
        return remote(give.at[pl.ds(2 * e, 2)], to, gsend.at[e], grecv.at[e], {"col": 1 - k})

    def wide_part(h, right, dst, first):
        def one(m, carry):
            got = tn(flat(gathered, h, m), right[...].reshape(-1, right.shape[2])).astype(BF)
            for b in range(2):
                lanes = pl.ds(pl.multiple_of((2 * m + b) * TALL, TALL), TALL)
                for j in range(4):
                    for u in range(2):
                        rows = slice(b * TALL + u * CHUNK, b * TALL + (u + 1) * CHUNK)
                        dst[2 * (first + j) + u, :, lanes] = got[rows, j * TALL : (j + 1) * TALL]
            return carry

        lax.fori_loop(0, width // 256, one, 0)

    fetch.wait()
    wide_part(1 - k, d_gate, give, 0)
    for e in range(4):
        swap(e, k).start()
    wide_part(k, d_gate, part, 4 * k)
    line.steps(4, 6)
    wide_part(1 - k, d_up, give, 4)
    for e in range(4, 8):
        swap(e, k).start()
    wide_part(k, d_up, part, 8 + 4 * k)
    total.relay(4)
    total.relay(5)
    for e in range(8):
        swap(e, 1 - k).wait_recv()
    io.spill(part)
    io.need(hidden, dy, wo, attn)
    line.steps(6, 13)
    gains = jnp.zeros((1, width), F32)
    for half in range(2):
        at = rows_of(half)
        d_nf = total.last(6 + half)
        h = hidden[at, :]
        gains = gains + jnp.sum(d_nf * h * rstd2[at, 0:1], 0, keepdims=True)
        scaled = d_nf * gain[...].reshape(1, width)
        d_hidden[at, :] = scaled
        stat[k, at, :] = jnp.broadcast_to(jnp.sum(scaled * h, 1, keepdims=True), (PIECE, LANE))
    gains_o[...] = gains
    inner = exchange(k, stat, ssem) / (2 * width)
    rs = rstd2[:, 0:1]
    value = dy[...].astype(F32) + rs * d_hidden[...] - hidden[...] * (rs * rs * rs * inner)
    d_hidden[...] = value
    dya[...] = value.astype(BF)
    gather.start()
    io.spill(d_hidden)

    def piece(i, row, half):
        at = rows_of(half)
        d0, d1 = gathered[0, row, at, :], gathered[1, row, at, :]
        d_attn[row, at, :] = (nt(d0, wo[0]) + nt(d1, wo[1])).astype(BF)
        a = attn[row, at, :]
        g0, g1 = tn(a, d0), tn(a, d1)

        @pl.when(i == 0)
        def _():
            grad[0] = g0
            grad[1] = g1

        @pl.when(i > 0)
        def _():
            grad[0] += g0
            grad[1] += g1

    def before(q):
        line.steps(jnp.where(q == 0, 13, 15 + 4 * q), 19 + 4 * q)

    gather.run(piece, before)
    give_o[...] = grad[1 - k].astype(BF)
    give_out = remote(give_o, his_o, gsem.at[0], gsem.at[1], {"col": 1 - k})
    give_out.start()
    q_cols = part_o.shape[0] * CHUNK
    mine = nn(spread(q_cols, 2 * LANE, k * (q_cols // 2)), grad[k].astype(BF))
    give_out.wait_recv()
    out = mine + nn(spread(q_cols, 2 * LANE, (1 - k) * (q_cols // 2)), his_o[...])
    for c in range(q_cols // CHUNK):
        part_o[c] = out[c * CHUNK : (c + 1) * CHUNK].astype(BF)
    line.rest(31)
    for e in range(8):
        swap(e, k).wait_send()
    give_out.wait_send()
    total.finish()


def contract(d_gate, d_up, wg, wu, hidden, rstd2, gain, dy, wo, attn, part_d, all_f):
    tokens, width = hidden.shape
    n = lax.axis_size("dp")
    outs = [sds((tokens, width), F32), sds((1, width), F32)]
    outs += [sds((MLP_CHUNKS - DOWN_CHUNKS, CHUNK, WIDE), BF), sds((OUT_CHUNKS - MLP_CHUNKS, CHUNK, WIDE), BF)]
    outs += [sds((4, tokens, 2 * LANE), BF)] + line_outs(TICKS, lags(n)[0])
    out_specs = [VM] * 5 + [ANY] + [VM] * 2
    scratch = [pltpu.VMEM((2, tokens, LANE), F32), DMA((2,))]
    scratch += [pltpu.VMEM((16, CHUNK, WIDE), BF), DMA((8,)), DMA((8,))]
    scratch += [pltpu.VMEM((2, 4, tokens, width), BF), pltpu.VMEM((tokens, width), BF)]
    scratch += [pltpu.VMEM((2, 2 * LANE, width), F32)] + [pltpu.VMEM((2 * LANE, width), BF)] * 2
    scratch += [DMA((2,)), DMA]
    scratch += sum_scratch(width) + GATHER_SEMS + line_scratch(n, TICKS, lags(n)[0])
    args = [d_gate, d_up, wg, wu, hidden, rstd2, gain, dy, wo, attn, part_d, all_f]
    ins = [VM] * 11 + [ANY]
    fetch = [0, 1, 2, 3, 10, 4, 7, 8, 9]
    return call(
        contract_kernel, 1, outs, ins, args, scratch, 5e10, vmem_limit(n), out_specs, fetch, [0, 2, 3, 4], 5
    )


def vmem_limit(n):
    return 60 if n <= 4 else 63


def columns(rows, cols, core, q_cols, k_cols):
    i = lax.broadcasted_iota(jnp.int32, (rows, cols), 0)
    at = lax.broadcasted_iota(jnp.int32, (rows, cols), 1)
    part, lane = i // LANE, i % LANE
    index = jnp.where(lane < HALF, lane, lane - (LANE // 2 - HALF))
    q = core * (q_cols // 2) + part * HD
    kv = q_cols + (part - 2) * k_cols + core * (k_cols // 2)
    to = jnp.where(part < 2, q, kv) + index
    pad = lane % (LANE // 2) >= HALF
    return jnp.where((at == to) & (pad == False), 1.0, 0.0).astype(BF)


def backward_kernel(
    q_cols, k_cols,
    io,
    qkv, kvt, lse, d_attn, cos, sin, middle, wd, hidden, wqkv, x, rstd1, d_hidden, gain, gains_f,
    part_m, part_o, acc_c, tot_c, normed_any,
    output, grad_x, gains_o, totals, totals_in,
    dk, dv, d_proj, normed, part, mine, give, his, gsem, stat, ssem, free, fsem,
    mine_g, pair_g, slots, gsend, grecv, *rest,
):
    r, k, rx, ry, r3 = place()
    width = x.shape[1]
    n = lax.axis_size("dp")
    z = lax.axis_index("dp")
    fetch = pltpu.make_async_copy(normed_any, normed, fsem)
    greet(rx, ry, k, True, True)
    sums = rest[:5]
    down = Sum(sums + rest[5:9])
    into = Sum(sums + rest[9:13])
    lag, lag_in = lags(n)
    count = ALL_CHUNKS - OUT_CHUNKS
    ticks, ticks_in = line_ticks(n, OUT_CHUNKS, lag) - TICKS, line_ticks(n, count, lag_in)
    parts = [(DOWN_CHUNKS, MLP_CHUNKS, part_m), (MLP_CHUNKS, OUT_CHUNKS, part_o)]
    line = Line(parts, totals, None, rest[13:23], TICKS, ticks, OUT_CHUNKS, lag, (acc_c, tot_c))
    line_in = Line([(0, count, part)], totals_in, None, rest[23:], 0, ticks_in, count, lag_in)
    io.need(part_m, part_o, middle, wd)
    line.open()
    io.more()

    def down_piece(row, half):
        m = middle[row, rows_of(half), :]
        return nn(m, wd[k]), nn(m, wd[1 - k])

    def early(j):
        @pl.when(j % 3 == 1)
        def _():
            line.step(j // 3)

    down.send_all(down_piece, early)

    fetch.start()
    io.need(qkv, kvt, d_attn, cos, sin)

    def unrotate(u, p):
        at = pl.ds(p * PIECE, PIECE)
        return u * cos[at, :] - pltpu.roll(u, LANE // 2, 1) * sin[at, :]

    def sequence(seq):
        base = pl.multiple_of(seq * LENGTH, LENGTH)

        def one_head(head, carry):
            for p in range(4):
                span = PIECE * (p + 1)
                row = seq * 2 + p // 2
                at = pl.ds((p % 2) * PIECE, PIECE)
                out = pl.ds(pl.multiple_of(base + p * PIECE, PIECE), PIECE)
                keys = qkv[2, pl.ds(base, span), :]
                q = qkv[head, out, :]
                lane = pl.ds(pl.multiple_of(head * LANE, LANE), LANE)
                do = d_attn[row, at, lane]
                e = jnp.exp(nt(keys, q) * SCALE - lse[head, seq * 4 + p])
                tail = jnp.where(causal((PIECE, PIECE)), e[span - PIECE :], 0.0)
                e = tail if p == 0 else jnp.concatenate([e[: span - PIECE], tail], 0)
                dp = nt(qkv[3, pl.ds(base, span), :], do)
                inner = jnp.sum(e * dp, 0, keepdims=True)
                ds = (e * (dp - inner)).astype(BF)
                dv[0:span, :] += nn(e.astype(BF), do)
                dk[0:span, :] += nn(ds, q)
                dq = nn(kvt[0, :, pl.ds(base, span)], ds).T * SCALE
                d_proj[out, lane] = unrotate(dq, p).astype(BF)
                if p % 2 == 1:
                    tick = 3 + seq * 8 + head * 4 + p - 1
                    line.steps(tick, tick + 2)
            return carry

        dk[...] = jnp.zeros_like(dk)
        dv[...] = jnp.zeros_like(dv)
        lax.fori_loop(0, 2, one_head, 0)
        for p in range(4):
            at = pl.ds(p * PIECE, PIECE)
            out = pl.ds(pl.multiple_of(base + p * PIECE, PIECE), PIECE)
            d_proj[out, 2 * LANE : 3 * LANE] = unrotate(dk[at, :] * SCALE, p).astype(BF)
            d_proj[out, 3 * LANE : 4 * LANE] = dv[at, :].astype(BF)

    def both(seq, carry):
        sequence(seq)

        @pl.when(seq == 0)
        def _():
            down.relay(4)
            down.relay(5)

        return carry

    lax.fori_loop(0, 2, both, 0)
    io.need(hidden)
    for half in range(2):
        at = rows_of(half)
        output[at, :] = hidden[at, :] + down.last(6 + half)
    down.finish()
    io.spill(output)
    for device in ({"row": rx}, {"row": ry}, {"col": 1 - k}):
        pl.semaphore_signal(free, inc=1, device_id=device, device_id_type=MESH)
    pl.semaphore_wait(free, 3)

    fetch.wait()

    def in_part(h, dst):
        def one(m, carry):
            dst[pl.ds(pl.multiple_of(m * 256, 256), 256), :] = tn(flat(normed, h, m), d_proj[...]).astype(BF)
            return carry

        lax.fori_loop(0, width // 256, one, 0)

    in_part(1 - k, give)
    swap = remote(give, his, gsem.at[0], gsem.at[1], {"col": 1 - k})
    swap.start()
    line.steps(19, 21)
    in_part(k, mine)
    line.steps(21, 23)
    cols = q_cols + 2 * k_cols
    got = nn(mine[...], columns(4 * LANE, cols, k, q_cols, k_cols))
    swap.wait_recv()
    got = got + nn(his[...], columns(4 * LANE, cols, 1 - k, q_cols, k_cols))
    for c in range(width // CHUNK):
        part[c] = got[c * CHUNK : (c + 1) * CHUNK].astype(BF)

    def into_piece(row, half):
        d = d_proj[pl.ds(pl.multiple_of(row * 2 * PIECE + half * PIECE, PIECE), PIECE), :]
        return nt(d, wqkv[k]), nt(d, wqkv[1 - k])

    line_in.open()

    def both_lines(t, carry):
        line.step(23 + t)
        line_in.step(t)
        return carry

    def beside(j):
        @pl.when(j % 2 == 1)
        def _():
            both_lines(j // 2, 0)

    io.need(wqkv)
    into.send_all(into_piece, beside)
    lax.fori_loop(4, 5, both_lines, 0)
    line_in.steps(5, 7)
    into.relay(4)
    into.relay(5)
    line_in.steps(7, 12)
    io.need(x, d_hidden)
    gains = jnp.zeros((1, width), F32)
    for half in range(2):
        at = rows_of(half)
        d_na = into.last(6 + half)
        xs = x[at, :].astype(F32)
        gains = gains + jnp.sum(d_na * xs * rstd1[at, 0:1], 0, keepdims=True)
        scaled = d_na * gain[...].reshape(1, width)
        grad_x[at, :] = scaled
        stat[k, at, :] = jnp.broadcast_to(jnp.sum(scaled * xs, 1, keepdims=True), (PIECE, LANE))

    def row_total(step, device):
        copy = remote(mine_g.at[step], pair_g.at[step], gsend.at[n + step], grecv.at[n + step], {"row": device})
        copy.start()
        return copy

    mine_g[0, 0:1] = gains
    mine_g[0, 1:2] = gains_f[...]
    over_x = row_total(0, rx)
    inner = exchange(k, stat, ssem) / (2 * width)
    rs = rstd1[:, 0:1]
    over_x.wait_recv()
    mine_g[1] = mine_g[0] + pair_g[0]
    over_y = row_total(1, ry)
    grad_x[...] = d_hidden[...] + rs * grad_x[...] - x[...].astype(F32) * (rs * rs * rs * inner)
    over_y.wait_recv()
    slots[z] = mine_g[1] + pair_g[1]

    def over_dp(t, mine):
        other = (z + t) % n
        g = z if mine else other
        return remote(slots.at[g], slots.at[g], gsend.at[t], grecv.at[g], {"dp": other})

    def start(t, carry):
        over_dp(t, True).start()
        return carry

    lax.fori_loop(1, n, start, 0)
    io.spill(grad_x)
    line_in.rest(12)
    line.rest(28)

    def wait(t, carry):
        over_dp(t, False).wait_recv()
        over_dp(t, True).wait_send()
        return carry

    lax.fori_loop(1, n, wait, 0)
    gains_o[...] = lax.fori_loop(1, n, lambda g, total: total + slots[g], slots[0])
    over_x.wait_send()
    over_y.wait_send()
    swap.wait_send()
    into.finish()


def backward(
    qkv, kvt, lse, d_attn, cos, sin, middle, wd, hidden, wqkv, x, rstd1, d_hidden, gain, gains_f,
    part_m, part_o, acc, tot, normed, q_cols, k_cols,
):
    tokens, width = x.shape
    n = lax.axis_size("dp")
    lag, lag_in = lags(n)
    ticks = line_ticks(n, OUT_CHUNKS, lag) - TICKS
    ticks_in = line_ticks(n, ALL_CHUNKS - OUT_CHUNKS, lag_in)
    outs = [sds((tokens, width), F32)] * 2 + [sds((2, width), F32)]
    outs += [sds((t, CHUNK, WIDE), BF) for t in (ticks, ticks_in)]
    scratch = [pltpu.VMEM((LENGTH, LANE), F32)] * 2 + [pltpu.VMEM((4 * tokens, 4 * LANE), BF)]
    scratch += [pltpu.VMEM((2, 4, tokens, width), BF), pltpu.VMEM((ALL_CHUNKS - OUT_CHUNKS, CHUNK, WIDE), BF)]
    scratch += [pltpu.VMEM((width, 4 * LANE), BF)] * 3 + [DMA((2,))]
    scratch += [pltpu.VMEM((2, tokens, LANE), F32), DMA((2,)), pltpu.SemaphoreType.REGULAR, DMA]
    scratch += [pltpu.VMEM((2, 2, width), F32)] * 2 + [pltpu.VMEM((n, 2, width), F32)]
    scratch += [DMA((n + 2,)), DMA((n + 2,))]
    both = sum_scratch(width)
    scratch += both + both[5:] + line_scratch(n, ticks, lag) + line_scratch(n, ticks_in, lag_in)
    args = [qkv, kvt, lse, d_attn, cos, sin, middle, wd, hidden, wqkv, x, rstd1, d_hidden, gain, gains_f]
    args += [part_m, part_o, acc, tot, normed]
    kernel = functools.partial(backward_kernel, q_cols, k_cols)
    ins = [VM] * (len(args) - 1) + [ANY]
    fetch = [15, 16, 6, 7, 0, 1, 3, 4, 5, 8, 9, 10, 12]
    return call(
        kernel, 2, outs, ins, args, scratch, 5e10, vmem_limit(n), [VM] * 3 + [ANY] * 2, fetch, [0, 1], 4
    )


SLOTS = 4


def unpack_kernel(q_cols, k_cols, tot1, tot2, tot3, down, gate, up, out, q_o, k_o, v_o, whole, last, wide, turned, isem, osem):
    n, s, _, _ = line_place()
    steps = 2 * (n // 2) - 2 - s
    lag, lag_in = lags(n)
    first = tot1.shape[0]
    loads = [
        pltpu.make_async_copy(tot1, whole.at[pl.ds(0, first)], isem.at[0]),
        pltpu.make_async_copy(tot2, whole.at[pl.ds(first, tot2.shape[0])], isem.at[1]),
        pltpu.make_async_copy(tot3, last, isem.at[2]),
    ]
    for c in loads:
        c.start()
    loads[0].wait()
    late = whole.shape[0] - OUT_CHUNKS > first - DOWN_CHUNKS
    if late:
        loads[1].wait()

    def chunk(c, lanes):
        return whole[c + lag * steps, :, lanes].astype(F32)

    drains = []

    def run(count, make, copies):
        def one(b, carry):
            slot = b % SLOTS

            @pl.when(b >= SLOTS)
            def _():
                for c in copies(b - SLOTS, slot):
                    c.wait()

            make(b, slot)
            for c in copies(b, slot):
                c.start()
            return carry

        lax.fori_loop(0, count, one, 0)

        def drain(b, carry):
            for c in copies(b, b % SLOTS):
                c.wait()
            return carry

        drains.append(lambda: lax.fori_loop(max(count - SLOTS, 0), count, drain, 0))

    def rows(b):
        return pl.ds(pl.multiple_of(b * TALL, TALL), TALL)

    def tall(g, start, to, count):
        def make(b, slot):
            for u in range(2):
                wide[g, slot, u * CHUNK : (u + 1) * CHUNK, 0:WIDE] = chunk(start + 2 * b + u, slice(0, WIDE))

        def copies(b, slot):
            return [pltpu.make_async_copy(wide.at[g, slot, :, pl.ds(0, WIDE)], to.at[rows(b)], osem.at[g, slot, 0])]

        run(count, make, copies)

    def broad(g, start, to):
        def make(b, slot):
            for c in range(8):
                for u in range(2):
                    got = chunk(start + 2 * c + u, rows(b))
                    wide[g, slot, u * CHUNK : (u + 1) * CHUNK, c * TALL : (c + 1) * TALL] = got

        def copies(b, slot):
            return [pltpu.make_async_copy(wide.at[g, slot], to.at[rows(b)], osem.at[g, slot, 0])]

        run(WIDE // TALL, make, copies)

    tall(0, 0, down, 8)
    if not late:
        loads[1].wait()
    broad(1, DOWN_CHUNKS, gate)
    broad(2, DOWN_CHUNKS + 16, up)
    tall(3, MLP_CHUNKS, out, q_cols // TALL)
    loads[2].wait()
    g = 4

    def make_in(b, slot):
        for u in range(2):
            got = last[2 * b + u + lag_in * steps].astype(F32)
            wide[g, slot, u * CHUNK : (u + 1) * CHUNK, 0:WIDE] = got
        turned[slot, 0] = wide[g, slot, :, q_cols : q_cols + k_cols].T
        turned[slot, 1] = wide[g, slot, :, q_cols + k_cols : WIDE].T

    def copies_in(b, slot):
        return [
            pltpu.make_async_copy(wide.at[g, slot, :, pl.ds(0, q_cols)], q_o.at[rows(b)], osem.at[g, slot, 0]),
            pltpu.make_async_copy(turned.at[slot, 0], k_o.at[:, rows(b)], osem.at[g, slot, 1]),
            pltpu.make_async_copy(turned.at[slot, 1], v_o.at[:, rows(b)], osem.at[g, slot, 2]),
        ]

    run(WIDE // TALL, make_in, copies_in)
    for drain in drains:
        drain()


def unpack(tots, q_cols, k_cols):
    outs = [sds((8 * TALL, WIDE), F32), sds((WIDE, 8 * TALL), F32), sds((WIDE, 8 * TALL), F32)]
    outs += [sds((q_cols, WIDE), F32), sds((WIDE, q_cols), F32), sds((k_cols, WIDE), F32), sds((k_cols, WIDE), F32)]
    return pl.pallas_call(
        functools.partial(unpack_kernel, q_cols, k_cols),
        out_shape=outs,
        in_specs=[ANY] * 3,
        out_specs=[ANY] * len(outs),
        scratch_shapes=[
            pltpu.VMEM((tots[0].shape[0] + tots[1].shape[0], CHUNK, WIDE), BF),
            pltpu.VMEM(tots[2].shape, BF),
            pltpu.VMEM((5, SLOTS, TALL, 8 * TALL), F32),
            pltpu.VMEM((SLOTS, 2, k_cols, TALL), F32),
            DMA((3,)),
            DMA((5, SLOTS, 3)),
        ],
        compiler_params=pltpu.CompilerParams(vmem_limit_bytes=62 << 20),
        cost_estimate=pl.CostEstimate(flops=0, bytes_accessed=3 * ALL_CHUNKS * TALL * WIDE, transcendentals=0),
    )(*tots)


def on_device(
    layer_input, gain_attn, gain_ffn, w_query, w_key, w_value, w_out, w_gate, w_up, w_down, cotangent
):
    tokens, width = layer_input.shape
    q_cols, k_cols = w_query.shape[1], w_key.shape[1]
    gain_a, gain_f = gain_attn, gain_ffn
    (
        normed, all_f, qkv, kvt, wqkv, wo, wg, wu, wd, cos, sin, rstd1,
        attn, lse, hidden, rstd2, part_d, middle, d_gate, d_up,
    ) = front(
        layer_input, cotangent, gain_a, gain_f,
        w_query, w_key.T, w_value.T, w_out, w_gate, w_up, w_down,
    )
    d_hidden, gains_f, part_m, part_o, d_attn, tot1, acc, tot = contract(
        d_gate, d_up, wg, wu, hidden, rstd2, gain_f, cotangent, wo, attn, part_d, all_f
    )
    output, grad_x, gains, tot2, tot3 = backward(
        qkv, kvt, lse, d_attn, cos, sin, middle, wd, hidden, wqkv, layer_input, rstd1, d_hidden,
        gain_a, gains_f, part_m, part_o, acc, tot, normed, q_cols, k_cols,
    )
    down, gate, up, out, g_q, g_k, g_v = unpack([tot1, tot2, tot3], q_cols, k_cols)
    return output, grad_x, gains[0], gains[1], g_q, g_k.T, g_v.T, out, gate, up, down


def solution(mesh):
    assert mesh.shape["row"] == 4 and mesh.shape["col"] == 2
    tokens = P(("dp", "row"), "col")
    wide = P("col", "row")
    tall = P("row", "col")
    return jax.shard_map(
        on_device,
        mesh=mesh,
        in_specs=(tokens, P("col"), P("col"), wide, wide, wide, tall, wide, wide, tall, tokens),
        out_specs=(tokens, tokens, P("col"), P("col"), wide, wide, wide, tall, wide, wide, tall),
        check_vma=False,
    )
```
